32 devices in a mesh: dp: 16 (over z, y, x), rep: 2 (over core).
Axes of the slice: x: 2, y: 2, z: 4, core: 2. Of those that a mesh axis runs over, the one named last changes fastest.
Arguments:
- queries: bfloat16 [2048, 2048], P(('dp', 'rep')), may hold values from -24 to 24
- documents: bfloat16 [2048, 2048], P(('dp', 'rep')), may hold values from -24 to 24
- partner: int32 [2048], P(('dp', 'rep')), may hold values from 0 to 2047, each once
Outputs:
- grad_queries: float32 [2048, 2048], P(('dp', 'rep'))
- grad_documents: float32 [2048, 2048], P(('dp', 'rep'))
The draws below stay inside these ranges and needn't reach their ends.
Inputs may be any that keep to these rules, and one draw needn't show every extreme that they name: `partner`: every document index appears exactly once.
All inputs are finite; a program needn't handle non-finite values.
Results may differ from the reference program's by a relative error of at most 0.0031.
Values may be sent and summed in bfloat16 or wider, within the bound.
No kernel may reach another device: no remote copies, remote signals or barrier semaphores. Data moves between devices by JAX's collectives and lax.ppermute only.
A program may use at most 256 MiB of HBM per device.

```python
import math
import jax
import jax.numpy as jnp
from jax import lax

D = 2048
WIDTHS = 9
PAIRS = 2048


def joint_draw(key):
    key_list = jax.random.split(jax.random.fold_in(key, 7), 2)
    query_part = jax.random.normal(key_list[0], (PAIRS, D), jnp.float32)
    document_part = jax.random.normal(key_list[1], (PAIRS, D), jnp.float32)
    return (jnp.clip(query_part, -24.0, 24.0), jnp.clip(document_part, -24.0, 24.0))


def draw_queries(key, part):
    return joint_draw(key)[0].astype(jnp.bfloat16)


def draw_documents(key, part):
    return joint_draw(key)[1].astype(jnp.bfloat16)


def setup_inputs(seed: int = 0) -> dict:
    seeds = jax.random.split(jax.random.key(seed), 4)
    queries = draw_queries(jax.random.fold_in(seeds[3], 71), 0)
    documents = draw_documents(jax.random.fold_in(seeds[3], 71), 0)
    partner = jax.random.permutation(seeds[2], PAIRS).astype(jnp.int32)
    return dict(queries=queries, documents=documents, partner=partner)


logit_gain = 3.0


def reference(queries, documents, partner):
    uppers = [D >> (WIDTHS - 1 - nested) for nested in range(WIDTHS)]
    lowers = [0] + uppers[:-1]
    block_rows = math.gcd(PAIRS, 512)
    block_count = PAIRS // block_rows
    doc_ids = jnp.arange(PAIRS, dtype=jnp.int32)

    def visit_block(doc_grad, block_data):
        rows_q, rows_p = block_data
        target = (rows_p[:, None] == doc_ids[None, :]).astype(jnp.float32)
        suffix = jnp.zeros((block_rows, PAIRS), jnp.float32)
        pieces = [None] * WIDTHS
        for nested in reversed(range(WIDTHS)):
            lower_col = lowers[nested]
            upper_col = uppers[nested]
            scale = logit_gain * upper_col ** -0.5
            logits = jnp.dot(rows_q[:, :upper_col], documents[:, :upper_col].T,
                             preferred_element_type=jnp.float32) * scale
            row_peak = jnp.max(logits, axis=1, keepdims=True)
            row_total = row_peak + jnp.log(jnp.sum(jnp.exp(logits - row_peak), axis=1, keepdims=True))
            suffix = suffix + (jnp.exp(logits - row_total) - target) * scale
            band = suffix.astype(jnp.bfloat16)
            pieces[nested] = jnp.dot(band, documents[:, lower_col:upper_col], preferred_element_type=jnp.float32)
            doc_grad = doc_grad.at[:, lower_col:upper_col].add(
                jnp.dot(band.T, rows_q[:, lower_col:upper_col], preferred_element_type=jnp.float32))
        return doc_grad, jnp.concatenate(pieces, axis=1)

    start_grad = jnp.zeros((PAIRS, D), jnp.float32)
    grad_documents, stacked = lax.scan(
        visit_block, start_grad,
        (queries.reshape(block_count, block_rows, D), partner.reshape(block_count, block_rows)))
    grad_queries = stacked.reshape(PAIRS, D)
    return grad_queries, grad_documents
```

```python
import functools
import math

import jax
import jax.numpy as jnp
from jax import lax
from jax.experimental import pallas as pl
from jax.experimental.pallas import tpu as pltpu
from jax.sharding import PartitionSpec as P

WIDTHS = 9
AXES = ("dp", "rep")
LOG2E = 1.4426950408889634
LN2 = 0.6931471805599453
STATS = 16
LANES = 128


logit_gain = 3.0


def width_list(feature_dim):
    return [feature_dim >> WIDTHS - 1 - nested for nested in range(WIDTHS)]


def transposed_dot(a, b):
    return lax.dot_general(a, b, (((1,), (1,)), ((), ())), preferred_element_type=jnp.float32)


def prefix_scores(v_ref, w_ref, rows, uppers):
    narrow = [m for m in uppers if m <= LANES]
    count = rows.size
    head = v_ref[rows, :LANES]
    lane = lax.broadcasted_iota(jnp.int32, head.shape, 1)
    masked = [jnp.where(lane < m, head, jnp.zeros_like(head)) for m in narrow]
    stacked = transposed_dot(jnp.concatenate(masked, axis=0), w_ref[:, :LANES])
    result = [stacked[k * count:(k + 1) * count] for k in range(len(narrow))]
    lower = narrow[-1]
    for upper in uppers[len(narrow):]:
        part = transposed_dot(v_ref[rows, lower:upper], w_ref[:, lower:upper])
        result.append(result[-1] + part)
        lower = upper
    return result


def block_of(total):
    return min(total, 256)


def load_tile(refs, scratch):
    at = 0
    for ref in refs:
        scratch[at:at + ref.shape[0], :] = ref[...]
        at += ref.shape[0]


def stats_kernel(pieces, uppers, *refs):
    role_ref, partner_ref = refs[:2]
    v_refs, w_refs = refs[2:2 + pieces], refs[2 + pieces:2 + 2 * pieces]
    out_ref, v_ref, w_ref, col_ref = refs[2 + 2 * pieces:]
    load_tile(v_refs, v_ref)
    load_tile(w_refs, w_ref)
    total = v_ref.shape[0]
    block = block_of(total)
    steps = total // block
    gains = [logit_gain * m ** -0.5 * LOG2E for m in uppers]
    own = partner_ref.shape[1]
    out_ref[...] = jnp.zeros_like(out_ref)

    @pl.when(role_ref[0] == 0)
    def _():
        for step in range(steps):
            rows = pl.ds(step * block, block)
            col_ref[rows, :] = jnp.zeros((block, LANES), jnp.float32)
            for k, s in enumerate(prefix_scores(v_ref, w_ref, rows, uppers)):
                logits = s * gains[k]
                peak = jnp.max(logits, axis=1, keepdims=True)
                mass = jnp.sum(jnp.exp2(logits - peak), axis=1, keepdims=True)
                col_ref[rows, k:k + 1] = peak + jnp.log(mass) * LOG2E
        out_ref[...] = col_ref[...].T[:STATS]

    @pl.when(role_ref[0] != 0)
    def _():
        peaks, masses = [None] * len(uppers), [None] * len(uppers)
        for step in range(steps):
            rows = pl.ds(step * block, block)
            for k, s in enumerate(prefix_scores(v_ref, w_ref, rows, uppers)):
                logits = s * gains[k]
                peak = jnp.max(logits, axis=0, keepdims=True)
                mass = jnp.sum(jnp.exp2(logits - peak), axis=0, keepdims=True)
                if step:
                    top = jnp.maximum(peak, peaks[k])
                    mass = mass * jnp.exp2(peak - top) + masses[k] * jnp.exp2(peaks[k] - top)
                    peak = top
                peaks[k], masses[k] = peak, mass
        for k in range(len(uppers)):
            out_ref[k:k + 1, :] = peaks[k] + jnp.log(masses[k]) * LOG2E

    out_ref[len(uppers):len(uppers) + 1, :own] = partner_ref[...]


def document_ids(shape, axis, first, own_rows, masks):
    at = lax.broadcasted_iota(jnp.int32, shape, axis)
    shift = own_rows.bit_length() - 1
    piece = at >> shift
    device = first ^ (piece & 1)
    for s, mask in enumerate(masks):
        device = device ^ (((piece >> (1 + s)) & 1) * mask)
    return (device * own_rows + (at & (own_rows - 1))).astype(jnp.float32)


def grads_kernel(pieces, uppers, own_rows, masks, *refs):
    me_ref = refs[0]
    groups = pieces // 2
    stat_refs = refs[1:1 + groups]
    v_refs = refs[1 + groups:1 + groups + pieces]
    w_refs = refs[1 + groups + pieces:1 + groups + 2 * pieces]
    out_refs = refs[1 + groups + 2 * pieces:1 + 2 * groups + 2 * pieces]
    v_ref, w_ref, score_ref, col_ref = refs[1 + 2 * groups + 2 * pieces:]
    load_tile(v_refs, v_ref)
    load_tile(w_refs, w_ref)
    total = v_ref.shape[0]
    block = block_of(total)
    chip_rows = total // groups
    count = len(uppers)
    scales = [logit_gain * m ** -0.5 for m in uppers]
    me = me_ref[0]
    lead = (me & 1) == 0

    parts = []
    partners = []
    for j, ref in enumerate(stat_refs):
        parts.append(jnp.concatenate(
            [ref[:, (i ^ j) * chip_rows:((i ^ j) + 1) * chip_rows] for i in range(groups)], axis=1))
        partners.append(ref[count:count + 1, :chip_rows])
    peak = functools.reduce(jnp.maximum, parts)
    mass = functools.reduce(lambda a, b: a + b, [jnp.exp2(part - peak) for part in parts])
    totals = peak + jnp.log(mass) * LOG2E
    partner_row = jnp.concatenate(partners, axis=1)
    packed = jnp.concatenate(
        [totals[:count], partner_row, jnp.zeros((LANES - count - 1, total), jnp.float32)], axis=0)
    col_ref[...] = packed.T
    zero_or = lambda keep, x: jnp.where(keep, x, jnp.zeros_like(x))
    document_row = document_ids((1, total), 1, me | 1, own_rows, masks)
    id_row = jnp.where(lead, document_row, partner_row)
    shifts = [math.log2(s) for s in scales]
    total_rows = [zero_or(jnp.logical_not(lead), totals[k:k + 1]) - shifts[k] for k in range(count)]

    narrow = [m for m in uppers if m <= LANES]
    for step in range(total // block):
        rows = pl.ds(step * block, block)
        document_col = document_ids((block, 1), 0, me | 1, own_rows, masks) if step == 0 else None
        at = lax.broadcasted_iota(jnp.int32, (block, 1), 0) + step * block
        shift = own_rows.bit_length() - 1
        piece = at >> shift
        device = (me | 1) ^ (piece & 1)
        for s, mask in enumerate(masks):
            device = device ^ (((piece >> (1 + s)) & 1) * mask)
        document_col = (device * own_rows + (at & (own_rows - 1))).astype(jnp.float32)
        id_col = jnp.where(lead, col_ref[rows, count:count + 1], document_col)
        hit = id_col == id_row
        for k, s in enumerate(prefix_scores(v_ref, w_ref, rows, uppers)):
            score_ref[k] = s
        running = None
        stack = []
        for k in reversed(range(count)):
            gain = scales[k] * LOG2E
            total_col = zero_or(lead, col_ref[rows, k:k + 1])
            weight = jnp.exp2(score_ref[k] * gain - total_col - total_rows[k])
            weight = weight - jnp.where(hit, scales[k], 0.0)
            running = weight if running is None else running + weight
            band = running.astype(jnp.bfloat16)
            if k >= len(narrow):
                lower, upper = uppers[k - 1], uppers[k]
                product = jnp.dot(band, w_ref[:, lower:upper], preferred_element_type=jnp.float32)
                store(out_refs, product, step * block, lower, upper, chip_rows)
            else:
                stack.append(band)
        product = jnp.dot(
            jnp.concatenate(stack, axis=0), w_ref[:, :LANES], preferred_element_type=jnp.float32)
        lane = lax.broadcasted_iota(jnp.int32, (block, LANES), 1)
        chosen = product[:block]
        for at_stack in range(1, len(stack)):
            k = len(narrow) - 1 - at_stack
            chosen = jnp.where(
                lane < uppers[k], product[at_stack * block:(at_stack + 1) * block], chosen)
        store(out_refs, chosen, step * block, 0, LANES, chip_rows)


def store(out_refs, value, first_row, lower, upper, chip_rows):
    for at in range(0, value.shape[0], chip_rows):
        ref = out_refs[(first_row + at) // chip_rows]
        ref[:, lower:upper] = value[at:at + chip_rows].astype(ref.dtype)


def on_device(queries, documents, partner):
    own_rows, feature_dim = queries.shape
    uppers = width_list(feature_dim)
    dp_size, rep_size = lax.axis_size("dp"), lax.axis_size("rep")
    devices = dp_size * rep_size
    bits = devices.bit_length() - 1
    assert rep_size == 2 and devices == 1 << bits and bits % 2 == 1
    stages = (bits - 1) // 2
    groups = 1 << stages
    pieces = 2 * groups
    query_masks = [1 << (2 * s + 1) for s in range(stages)]
    document_masks = [1 << (2 * s + 2) for s in range(stages)]
    total = pieces * own_rows
    chip_rows = 2 * own_rows

    role = lax.axis_index("rep")
    me = (lax.axis_index("dp") * rep_size + role).astype(jnp.int32).reshape(1)
    lead = role == 0

    def exchange(x, masks_of):
        return lax.ppermute(x, AXES, [(i, i ^ masks_of(i)) for i in range(devices)])

    def swap(x):
        return exchange(x, lambda i: 1)

    def along(x, stage):
        return exchange(x, lambda i: document_masks[stage] if i & 1 else query_masks[stage])

    mine = jnp.where(lead, queries, documents)
    other = jnp.where(lead, documents, queries)
    v = {(0, 0): mine, (0, 1): swap(other)}
    w = {(0, 0): swap(mine), (0, 1): other}
    for stage in reversed(range(stages)):
        for j in [j for j in range(groups) if (j, 0) in v]:
            for t in range(2):
                v[j | 1 << stage, t] = along(v[j, t], stage)
    for key in sorted(v):
        if key[0]:
            w[key] = swap(v[key])
    order = [(j, t) for j in range(groups) for t in range(2)]
    v_list, w_list = [v[key] for key in order], [w[key] for key in order]

    own_partner = partner.astype(jnp.float32).reshape(1, own_rows)
    far_partner = swap(own_partner)
    chip_partner = jnp.where(
        lead,
        jnp.concatenate([own_partner, far_partner], axis=1),
        jnp.concatenate([far_partner, own_partner], axis=1))

    vmem = pl.BlockSpec(memory_space=pltpu.VMEM)
    smem = pl.BlockSpec(memory_space=pltpu.SMEM)
    limit = 60 << 20
    stats = pl.pallas_call(
        functools.partial(stats_kernel, pieces, uppers),
        out_shape=jax.ShapeDtypeStruct((STATS, total), jnp.float32),
        in_specs=[smem] + [vmem] * (1 + 2 * pieces),
        out_specs=vmem,
        scratch_shapes=[
            pltpu.VMEM((total, feature_dim), jnp.bfloat16),
            pltpu.VMEM((total, feature_dim), jnp.bfloat16),
            pltpu.VMEM((total, LANES), jnp.float32),
        ],
        compiler_params=pltpu.CompilerParams(vmem_limit_bytes=limit),
        cost_estimate=pl.CostEstimate(
            flops=2 * total * total * feature_dim, transcendentals=WIDTHS * total * total,
            bytes_accessed=4 * total * feature_dim),
        name="tile_stats",
    )(role.astype(jnp.int32).reshape(1), chip_partner, *v_list, *w_list)

    def query_mask(j):
        return sum(mask for s, mask in enumerate(query_masks) if j >> s & 1)

    stat_list = [stats] + [exchange(stats, lambda i: query_mask(j)) for j in range(1, groups)]

    partial = pl.pallas_call(
        functools.partial(grads_kernel, pieces, uppers, own_rows, document_masks),
        out_shape=[
            jax.ShapeDtypeStruct((chip_rows, feature_dim), jnp.bfloat16 if j & 1 else jnp.float32)
            for j in range(groups)],
        in_specs=[smem] + [vmem] * (groups + 2 * pieces),
        out_specs=[vmem] * groups,
        scratch_shapes=[
            pltpu.VMEM((total, feature_dim), jnp.bfloat16),
            pltpu.VMEM((total, feature_dim), jnp.bfloat16),
            pltpu.VMEM((WIDTHS, block_of(total), total), jnp.float32),
            pltpu.VMEM((total, LANES), jnp.float32),
        ],
        compiler_params=pltpu.CompilerParams(vmem_limit_bytes=limit),
        cost_estimate=pl.CostEstimate(
            flops=4 * total * total * feature_dim, transcendentals=WIDTHS * total * total,
            bytes_accessed=8 * total * feature_dim),
        name="tile_grads",
    )(me, *stat_list, *v_list, *w_list)
    partial = dict(enumerate(partial))

    for stage in range(stages):
        step = 1 << stage
        for j in sorted([j for j in partial if j & step], reverse=True):
            arrived = along(partial.pop(j).astype(jnp.bfloat16), stage)
            partial[j ^ step] = partial[j ^ step] + arrived.astype(jnp.float32)
    result = partial[0]
    kept, sent = result[:own_rows], result[own_rows:]
    arrived = swap(sent)
    return jnp.where(lead, kept, arrived), jnp.where(lead, arrived, kept)


def solution(mesh):
    return jax.shard_map(
        on_device,
        mesh=mesh,
        in_specs=(P(AXES, None), P(AXES, None), P(AXES)),
        out_specs=(P(AXES, None), P(AXES, None)),
        check_vma=False,
    )
```

```python
import functools
import math

import jax
import jax.numpy as jnp
from jax import lax
from jax.experimental import pallas as pl
from jax.experimental.pallas import tpu as pltpu
from jax.sharding import PartitionSpec as P

WIDTHS = 9
AXES = ("dp", "rep")
LOG2E = 1.4426950408889634
LN2 = 0.6931471805599453
STATS = 16
LANES = 128


logit_gain = 3.0


def width_list(feature_dim):
    return [feature_dim >> WIDTHS - 1 - nested for nested in range(WIDTHS)]


def transposed_dot(a, b):
    return lax.dot_general(a, b, (((1,), (1,)), ((), ())), preferred_element_type=jnp.float32)


def prefix_scores(v_ref, w_ref, rows, uppers):
    narrow = [m for m in uppers if m <= LANES]
    count = rows.size
    head = v_ref[rows, :LANES]
    lane = lax.broadcasted_iota(jnp.int32, head.shape, 1)
    masked = [jnp.where(lane < m, head, jnp.zeros_like(head)) for m in narrow]
    stacked = transposed_dot(jnp.concatenate(masked, axis=0), w_ref[:, :LANES])
    result = [stacked[k * count:(k + 1) * count] for k in range(len(narrow))]
    lower = narrow[-1]
    for upper in uppers[len(narrow):]:
        part = transposed_dot(v_ref[rows, lower:upper], w_ref[:, lower:upper])
        result.append(result[-1] + part)
        lower = upper
    return result


def block_of(total):
    return min(total, 256)


def load_tile(refs, scratch):
    at = 0
    for ref in refs:
        scratch[at:at + ref.shape[0], :] = ref[...]
        at += ref.shape[0]


def stats_kernel(pieces, uppers, *refs):
    role_ref, partner_ref = refs[:2]
    v_refs, w_refs = refs[2:2 + pieces], refs[2 + pieces:2 + 2 * pieces]
    out_ref, v_ref, w_ref, col_ref = refs[2 + 2 * pieces:]
    load_tile(v_refs, v_ref)
    load_tile(w_refs, w_ref)
    total = v_ref.shape[0]
    block = block_of(total)
    steps = total // block
    gains = [logit_gain * m ** -0.5 * LOG2E for m in uppers]
    own = partner_ref.shape[1]
    out_ref[...] = jnp.zeros_like(out_ref)

    @pl.when((role_ref[0] & 1) == 0)
    def _():
        for step in range(steps):
            rows = pl.ds(step * block, block)
            col_ref[rows, :] = jnp.zeros((block, LANES), jnp.float32)
            for k, s in enumerate(prefix_scores(v_ref, w_ref, rows, uppers)):
                logits = s * gains[k]
                peak = jnp.max(logits, axis=1, keepdims=True)
                mass = jnp.sum(jnp.exp2(logits - peak), axis=1, keepdims=True)
                col_ref[rows, k:k + 1] = peak + jnp.log(mass) * LOG2E
        out_ref[...] = col_ref[...].T[:STATS]

    @pl.when((role_ref[0] & 1) != 0)
    def _():
        peaks, masses = [None] * len(uppers), [None] * len(uppers)
        for step in range(steps):
            rows = pl.ds(step * block, block)
            for k, s in enumerate(prefix_scores(v_ref, w_ref, rows, uppers)):
                logits = s * gains[k]
                peak = jnp.max(logits, axis=0, keepdims=True)
                mass = jnp.sum(jnp.exp2(logits - peak), axis=0, keepdims=True)
                if step:
                    top = jnp.maximum(peak, peaks[k])
                    mass = mass * jnp.exp2(peak - top) + masses[k] * jnp.exp2(peaks[k] - top)
                    peak = top
                peaks[k], masses[k] = peak, mass
        for k in range(len(uppers)):
            out_ref[k:k + 1, :] = peaks[k] + jnp.log(masses[k]) * LOG2E

    out_ref[len(uppers):len(uppers) + 1, :own] = partner_ref[...]


def document_ids(shape, axis, first, own_rows, masks, start=0):
    at = lax.broadcasted_iota(jnp.int32, shape, axis) + start
    shift = own_rows.bit_length() - 1
    piece = at >> shift
    device = first ^ (piece & 1)
    for s, mask in enumerate(masks):
        device = device ^ (((piece >> (1 + s)) & 1) * mask)
    return (device * own_rows + (at & (own_rows - 1))).astype(jnp.float32)


def grads_kernel(pieces, uppers, own_rows, masks, *refs):
    me_ref = refs[0]
    groups = pieces // 2
    stat_refs = refs[1:1 + groups]
    v_refs = refs[1 + groups:1 + groups + pieces]
    w_refs = refs[1 + groups + pieces:1 + groups + 2 * pieces]
    out_refs = refs[1 + groups + 2 * pieces:1 + 2 * groups + 2 * pieces]
    v_ref, w_ref, score_ref, col_ref = refs[1 + 2 * groups + 2 * pieces:]
    load_tile(v_refs, v_ref)
    load_tile(w_refs, w_ref)
    total = v_ref.shape[0]
    block = block_of(total)
    chip_rows = total // groups
    count = len(uppers)
    scales = [logit_gain * m ** -0.5 for m in uppers]
    me = me_ref[0]
    lead = (me & 1) == 0

    parts = []
    partners = []
    for j, ref in enumerate(stat_refs):
        parts.append(jnp.concatenate(
            [ref[:, (i ^ j) * chip_rows:((i ^ j) + 1) * chip_rows] for i in range(groups)], axis=1))
        partners.append(ref[count:count + 1, :chip_rows])
    peak = functools.reduce(jnp.maximum, parts)
    mass = functools.reduce(lambda a, b: a + b, [jnp.exp2(part - peak) for part in parts])
    totals = peak + jnp.log(mass) * LOG2E
    partner_row = jnp.concatenate(partners, axis=1)
    packed = jnp.concatenate(
        [totals[:count], partner_row, jnp.zeros((LANES - count - 1, total), jnp.float32)], axis=0)
    col_ref[...] = packed.T
    zero_or = lambda keep, x: jnp.where(keep, x, jnp.zeros_like(x))
    document_row = document_ids((1, total), 1, me | 1, own_rows, masks)
    id_row = jnp.where(lead, document_row, partner_row)
    shifts = [math.log2(s) for s in scales]
    total_rows = [zero_or(jnp.logical_not(lead), totals[k:k + 1]) - shifts[k] for k in range(count)]

    narrow = [m for m in uppers if m <= LANES]
    for step in range(total // block):
        rows = pl.ds(step * block, block)
        document_col = document_ids((block, 1), 0, me | 1, own_rows, masks, step * block)
        id_col = jnp.where(lead, col_ref[rows, count:count + 1], document_col)
        hit = id_col == id_row
        for k, s in enumerate(prefix_scores(v_ref, w_ref, rows, uppers)):
            score_ref[k] = s
        running = None
        stack = []
        for k in reversed(range(count)):
            gain = scales[k] * LOG2E
            total_col = zero_or(lead, col_ref[rows, k:k + 1])
            weight = jnp.exp2(score_ref[k] * gain - total_col - total_rows[k])
            weight = weight - jnp.where(hit, scales[k], 0.0)
            running = weight if running is None else running + weight
            band = running.astype(jnp.bfloat16)
            if k >= len(narrow):
                lower, upper = uppers[k - 1], uppers[k]
                product = jnp.dot(band, w_ref[:, lower:upper], preferred_element_type=jnp.float32)
                store(out_refs, product, step * block, lower, upper, chip_rows)
            else:
                stack.append(band)
        product = jnp.dot(
            jnp.concatenate(stack, axis=0), w_ref[:, :LANES], preferred_element_type=jnp.float32)
        lane = lax.broadcasted_iota(jnp.int32, (block, LANES), 1)
        chosen = product[:block]
        for at_stack in range(1, len(stack)):
            k = len(narrow) - 1 - at_stack
            chosen = jnp.where(
                lane < uppers[k], product[at_stack * block:(at_stack + 1) * block], chosen)
        store(out_refs, chosen, step * block, 0, LANES, chip_rows)


def rows_of(refs, lower, upper):
    return jnp.concatenate([ref[:, lower:upper] for ref in refs], axis=0)


def quadrant_scores(v_refs, w_refs, uppers):
    narrow = [m for m in uppers if m <= LANES]
    head = rows_of(v_refs, 0, LANES)
    count = head.shape[0]
    lane = lax.broadcasted_iota(jnp.int32, head.shape, 1)
    masked = [jnp.where(lane < m, head, jnp.zeros_like(head)) for m in narrow]
    stacked = transposed_dot(jnp.concatenate(masked, axis=0), rows_of(w_refs, 0, LANES))
    for k in range(len(narrow)):
        yield stacked[k * count:(k + 1) * count]
    lower, running = narrow[-1], stacked[-count:]
    for upper in uppers[len(narrow):]:
        running = running + transposed_dot(
            rows_of(v_refs, lower, upper), rows_of(w_refs, lower, upper))
        yield running
        lower = upper


def quadrant(lead, v_refs, w_refs, uppers, refs):
    power_ref, col_peak, col_mass, row_peak, row_mass = refs
    gains = [logit_gain * m ** -0.5 * LOG2E for m in uppers]
    half = power_ref.shape[1]

    @pl.when(lead)
    def _():
        lane = lax.broadcasted_iota(jnp.int32, (half, LANES), 1)
        peaks = jnp.zeros((half, LANES), jnp.float32)
        masses = jnp.ones((half, LANES), jnp.float32)
        for k, s in enumerate(quadrant_scores(v_refs, w_refs, uppers)):
            logits = s * gains[k]
            peak = jnp.max(logits, axis=1, keepdims=True)
            power = jnp.exp2(logits - peak)
            power_ref[k] = power
            peaks = jnp.where(lane == k, peak, peaks)
            masses = jnp.where(lane == k, jnp.sum(power, axis=1, keepdims=True), masses)
        col_peak[...] = peaks
        col_mass[...] = masses

    @pl.when(jnp.logical_not(lead))
    def _():
        row_peak[...] = jnp.zeros_like(row_peak)
        row_mass[...] = jnp.ones_like(row_mass)
        for k, s in enumerate(quadrant_scores(v_refs, w_refs, uppers)):
            logits = s * gains[k]
            peak = jnp.max(logits, axis=0, keepdims=True)
            power = jnp.exp2(logits - peak)
            power_ref[k] = power
            row_peak[k:k + 1, :] = peak
            row_mass[k:k + 1, :] = jnp.sum(power, axis=0, keepdims=True)


def first_kernel(half_pieces, uppers, *refs):
    role_ref, partner_ref = refs[:2]
    v_refs, w_refs = refs[2:2 + half_pieces], refs[2 + half_pieces:2 + 2 * half_pieces]
    outs = refs[2 + 2 * half_pieces:]
    quadrant((role_ref[0] & 1) == 0, v_refs, w_refs, uppers, outs[:5])
    outs[5][...] = partner_ref[...]


def log_sum(peak_a, mass_a, peak_b, mass_b):
    top = jnp.maximum(peak_a, peak_b)
    return top + jnp.log(
        mass_a * jnp.exp2(peak_a - top) + mass_b * jnp.exp2(peak_b - top)) * LOG2E


def second_kernel(half_pieces, uppers, *refs):
    role_ref, partner_ref = refs[:2]
    first = refs[2:6]
    at = 6 + 2 * half_pieces
    v_refs, w_refs = refs[6:at], refs[at:at + 2 * half_pieces]
    outs = refs[at + 2 * half_pieces:]
    q12, q21, q22, stats_ref = outs[:5], outs[5:10], outs[10:15], outs[15]
    lead = (role_ref[0] & 1) == 0
    v_low, v_high = v_refs[:half_pieces], v_refs[half_pieces:]
    w_low, w_high = w_refs[:half_pieces], w_refs[half_pieces:]
    quadrant(lead, v_low, w_high, uppers, q12)
    quadrant(lead, v_high, w_low, uppers, q21)
    quadrant(lead, v_high, w_high, uppers, q22)

    @pl.when(lead)
    def _():
        low = log_sum(first[0][...], first[1][...], q12[1][...], q12[2][...])
        high = log_sum(q21[1][...], q21[2][...], q22[1][...], q22[2][...])
        stats_ref[...] = jnp.concatenate([low, high], axis=0).T[:STATS]

    @pl.when(jnp.logical_not(lead))
    def _():
        low = log_sum(first[2][...], first[3][...], q21[3][...], q21[4][...])
        high = log_sum(q12[3][...], q12[4][...], q22[3][...], q22[4][...])
        stats_ref[...] = jnp.concatenate([low, high], axis=1)

    count = len(uppers)
    stats_ref[count:count + 1, :partner_ref.shape[1]] = partner_ref[...]


def band_kernel(groups, uppers, widths, own_rows, masks, follows, *refs):
    me_ref = refs[0]
    stat_refs = refs[1:1 + groups]
    at = 1 + groups
    power_refs = refs[at:at + 4]
    col_refs, row_refs = refs[at + 4:at + 8], refs[at + 8:at + 12]
    at += 12
    w_refs = refs[at:at + 2 * groups]
    at += 2 * groups
    before_ref = None
    if follows:
        before_ref, at = refs[at], at + 1
    out_refs = refs[at:at + groups]
    at += groups
    after_ref = None
    if not follows:
        after_ref, at = refs[at], at + 1
    w_ref, = refs[at:]
    base = 0 if widths[-1] == 0 else uppers[widths[-1] - 1]
    top = uppers[widths[0]]
    for i, ref in enumerate(w_refs):
        w_ref[i * own_rows:(i + 1) * own_rows, :] = ref[:, base:top]

    total = w_ref.shape[0]
    half = total // 2
    chip_rows = total // groups
    count = len(uppers)
    scales = [logit_gain * m ** -0.5 for m in uppers]
    me = me_ref[0]
    lead = (me & 1) == 0
    parts, partners = [], []
    for j, ref in enumerate(stat_refs):
        parts.append(jnp.concatenate(
            [ref[:, (i ^ j) * chip_rows:((i ^ j) + 1) * chip_rows] for i in range(groups)], axis=1))
        partners.append(ref[count:count + 1, :chip_rows])
    peak = functools.reduce(jnp.maximum, parts)
    mass = functools.reduce(lambda a, b: a + b, [jnp.exp2(part - peak) for part in parts])
    partner_row = jnp.concatenate(partners, axis=1)
    sub = lax.broadcasted_iota(jnp.int32, (STATS, total), 0)
    totals = peak + jnp.log(mass) * LOG2E
    for k in range(count):
        totals = jnp.where(sub == k, totals - math.log2(scales[k]), totals)
    packed = jnp.concatenate(
        [totals[:count], partner_row, jnp.zeros((LANES - count - 1, total), jnp.float32)], axis=0)
    cols = packed.T
    id_row = jnp.where(
        lead, document_ids((1, total), 1, me | 1, own_rows, masks), partner_row)
    id_col = jnp.where(
        lead, cols[:, count:count + 1],
        document_ids((total, 1), 0, me | 1, own_rows, masks))

    narrow = [k for k in widths if uppers[k] <= LANES]
    for high in (1, 0):
        rows = slice(high * half, (high + 1) * half)
        hit = id_col[rows] == id_row
        col_gain, row_gain = [], []
        for right in (0, 1):
            q = 2 * high + right
            across = slice(right * half, (right + 1) * half)
            col_gain.append(jnp.where(lead, jnp.exp2(col_refs[q][...] - cols[rows]), 1.0))
            row_gain.append(jnp.where(lead, 1.0, jnp.exp2(row_refs[q][...] - totals[:, across])))
        running = before_ref[rows, :] if follows else None
        stack = []
        for k in widths:
            weight = jnp.concatenate([
                power_refs[2 * high + right][k]
                * col_gain[right][:, k:k + 1] * row_gain[right][k:k + 1, :]
                for right in (0, 1)], axis=1)
            weight = weight - jnp.where(hit, scales[k], 0.0)
            running = weight if running is None else running + weight
            band = running.astype(jnp.bfloat16)
            if k not in narrow:
                lower, upper = uppers[k - 1] - base, uppers[k] - base
                product = jnp.dot(band, w_ref[:, lower:upper], preferred_element_type=jnp.float32)
                store(out_refs, product, high * half, lower, upper, chip_rows)
            else:
                stack.append(band)
        if not follows:
            after_ref[rows, :] = running
        if narrow:
            product = jnp.dot(
                jnp.concatenate(stack, axis=0), w_ref[:, :LANES],
                preferred_element_type=jnp.float32)
            lane = lax.broadcasted_iota(jnp.int32, (half, LANES), 1)
            chosen = product[:half]
            for i in range(1, len(stack)):
                chosen = jnp.where(lane < uppers[narrow[i]], product[i * half:(i + 1) * half], chosen)
            store(out_refs, chosen, high * half, 0, LANES, chip_rows)


def store(out_refs, value, first_row, lower, upper, chip_rows):
    for at in range(0, value.shape[0], chip_rows):
        ref = out_refs[(first_row + at) // chip_rows]
        ref[:, lower:upper] = value[at:at + chip_rows].astype(ref.dtype)


def on_device(queries, documents, partner):
    own_rows, feature_dim = queries.shape
    uppers = width_list(feature_dim)
    dp_size, rep_size = lax.axis_size("dp"), lax.axis_size("rep")
    devices = dp_size * rep_size
    bits = devices.bit_length() - 1
    assert rep_size == 2 and devices == 1 << bits and bits % 2 == 1
    stages = (bits - 1) // 2
    groups = 1 << stages
    pieces = 2 * groups
    query_masks = [1 << (2 * s + 1) for s in range(stages)]
    document_masks = [1 << (2 * s + 2) for s in range(stages)]
    total = pieces * own_rows
    chip_rows = 2 * own_rows

    role = lax.axis_index("rep")
    me = (lax.axis_index("dp") * rep_size + role).astype(jnp.int32).reshape(1)
    lead = role == 0

    def exchange(x, masks_of):
        return lax.ppermute(x, AXES, [(i, i ^ masks_of(i)) for i in range(devices)])

    def swap(x):
        return exchange(x, lambda i: 1)

    def along(x, stage):
        return exchange(x, lambda i: document_masks[stage] if i & 1 else query_masks[stage])

    mine = jnp.where(lead, queries, documents)
    other = jnp.where(lead, documents, queries)
    v = {(0, 0): mine, (0, 1): swap(other)}
    w = {(0, 0): swap(mine), (0, 1): other}
    for stage in reversed(range(stages)):
        for j in [j for j in range(groups) if (j, 0) in v]:
            for t in range(2):
                v[j | 1 << stage, t] = along(v[j, t], stage)
    for key in sorted(v):
        if key[0]:
            w[key] = swap(v[key])
    order = [(j, t) for j in range(groups) for t in range(2)]
    v_list, w_list = [v[key] for key in order], [w[key] for key in order]

    own_partner = partner.astype(jnp.float32).reshape(1, own_rows)
    far_partner = swap(own_partner)
    chip_partner = jnp.where(
        lead,
        jnp.concatenate([own_partner, far_partner], axis=1),
        jnp.concatenate([far_partner, own_partner], axis=1))

    vmem = pl.BlockSpec(memory_space=pltpu.VMEM)
    smem = pl.BlockSpec(memory_space=pltpu.SMEM)

    def query_mask(j):
        return sum(mask for s, mask in enumerate(query_masks) if j >> s & 1)

    def gathered(stats):
        return [stats] + [exchange(stats, lambda i: query_mask(j)) for j in range(1, groups)]

    shape = lambda *dims: jax.ShapeDtypeStruct(dims, jnp.float32)

    def gradient_shapes(columns):
        return [
            jax.ShapeDtypeStruct((chip_rows, columns), jnp.bfloat16 if j & 1 else jnp.float32)
            for j in range(groups)]

    if WIDTHS * total * total * 4 > 16 << 20:
        limit = 60 << 20
        stats = pl.pallas_call(
            functools.partial(stats_kernel, pieces, uppers),
            out_shape=shape(STATS, total),
            in_specs=[smem] + [vmem] * (1 + 2 * pieces),
            out_specs=vmem,
            scratch_shapes=[
                pltpu.VMEM((total, feature_dim), jnp.bfloat16),
                pltpu.VMEM((total, feature_dim), jnp.bfloat16),
                pltpu.VMEM((total, LANES), jnp.float32),
            ],
            compiler_params=pltpu.CompilerParams(vmem_limit_bytes=limit),
            name="tile_stats",
        )(me, chip_partner, *v_list, *w_list)
        whole = pl.pallas_call(
            functools.partial(grads_kernel, pieces, uppers, own_rows, document_masks),
            out_shape=gradient_shapes(feature_dim),
            in_specs=[smem] + [vmem] * (groups + 2 * pieces),
            out_specs=[vmem] * groups,
            scratch_shapes=[
                pltpu.VMEM((total, feature_dim), jnp.bfloat16),
                pltpu.VMEM((total, feature_dim), jnp.bfloat16),
                pltpu.VMEM((WIDTHS, block_of(total), total), jnp.float32),
                pltpu.VMEM((total, LANES), jnp.float32),
            ],
            compiler_params=pltpu.CompilerParams(vmem_limit_bytes=limit),
            name="tile_grads",
        )(me, *gathered(stats), *v_list, *w_list)
        chunks = [whole]
    else:
        half = total // 2
        half_pieces = pieces // 2
        quadrant_shapes = [
            shape(WIDTHS, half, half), shape(half, LANES), shape(half, LANES),
            shape(STATS, half), shape(STATS, half)]
        limit = 20 << 20
        params = pltpu.CompilerParams(vmem_limit_bytes=limit)
        work = 2 * half * half * feature_dim
        *q11, chip_partner = pl.pallas_call(
            functools.partial(first_kernel, half_pieces, uppers),
            out_shape=quadrant_shapes + [shape(1, chip_rows)],
            in_specs=[smem] + [vmem] * (1 + 2 * half_pieces),
            out_specs=[vmem] * 6,
            compiler_params=params,
            cost_estimate=pl.CostEstimate(
                flops=3 * work, transcendentals=0, bytes_accessed=2 * total * feature_dim),
            name="first_quadrant",
        )(me, chip_partner, *v_list[:half_pieces], *w_list[:half_pieces])
        *rest, stats = pl.pallas_call(
            functools.partial(second_kernel, half_pieces, uppers),
            out_shape=quadrant_shapes * 3 + [shape(STATS, total)],
            in_specs=[smem] + [vmem] * (5 + 2 * pieces),
            out_specs=[vmem] * 16,
            compiler_params=params,
            cost_estimate=pl.CostEstimate(
                flops=9 * work, transcendentals=0, bytes_accessed=4 * total * feature_dim),
            name="other_quadrants",
        )(me, chip_partner, *q11[1:], *v_list, *w_list)
        quads = [q11, rest[:5], rest[5:10], rest[10:15]]
        common = [me, *gathered(stats), *[q[0] for q in quads], *[q[1] for q in quads],
                  *[q[3] for q in quads], *w_list]
        last = WIDTHS - 1

        def bands(widths, more, follows, name):
            base = 0 if widths[-1] == 0 else uppers[widths[-1] - 1]
            columns = uppers[widths[0]] - base
            return pl.pallas_call(
                functools.partial(
                    band_kernel, groups, uppers, widths, own_rows, document_masks, follows),
                out_shape=gradient_shapes(columns) + ([] if follows else [shape(total, total)]),
                in_specs=[smem] + [vmem] * (len(common) - 1 + len(more)),
                out_specs=[vmem] * (groups + (not follows)),
                scratch_shapes=[pltpu.VMEM((total, columns), jnp.bfloat16)],
                compiler_params=params,
                cost_estimate=pl.CostEstimate(
                    flops=2 * total * total * feature_dim, transcendentals=0,
                    bytes_accessed=4 * total * feature_dim),
                name=name,
            )(*common, *more)

        *widest, running = bands([last], [], False, "last_band")
        others = bands(list(reversed(range(last))), [running], True, "other_bands")
        chunks = [widest, others]

    mine_parts, other_parts = [], []
    for chunk in chunks:
        partial = dict(enumerate(chunk))
        for stage in range(stages - 1):
            step = 1 << stage
            for j in sorted([j for j in partial if j & step], reverse=True):
                arrived = along(partial.pop(j).astype(jnp.bfloat16), stage)
                partial[j ^ step] = partial[j ^ step] + arrived.astype(jnp.float32)
        stage = stages - 1
        outgoing = partial[1 << stage].astype(jnp.bfloat16)
        far = lambda i: document_masks[stage] ^ 1 if i & 1 else query_masks[stage] ^ 1
        near_arrived = along(outgoing[:own_rows], stage)
        far_arrived = exchange(outgoing[own_rows:], far)
        kept = partial[0]
        mine_parts.append(kept[:own_rows] + near_arrived.astype(jnp.float32))
        other_parts.append(swap(kept[own_rows:]) + far_arrived.astype(jnp.float32))
    mine_parts, other_parts = mine_parts[::-1], other_parts[::-1]
    ours = jnp.concatenate(mine_parts, axis=1)
    theirs = jnp.concatenate(other_parts, axis=1)
    return jnp.where(lead, ours, theirs), jnp.where(lead, theirs, ours)


def solution(mesh):
    return jax.shard_map(
        on_device,
        mesh=mesh,
        in_specs=(P(AXES, None), P(AXES, None), P(AXES)),
        out_specs=(P(AXES, None), P(AXES, None)),
        check_vma=False,
    )
```

```python
import functools
import math

import jax
import jax.numpy as jnp
from jax import lax
from jax.experimental import pallas as pl
from jax.experimental.pallas import tpu as pltpu
from jax.sharding import PartitionSpec as P


WIDTHS = 9
AXES = ("dp", "rep")
LOG2E = 1.4426950408889634
STATS = 16
LANES = 128


logit_gain = 3.0


def width_list(feature_dim):
    return [feature_dim >> WIDTHS - 1 - nested for nested in range(WIDTHS)]


def transposed_dot(a, b):
    return lax.dot_general(a, b, (((1,), (1,)), ((), ())), preferred_element_type=jnp.float32)


def prefix_scores(v_ref, w_ref, rows, uppers):
    narrow = [m for m in uppers if m <= LANES]
    count = rows.size
    head = v_ref[rows, :LANES]
    lane = lax.broadcasted_iota(jnp.int32, head.shape, 1)
    masked = [jnp.where(lane < m, head, jnp.zeros_like(head)) for m in narrow]
    stacked = transposed_dot(jnp.concatenate(masked, axis=0), w_ref[:, :LANES])
    result = [stacked[k * count:(k + 1) * count] for k in range(len(narrow))]
    lower = narrow[-1]
    for upper in uppers[len(narrow):]:
        part = transposed_dot(v_ref[rows, lower:upper], w_ref[:, lower:upper])
        result.append(result[-1] + part)
        lower = upper
    return result


def block_of(total):
    return min(total, 256)


def load_tile(refs, scratch):
    at = 0
    for ref in refs:
        scratch[at:at + ref.shape[0], :] = ref[...]
        at += ref.shape[0]


def stats_kernel(pieces, uppers, *refs):
    role_ref, partner_ref = refs[:2]
    v_refs, w_refs = refs[2:2 + pieces], refs[2 + pieces:2 + 2 * pieces]
    out_ref, v_ref, w_ref, col_ref = refs[2 + 2 * pieces:]
    load_tile(v_refs, v_ref)
    load_tile(w_refs, w_ref)
    total = v_ref.shape[0]
    block = block_of(total)
    steps = total // block
    gains = [logit_gain * m ** -0.5 * LOG2E for m in uppers]
    own = partner_ref.shape[1]
    out_ref[...] = jnp.zeros_like(out_ref)

    @pl.when((role_ref[0] & 1) == 0)
    def _():
        for step in range(steps):
            rows = pl.ds(step * block, block)
            col_ref[rows, :] = jnp.zeros((block, LANES), jnp.float32)
            for k, s in enumerate(prefix_scores(v_ref, w_ref, rows, uppers)):
                logits = s * gains[k]
                peak = jnp.max(logits, axis=1, keepdims=True)
                mass = jnp.sum(jnp.exp2(logits - peak), axis=1, keepdims=True)
                col_ref[rows, k:k + 1] = peak + jnp.log(mass) * LOG2E
        out_ref[...] = col_ref[...].T[:STATS]

    @pl.when((role_ref[0] & 1) != 0)
    def _():
        peaks, masses = [None] * len(uppers), [None] * len(uppers)
        for step in range(steps):
            rows = pl.ds(step * block, block)
            for k, s in enumerate(prefix_scores(v_ref, w_ref, rows, uppers)):
                logits = s * gains[k]
                peak = jnp.max(logits, axis=0, keepdims=True)
                mass = jnp.sum(jnp.exp2(logits - peak), axis=0, keepdims=True)
                if step:
                    top = jnp.maximum(peak, peaks[k])
                    mass = mass * jnp.exp2(peak - top) + masses[k] * jnp.exp2(peaks[k] - top)
                    peak = top
                peaks[k], masses[k] = peak, mass
        for k in range(len(uppers)):
            out_ref[k:k + 1, :] = peaks[k] + jnp.log(masses[k]) * LOG2E

    out_ref[len(uppers):len(uppers) + 1, :own] = partner_ref[...]


def document_ids(shape, axis, first, own_rows, masks, start=0):
    at = lax.broadcasted_iota(jnp.int32, shape, axis) + start
    shift = own_rows.bit_length() - 1
    piece = at >> shift
    device = first ^ (piece & 1)
    for s, mask in enumerate(masks):
        device = device ^ (((piece >> (1 + s)) & 1) * mask)
    return (device * own_rows + (at & (own_rows - 1))).astype(jnp.float32)


def grads_kernel(pieces, uppers, own_rows, masks, *refs):
    me_ref = refs[0]
    groups = pieces // 2
    stat_refs = refs[1:1 + groups]
    v_refs = refs[1 + groups:1 + groups + pieces]
    w_refs = refs[1 + groups + pieces:1 + groups + 2 * pieces]
    out_refs = refs[1 + groups + 2 * pieces:1 + 2 * groups + 2 * pieces]
    v_ref, w_ref, score_ref, col_ref = refs[1 + 2 * groups + 2 * pieces:]
    load_tile(v_refs, v_ref)
    load_tile(w_refs, w_ref)
    total = v_ref.shape[0]
    block = block_of(total)
    chip_rows = total // groups
    count = len(uppers)
    scales = [logit_gain * m ** -0.5 for m in uppers]
    me = me_ref[0]
    lead = (me & 1) == 0

    parts = []
    partners = []
    for j, ref in enumerate(stat_refs):
        parts.append(jnp.concatenate(
            [ref[:, (i ^ j) * chip_rows:((i ^ j) + 1) * chip_rows] for i in range(groups)], axis=1))
        partners.append(ref[count:count + 1, :chip_rows])
    peak = functools.reduce(jnp.maximum, parts)
    mass = functools.reduce(lambda a, b: a + b, [jnp.exp2(part - peak) for part in parts])
    totals = peak + jnp.log(mass) * LOG2E
    partner_row = jnp.concatenate(partners, axis=1)
    packed = jnp.concatenate(
        [totals[:count], partner_row, jnp.zeros((LANES - count - 1, total), jnp.float32)], axis=0)
    col_ref[...] = packed.T
    zero_or = lambda keep, x: jnp.where(keep, x, jnp.zeros_like(x))
    document_row = document_ids((1, total), 1, me | 1, own_rows, masks)
    id_row = jnp.where(lead, document_row, partner_row)
    shifts = [math.log2(s) for s in scales]
    total_rows = [zero_or(jnp.logical_not(lead), totals[k:k + 1]) - shifts[k] for k in range(count)]

    narrow = [m for m in uppers if m <= LANES]
    for step in range(total // block):
        rows = pl.ds(step * block, block)
        document_col = document_ids((block, 1), 0, me | 1, own_rows, masks, step * block)
        id_col = jnp.where(lead, col_ref[rows, count:count + 1], document_col)
        hit = id_col == id_row
        for k, s in enumerate(prefix_scores(v_ref, w_ref, rows, uppers)):
            score_ref[k] = s
        running = None
        stack = []
        for k in reversed(range(count)):
            gain = scales[k] * LOG2E
            total_col = zero_or(lead, col_ref[rows, k:k + 1])
            weight = jnp.exp2(score_ref[k] * gain - total_col - total_rows[k])
            weight = weight - jnp.where(hit, scales[k], 0.0)
            running = weight if running is None else running + weight
            band = running.astype(jnp.bfloat16)
            if k >= len(narrow):
                lower, upper = uppers[k - 1], uppers[k]
                product = jnp.dot(band, w_ref[:, lower:upper], preferred_element_type=jnp.float32)
                store(out_refs, product, step * block, lower, upper, chip_rows)
            else:
                stack.append(band)
        product = jnp.dot(
            jnp.concatenate(stack, axis=0), w_ref[:, :LANES], preferred_element_type=jnp.float32)
        lane = lax.broadcasted_iota(jnp.int32, (block, LANES), 1)
        chosen = product[:block]
        for at_stack in range(1, len(stack)):
            k = len(narrow) - 1 - at_stack
            chosen = jnp.where(
                lane < uppers[k], product[at_stack * block:(at_stack + 1) * block], chosen)
        store(out_refs, chosen, step * block, 0, LANES, chip_rows)


def rows_of(refs, lower, upper):
    return jnp.concatenate([ref[:, lower:upper] for ref in refs], axis=0)


def subtile_scores(v_refs, w_refs, uppers):
    narrow = [m for m in uppers if m <= LANES]
    head = rows_of(v_refs, 0, LANES)
    count = head.shape[0]
    lane = lax.broadcasted_iota(jnp.int32, head.shape, 1)
    masked = [jnp.where(lane < m, head, jnp.zeros_like(head)) for m in narrow]
    stacked = transposed_dot(jnp.concatenate(masked, axis=0), rows_of(w_refs, 0, LANES))
    for k in range(len(narrow)):
        yield stacked[k * count:(k + 1) * count]
    lower, running = narrow[-1], stacked[-count:]
    for upper in uppers[len(narrow):]:
        running = running + transposed_dot(
            rows_of(v_refs, lower, upper), rows_of(w_refs, lower, upper))
        yield running
        lower = upper


def subtile(lead, v_refs, w_refs, uppers, refs):
    power_ref, col_peak, col_mass, row_peak, row_mass = refs
    gains = [logit_gain * m ** -0.5 * LOG2E for m in uppers]
    count = power_ref.shape[1]

    @pl.when(lead)
    def _():
        lane = lax.broadcasted_iota(jnp.int32, (count, LANES), 1)
        peaks = jnp.zeros((count, LANES), jnp.float32)
        masses = jnp.ones((count, LANES), jnp.float32)
        for k, s in enumerate(subtile_scores(v_refs, w_refs, uppers)):
            logits = s * gains[k]
            peak = jnp.max(logits, axis=1, keepdims=True)
            power = jnp.exp2(logits - peak)
            power_ref[k] = power
            peaks = jnp.where(lane == k, peak, peaks)
            masses = jnp.where(lane == k, jnp.sum(power, axis=1, keepdims=True), masses)
        col_peak[...] = peaks
        col_mass[...] = masses

    @pl.when(jnp.logical_not(lead))
    def _():
        row_peak[...] = jnp.zeros_like(row_peak)
        row_mass[...] = jnp.ones_like(row_mass)
        for k, s in enumerate(subtile_scores(v_refs, w_refs, uppers)):
            logits = s * gains[k]
            peak = jnp.max(logits, axis=0, keepdims=True)
            power = jnp.exp2(logits - peak)
            power_ref[k] = power
            row_peak[k:k + 1, :] = peak
            row_mass[k:k + 1, :] = jnp.sum(power, axis=0, keepdims=True)


def log_sum(pairs):
    top = functools.reduce(jnp.maximum, [peak for peak, _ in pairs])
    mass = functools.reduce(
        lambda a, b: a + b, [mass * jnp.exp2(peak - top) for peak, mass in pairs])
    return top + jnp.log(mass) * LOG2E


def tile_kernel(tiles, uppers, own_rows, pieces, finish, *refs):
    me_ref, partner_ref = refs[:2]
    v_refs, w_refs = refs[2:2 + pieces], refs[2 + pieces:2 + 2 * pieces]
    at = 2 + 2 * pieces
    earlier = refs[at:at + 4 * finish]
    outs = refs[at + 4 * finish:]
    lead = (me_ref[0] & 1) == 0
    for i, (r0, r1, c0, c1) in enumerate(tiles):
        subtile(
            lead, v_refs[2 * r0:2 * r1], w_refs[2 * c0:2 * c1], uppers, outs[5 * i:5 * i + 5])
    if not finish:
        outs[-1][...] = partner_ref[...]
        return
    stats_ref = outs[-1]
    every = [earlier[4 * i:4 * i + 4] for i in range(finish)]
    every += [outs[5 * i + 1:5 * i + 5] for i in range(len(tiles))]
    shapes = subtiles(pieces // 2)
    segments = segments_of(pieces // 2)
    chip_rows = 2 * own_rows

    @pl.when(lead)
    def _():
        merged = []
        for s0, s1 in segments:
            pairs = []
            for (r0, r1, _, _), tile in zip(shapes, every):
                if r0 <= s0 and s1 <= r1:
                    rows = slice((s0 - r0) * chip_rows, (s1 - r0) * chip_rows)
                    pairs.append((tile[0][rows, :], tile[1][rows, :]))
            merged.append(log_sum(pairs))
        stats_ref[...] = jnp.concatenate(merged, axis=0).T[:STATS]

    @pl.when(jnp.logical_not(lead))
    def _():
        for s0, s1 in segments:
            pairs = []
            for (_, _, c0, c1), tile in zip(shapes, every):
                if c0 <= s0 and s1 <= c1:
                    across = slice((s0 - c0) * chip_rows, (s1 - c0) * chip_rows)
                    pairs.append((tile[2][:, across], tile[3][:, across]))
            stats_ref[:, s0 * chip_rows:s1 * chip_rows] = log_sum(pairs)

    count = len(uppers)
    stats_ref[count:count + 1, :chip_rows] = partner_ref[...]


def segments_of(groups):
    low, middle = groups // 2, groups // 2 + groups // 4
    return [(0, low), (low, middle), (middle, groups)]


def subtiles(groups):
    (_, low), (_, middle), _ = segments_of(groups)
    return [(0, low, 0, low), (0, low, low, middle), (low, middle, 0, middle),
            (0, middle, middle, groups), (middle, groups, 0, groups)]


def band_kernel(groups, uppers, widths, own_rows, masks, follows, *refs):
    me_ref = refs[0]
    stat_refs = refs[1:1 + groups]
    at = 1 + groups
    shapes = subtiles(groups)
    tiles = len(shapes)
    power_refs, col_refs, row_refs = [refs[at + i * tiles:at + (i + 1) * tiles] for i in range(3)]
    at += 3 * tiles
    w_refs = refs[at:at + 2 * groups]
    at += 2 * groups
    before_ref = None
    if follows:
        before_ref, at = refs[at], at + 1
    out_refs = refs[at:at + groups]
    at += groups
    after_ref = None
    if not follows:
        after_ref, at = refs[at], at + 1
    w_ref, = refs[at:]
    base = 0 if widths[-1] == 0 else uppers[widths[-1] - 1]
    top = uppers[widths[0]]
    for i, ref in enumerate(w_refs):
        w_ref[i * own_rows:(i + 1) * own_rows, :] = ref[:, base:top]

    total = w_ref.shape[0]
    chip_rows = total // groups
    count = len(uppers)
    scales = [logit_gain * m ** -0.5 for m in uppers]
    me = me_ref[0]
    lead = (me & 1) == 0
    parts, partners = [], []
    for j, ref in enumerate(stat_refs):
        parts.append(jnp.concatenate(
            [ref[:, (i ^ j) * chip_rows:((i ^ j) + 1) * chip_rows] for i in range(groups)], axis=1))
        partners.append(ref[count:count + 1, :chip_rows])
    peak = functools.reduce(jnp.maximum, parts)
    mass = functools.reduce(lambda a, b: a + b, [jnp.exp2(part - peak) for part in parts])
    partner_row = jnp.concatenate(partners, axis=1)
    sub = lax.broadcasted_iota(jnp.int32, (STATS, total), 0)
    totals = peak + jnp.log(mass) * LOG2E
    for k in range(count):
        totals = jnp.where(sub == k, totals - math.log2(scales[k]), totals)
    packed = jnp.concatenate(
        [totals[:count], partner_row, jnp.zeros((LANES - count - 1, total), jnp.float32)], axis=0)
    cols = packed.T
    id_row = jnp.where(
        lead, document_ids((1, total), 1, me | 1, own_rows, masks), partner_row)
    id_col = jnp.where(
        lead, cols[:, count:count + 1],
        document_ids((total, 1), 0, me | 1, own_rows, masks))

    segments = segments_of(groups)
    narrow = [k for k in widths if uppers[k] <= LANES]
    for block in (segments[1:], segments[:1]):
        first = block[0][0] * chip_rows
        rows = slice(first, block[-1][1] * chip_rows)
        height = rows.stop - first
        hit = id_col[rows] == id_row
        strips = []
        for s0, s1 in block:
            strip = []
            for (r0, r1, c0, c1), power, col_peak, row_peak in zip(
                    shapes, power_refs, col_refs, row_refs):
                if r0 <= s0 and s1 <= r1:
                    inner = slice((s0 - r0) * chip_rows, (s1 - r0) * chip_rows)
                    outer = slice(s0 * chip_rows, s1 * chip_rows)
                    across = slice(c0 * chip_rows, c1 * chip_rows)
                    strip.append((
                        c0, power, inner,
                        jnp.where(lead, jnp.exp2(col_peak[inner, :] - cols[outer]), 1.0),
                        jnp.where(lead, 1.0, jnp.exp2(row_peak[...] - totals[:, across]))))
            strips.append(sorted(strip, key=lambda item: item[0]))
        running = before_ref[rows, :] if follows else None
        stack = []
        for k in widths:
            weight = jnp.concatenate([
                jnp.concatenate([
                    power[k, inner] * col_gain[:, k:k + 1] * row_gain[k:k + 1, :]
                    for _, power, inner, col_gain, row_gain in strip], axis=1)
                for strip in strips], axis=0)
            weight = weight - jnp.where(hit, scales[k], 0.0)
            running = weight if running is None else running + weight
            band = running.astype(jnp.bfloat16)
            if k not in narrow:
                lower, upper = uppers[k - 1] - base, uppers[k] - base
                product = jnp.dot(band, w_ref[:, lower:upper], preferred_element_type=jnp.float32)
                store(out_refs, product, first, lower, upper, chip_rows)
            else:
                stack.append(band)
        if not follows:
            after_ref[rows, :] = running
        if narrow:
            product = jnp.dot(
                jnp.concatenate(stack, axis=0), w_ref[:, :LANES],
                preferred_element_type=jnp.float32)
            lane = lax.broadcasted_iota(jnp.int32, (height, LANES), 1)
            chosen = product[:height]
            for i in range(1, len(stack)):
                chosen = jnp.where(
                    lane < uppers[narrow[i]], product[i * height:(i + 1) * height], chosen)
            store(out_refs, chosen, first, 0, LANES, chip_rows)


def store(out_refs, value, first_row, lower, upper, chip_rows):
    for at in range(0, value.shape[0], chip_rows):
        ref = out_refs[(first_row + at) // chip_rows]
        ref[:, lower:upper] = value[at:at + chip_rows].astype(ref.dtype)


def on_device(queries, documents, partner):
    own_rows, feature_dim = queries.shape
    uppers = width_list(feature_dim)
    dp_size, rep_size = lax.axis_size("dp"), lax.axis_size("rep")
    devices = dp_size * rep_size
    bits = devices.bit_length() - 1
    assert rep_size == 2 and devices == 1 << bits and bits % 2 == 1
    stages = (bits - 1) // 2
    groups = 1 << stages
    pieces = 2 * groups
    query_masks = [1 << (2 * s + 1) for s in range(stages)]
    document_masks = [1 << (2 * s + 2) for s in range(stages)]
    total = pieces * own_rows
    chip_rows = 2 * own_rows

    role = lax.axis_index("rep")
    me = (lax.axis_index("dp") * rep_size + role).astype(jnp.int32).reshape(1)
    lead = role == 0

    def exchange(x, masks_of):
        return lax.ppermute(x, AXES, [(i, i ^ masks_of(i)) for i in range(devices)])

    def swap(x):
        return exchange(x, lambda i: 1)

    def along(x, stage):
        return exchange(x, lambda i: document_masks[stage] if i & 1 else query_masks[stage])

    mine = jnp.where(lead, queries, documents)
    other = jnp.where(lead, documents, queries)
    v = {(0, 0): mine, (0, 1): swap(other)}
    w = {(0, 0): swap(mine), (0, 1): other}
    for stage in reversed(range(stages)):
        for j in [j for j in range(groups) if (j, 0) in v]:
            for t in range(2):
                v[j | 1 << stage, t] = along(v[j, t], stage)
    for j, t in sorted(v):
        if j:
            w[j, t] = swap(v[j, t])
    order = [(j, t) for j in range(groups) for t in range(2)]
    v_list, w_list = [v[key] for key in order], [w[key] for key in order]

    own_partner = partner.astype(jnp.float32).reshape(1, own_rows)
    far_partner = swap(own_partner)
    chip_partner = jnp.where(
        lead,
        jnp.concatenate([own_partner, far_partner], axis=1),
        jnp.concatenate([far_partner, own_partner], axis=1))

    vmem = pl.BlockSpec(memory_space=pltpu.VMEM)
    smem = pl.BlockSpec(memory_space=pltpu.SMEM)

    def query_mask(j):
        return sum(mask for s, mask in enumerate(query_masks) if j >> s & 1)

    def gathered(stats):
        return [stats] + [exchange(stats, lambda i: query_mask(j)) for j in range(1, groups)]

    shape = lambda *dims: jax.ShapeDtypeStruct(dims, jnp.float32)

    def gradient_shapes(columns):
        return [
            jax.ShapeDtypeStruct((chip_rows, columns), jnp.bfloat16 if j & 1 else jnp.float32)
            for j in range(groups)]

    if WIDTHS * total * total * 4 > 16 << 20:
        limit = 60 << 20
        stats = pl.pallas_call(
            functools.partial(stats_kernel, pieces, uppers),
            out_shape=shape(STATS, total),
            in_specs=[smem] + [vmem] * (1 + 2 * pieces),
            out_specs=vmem,
            scratch_shapes=[
                pltpu.VMEM((total, feature_dim), jnp.bfloat16),
                pltpu.VMEM((total, feature_dim), jnp.bfloat16),
                pltpu.VMEM((total, LANES), jnp.float32),
            ],
            compiler_params=pltpu.CompilerParams(vmem_limit_bytes=limit),
            name="tile_stats",
        )(me, chip_partner, *v_list, *w_list)
        whole = pl.pallas_call(
            functools.partial(grads_kernel, pieces, uppers, own_rows, document_masks),
            out_shape=gradient_shapes(feature_dim),
            in_specs=[smem] + [vmem] * (groups + 2 * pieces),
            out_specs=[vmem] * groups,
            scratch_shapes=[
                pltpu.VMEM((total, feature_dim), jnp.bfloat16),
                pltpu.VMEM((total, feature_dim), jnp.bfloat16),
                pltpu.VMEM((WIDTHS, block_of(total), total), jnp.float32),
                pltpu.VMEM((total, LANES), jnp.float32),
            ],
            compiler_params=pltpu.CompilerParams(vmem_limit_bytes=limit),
            name="tile_grads",
        )(me, *gathered(stats), *v_list, *w_list)
        chunks = [whole]
    else:
        shapes = subtiles(groups)
        limit = 20 << 20
        params = pltpu.CompilerParams(vmem_limit_bytes=limit)

        def tile(span, partner_row, earlier=()):
            reach = 2 * max(max(shapes[i][1], shapes[i][3]) for i in span)
            stat_shapes = [shape(STATS, total)] if earlier else [shape(1, chip_rows)]
            result, area = [], 0
            for i in span:
                r0, r1, c0, c1 = shapes[i]
                tall, wide = (r1 - r0) * chip_rows, (c1 - c0) * chip_rows
                area += tall * wide
                result += [shape(WIDTHS, tall, wide), shape(tall, LANES), shape(tall, LANES),
                           shape(STATS, wide), shape(STATS, wide)]
            *arrays, last_array = pl.pallas_call(
                functools.partial(
                    tile_kernel, [shapes[i] for i in span], uppers, own_rows, reach,
                    len(earlier)),
                out_shape=result + stat_shapes,
                in_specs=[smem] + [vmem] * (1 + 2 * reach + 4 * len(earlier)),
                out_specs=[vmem] * (len(result) + 1),
                compiler_params=params,
                cost_estimate=pl.CostEstimate(
                    flops=6 * area * feature_dim, transcendentals=0,
                    bytes_accessed=2 * total * feature_dim),
            )(me, partner_row, *v_list[:reach], *w_list[:reach],
              *[a for one in earlier for a in one[1:]])
            return [arrays[5 * i:5 * i + 5] for i in range(len(span))], last_array

        done, chip_partner = tile([0], chip_partner)
        more, chip_partner = tile([1, 2], chip_partner)
        done += more
        more, stats = tile([3, 4], chip_partner, done)
        done += more
        common = [me, *gathered(stats), *[t[0] for t in done], *[t[1] for t in done],
                  *[t[3] for t in done], *w_list]
        last = WIDTHS - 1

        def bands(widths, more, follows):
            base = 0 if widths[-1] == 0 else uppers[widths[-1] - 1]
            columns = uppers[widths[0]] - base
            return pl.pallas_call(
                functools.partial(
                    band_kernel, groups, uppers, widths, own_rows, document_masks, follows),
                out_shape=gradient_shapes(columns) + ([] if follows else [shape(total, total)]),
                in_specs=[smem] + [vmem] * (len(common) - 1 + len(more)),
                out_specs=[vmem] * (groups + (not follows)),
                scratch_shapes=[pltpu.VMEM((total, columns), jnp.bfloat16)],
                compiler_params=params,
                cost_estimate=pl.CostEstimate(
                    flops=2 * total * total * feature_dim, transcendentals=0,
                    bytes_accessed=4 * total * feature_dim),
            )(*common, *more)

        *widest, running = bands([last], [], False)
        others = bands(list(reversed(range(last))), [running], True)
        chunks = [widest, others]

    mine_parts, other_parts = [], []
    for c, chunk in enumerate(chunks):
        partial = dict(enumerate(chunk))
        for stage in range(stages - 1):
            step = 1 << stage
            for j in sorted([j for j in partial if j & step], reverse=True):
                arrived = along(partial.pop(j).astype(jnp.bfloat16), stage)
                partial[j ^ step] = partial[j ^ step] + arrived.astype(jnp.float32)
        stage = stages - 1
        outgoing = partial[1 << stage].astype(jnp.bfloat16)
        kept = partial[0]
        if c < len(chunks) - 1:
            arrived = along(outgoing, stage)
            kept = kept + arrived.astype(jnp.float32)
            mine_parts.append(kept[:own_rows])
            other_parts.append(swap(kept[own_rows:]))
        else:
            far = lambda i: document_masks[stage] ^ 1 if i & 1 else query_masks[stage] ^ 1
            near_arrived = along(outgoing[:own_rows], stage)
            far_arrived = exchange(outgoing[own_rows:], far)
            mine_parts.append(kept[:own_rows] + near_arrived.astype(jnp.float32))
            other_parts.append(
                swap(kept[own_rows:]) + far_arrived.astype(jnp.float32))
    mine_parts, other_parts = mine_parts[::-1], other_parts[::-1]
    ours = jnp.concatenate(mine_parts, axis=1)
    theirs = jnp.concatenate(other_parts, axis=1)
    return jnp.where(lead, ours, theirs), jnp.where(lead, theirs, ours)


def solution(mesh):
    return jax.shard_map(
        on_device,
        mesh=mesh,
        in_specs=(P(AXES, None), P(AXES, None), P(AXES)),
        out_specs=(P(AXES, None), P(AXES, None)),
        check_vma=False,
    )
```

```python
import functools
import math

import jax
import jax.numpy as jnp
from jax import lax
from jax.experimental import pallas as pl
from jax.experimental.pallas import tpu as pltpu
from jax.sharding import PartitionSpec as P


WIDTHS = 9
AXES = ("dp", "rep")
LOG2E = 1.4426950408889634
STATS = 16
LANES = 128


logit_gain = 3.0


def width_list(feature_dim):
    return [feature_dim >> WIDTHS - 1 - nested for nested in range(WIDTHS)]


def transposed_dot(a, b):
    return lax.dot_general(a, b, (((1,), (1,)), ((), ())), preferred_element_type=jnp.float32)


def prefix_scores(v_ref, w_ref, rows, uppers):
    narrow = [m for m in uppers if m <= LANES]
    count = rows.size
    head = v_ref[rows, :LANES]
    lane = lax.broadcasted_iota(jnp.int32, head.shape, 1)
    masked = [jnp.where(lane < m, head, jnp.zeros_like(head)) for m in narrow]
    stacked = transposed_dot(jnp.concatenate(masked, axis=0), w_ref[:, :LANES])
    result = [stacked[k * count:(k + 1) * count] for k in range(len(narrow))]
    lower = narrow[-1]
    for upper in uppers[len(narrow):]:
        part = transposed_dot(v_ref[rows, lower:upper], w_ref[:, lower:upper])
        result.append(result[-1] + part)
        lower = upper
    return result


def block_of(total):
    return min(total, 256)


def load_tile(refs, scratch):
    at = 0
    for ref in refs:
        scratch[at:at + ref.shape[0], :] = ref[...]
        at += ref.shape[0]


def stats_kernel(pieces, uppers, *refs):
    role_ref, partner_ref = refs[:2]
    v_refs, w_refs = refs[2:2 + pieces], refs[2 + pieces:2 + 2 * pieces]
    out_ref, v_ref, w_ref, col_ref = refs[2 + 2 * pieces:]
    load_tile(v_refs, v_ref)
    load_tile(w_refs, w_ref)
    total = v_ref.shape[0]
    block = block_of(total)
    steps = total // block
    gains = [logit_gain * m ** -0.5 * LOG2E for m in uppers]
    own = partner_ref.shape[1]
    out_ref[...] = jnp.zeros_like(out_ref)

    @pl.when((role_ref[0] & 1) == 0)
    def _():
        for step in range(steps):
            rows = pl.ds(step * block, block)
            col_ref[rows, :] = jnp.zeros((block, LANES), jnp.float32)
            for k, s in enumerate(prefix_scores(v_ref, w_ref, rows, uppers)):
                logits = s * gains[k]
                peak = jnp.max(logits, axis=1, keepdims=True)
                mass = jnp.sum(jnp.exp2(logits - peak), axis=1, keepdims=True)
                col_ref[rows, k:k + 1] = peak + jnp.log(mass) * LOG2E
        out_ref[...] = col_ref[...].T[:STATS]

    @pl.when((role_ref[0] & 1) != 0)
    def _():
        peaks, masses = [None] * len(uppers), [None] * len(uppers)
        for step in range(steps):
            rows = pl.ds(step * block, block)
            for k, s in enumerate(prefix_scores(v_ref, w_ref, rows, uppers)):
                logits = s * gains[k]
                peak = jnp.max(logits, axis=0, keepdims=True)
                mass = jnp.sum(jnp.exp2(logits - peak), axis=0, keepdims=True)
                if step:
                    top = jnp.maximum(peak, peaks[k])
                    mass = mass * jnp.exp2(peak - top) + masses[k] * jnp.exp2(peaks[k] - top)
                    peak = top
                peaks[k], masses[k] = peak, mass
        for k in range(len(uppers)):
            out_ref[k:k + 1, :] = peaks[k] + jnp.log(masses[k]) * LOG2E

    out_ref[len(uppers):len(uppers) + 1, :own] = partner_ref[...]


def document_ids(shape, axis, first, own_rows, masks, start=0):
    at = lax.broadcasted_iota(jnp.int32, shape, axis) + start
    shift = own_rows.bit_length() - 1
    piece = at >> shift
    device = first ^ (piece & 1)
    for s, mask in enumerate(masks):
        device = device ^ (((piece >> (1 + s)) & 1) * mask)
    return (device * own_rows + (at & (own_rows - 1))).astype(jnp.float32)


def grads_kernel(pieces, uppers, own_rows, masks, *refs):
    me_ref = refs[0]
    groups = pieces // 2
    stat_refs = refs[1:1 + groups]
    v_refs = refs[1 + groups:1 + groups + pieces]
    w_refs = refs[1 + groups + pieces:1 + groups + 2 * pieces]
    out_refs = refs[1 + groups + 2 * pieces:1 + 2 * groups + 2 * pieces]
    v_ref, w_ref, score_ref, col_ref = refs[1 + 2 * groups + 2 * pieces:]
    load_tile(v_refs, v_ref)
    load_tile(w_refs, w_ref)
    total = v_ref.shape[0]
    block = block_of(total)
    chip_rows = total // groups
    count = len(uppers)
    scales = [logit_gain * m ** -0.5 for m in uppers]
    me = me_ref[0]
    lead = (me & 1) == 0

    parts = []
    partners = []
    for j, ref in enumerate(stat_refs):
        parts.append(jnp.concatenate(
            [ref[:, (i ^ j) * chip_rows:((i ^ j) + 1) * chip_rows] for i in range(groups)], axis=1))
        partners.append(ref[count:count + 1, :chip_rows])
    peak = functools.reduce(jnp.maximum, parts)
    mass = functools.reduce(lambda a, b: a + b, [jnp.exp2(part - peak) for part in parts])
    totals = peak + jnp.log(mass) * LOG2E
    partner_row = jnp.concatenate(partners, axis=1)
    packed = jnp.concatenate(
        [totals[:count], partner_row, jnp.zeros((LANES - count - 1, total), jnp.float32)], axis=0)
    col_ref[...] = packed.T
    zero_or = lambda keep, x: jnp.where(keep, x, jnp.zeros_like(x))
    document_row = document_ids((1, total), 1, me | 1, own_rows, masks)
    id_row = jnp.where(lead, document_row, partner_row)
    shifts = [math.log2(s) for s in scales]
    total_rows = [zero_or(jnp.logical_not(lead), totals[k:k + 1]) - shifts[k] for k in range(count)]

    narrow = [m for m in uppers if m <= LANES]
    for step in range(total // block):
        rows = pl.ds(step * block, block)
        document_col = document_ids((block, 1), 0, me | 1, own_rows, masks, step * block)
        id_col = jnp.where(lead, col_ref[rows, count:count + 1], document_col)
        hit = id_col == id_row
        for k, s in enumerate(prefix_scores(v_ref, w_ref, rows, uppers)):
            score_ref[k] = s
        running = None
        stack = []
        for k in reversed(range(count)):
            gain = scales[k] * LOG2E
            total_col = zero_or(lead, col_ref[rows, k:k + 1])
            weight = jnp.exp2(score_ref[k] * gain - total_col - total_rows[k])
            weight = weight - jnp.where(hit, scales[k], 0.0)
            running = weight if running is None else running + weight
            band = running.astype(jnp.bfloat16)
            if k >= len(narrow):
                lower, upper = uppers[k - 1], uppers[k]
                product = jnp.dot(band, w_ref[:, lower:upper], preferred_element_type=jnp.float32)
                store(out_refs, product, step * block, lower, upper, chip_rows)
            else:
                stack.append(band)
        product = jnp.dot(
            jnp.concatenate(stack, axis=0), w_ref[:, :LANES], preferred_element_type=jnp.float32)
        lane = lax.broadcasted_iota(jnp.int32, (block, LANES), 1)
        chosen = product[:block]
        for at_stack in range(1, len(stack)):
            k = len(narrow) - 1 - at_stack
            chosen = jnp.where(
                lane < uppers[k], product[at_stack * block:(at_stack + 1) * block], chosen)
        store(out_refs, chosen, step * block, 0, LANES, chip_rows)


def rows_of(refs, lower, upper):
    return jnp.concatenate([ref[:, lower:upper] for ref in refs], axis=0)


def subtile_scores(v_refs, w_refs, uppers):
    narrow = [m for m in uppers if m <= LANES]
    left, right = rows_of(v_refs, 0, LANES), rows_of(w_refs, 0, LANES)
    slim = right.shape[0] < 2 * LANES
    head = right if slim else left
    count = head.shape[0]
    lane = lax.broadcasted_iota(jnp.int32, head.shape, 1)
    masked = jnp.concatenate(
        [jnp.where(lane < m, head, jnp.zeros_like(head)) for m in narrow], axis=0)
    if slim:
        stacked = transposed_dot(left, masked)
        parts = [stacked[:, k * count:(k + 1) * count] for k in range(len(narrow))]
    else:
        stacked = transposed_dot(masked, right)
        parts = [stacked[k * count:(k + 1) * count] for k in range(len(narrow))]
    yield from parts
    lower, running = narrow[-1], parts[-1]
    for upper in uppers[len(narrow):]:
        running = running + transposed_dot(
            rows_of(v_refs, lower, upper), rows_of(w_refs, lower, upper))
        yield running
        lower = upper


def subtile(lead, v_refs, w_refs, uppers, refs):
    power_ref, col_peak, col_mass, row_peak, row_mass = refs
    gains = [logit_gain * m ** -0.5 * LOG2E for m in uppers]
    count = power_ref.shape[1]

    @pl.when(lead)
    def _():
        lane = lax.broadcasted_iota(jnp.int32, (count, LANES), 1)
        peaks = jnp.zeros((count, LANES), jnp.float32)
        masses = jnp.ones((count, LANES), jnp.float32)
        for k, s in enumerate(subtile_scores(v_refs, w_refs, uppers)):
            logits = s * gains[k]
            peak = jnp.max(logits, axis=1, keepdims=True)
            power = jnp.exp2(logits - peak)
            power_ref[k] = power
            peaks = jnp.where(lane == k, peak, peaks)
            masses = jnp.where(lane == k, jnp.sum(power, axis=1, keepdims=True), masses)
        col_peak[...] = peaks
        col_mass[...] = masses

    @pl.when(jnp.logical_not(lead))
    def _():
        row_peak[...] = jnp.zeros_like(row_peak)
        row_mass[...] = jnp.ones_like(row_mass)
        for k, s in enumerate(subtile_scores(v_refs, w_refs, uppers)):
            logits = s * gains[k]
            peak = jnp.max(logits, axis=0, keepdims=True)
            power = jnp.exp2(logits - peak)
            power_ref[k] = power
            row_peak[k:k + 1, :] = peak
            row_mass[k:k + 1, :] = jnp.sum(power, axis=0, keepdims=True)


def log_sum(pairs):
    top = functools.reduce(jnp.maximum, [peak for peak, _ in pairs])
    mass = functools.reduce(
        lambda a, b: a + b, [mass * jnp.exp2(peak - top) for peak, mass in pairs])
    return top + jnp.log(mass) * LOG2E


def tile_kernel(span, groups, uppers, own_rows, finish, *refs):
    shapes = subtiles(groups)
    tiles = [shapes[i] for i in span]
    r0, r1, c0, c1 = extent(tiles)
    me_ref, partner_ref = refs[:2]
    at = 2 + 2 * (r1 - r0)
    v_refs, w_refs = refs[2:at], refs[at:at + 2 * (c1 - c0)]
    at += 2 * (c1 - c0)
    earlier = refs[at:at + 4 * finish]
    outs = refs[at + 4 * finish:]
    lead = (me_ref[0] & 1) == 0
    for i, (t0, t1, u0, u1) in enumerate(tiles):
        subtile(
            lead, v_refs[2 * (t0 - r0):2 * (t1 - r0)], w_refs[2 * (u0 - c0):2 * (u1 - c0)],
            uppers, outs[5 * i:5 * i + 5])
    if not finish:
        outs[-1][...] = partner_ref[...]
        return
    stats_ref = outs[-1]
    every = [earlier[4 * i:4 * i + 4] for i in range(finish)]
    every += [outs[5 * i + 1:5 * i + 5] for i in range(len(tiles))]
    segments = segments_of(groups)
    chip_rows = 2 * own_rows

    @pl.when(lead)
    def _():
        merged = []
        for s0, s1 in segments:
            pairs = []
            for (r0, r1, _, _), tile in zip(shapes, every):
                if r0 <= s0 and s1 <= r1:
                    rows = slice((s0 - r0) * chip_rows, (s1 - r0) * chip_rows)
                    pairs.append((tile[0][rows, :], tile[1][rows, :]))
            merged.append(log_sum(pairs))
        stats_ref[...] = jnp.concatenate(merged, axis=0).T[:STATS]

    @pl.when(jnp.logical_not(lead))
    def _():
        for s0, s1 in segments:
            pairs = []
            for (_, _, c0, c1), tile in zip(shapes, every):
                if c0 <= s0 and s1 <= c1:
                    across = slice((s0 - c0) * chip_rows, (s1 - c0) * chip_rows)
                    pairs.append((tile[2][:, across], tile[3][:, across]))
            stats_ref[:, s0 * chip_rows:s1 * chip_rows] = log_sum(pairs)

    count = len(uppers)
    stats_ref[count:count + 1, :chip_rows] = partner_ref[...]


def segments_of(groups):
    low, middle = groups // 2, groups // 2 + groups // 4
    return [(0, low), (low, middle), (middle, groups)]


def subtiles(groups):
    (_, low), (_, middle), _ = segments_of(groups)
    return [(0, low, 0, low), (0, low, low, middle), (low, middle, 0, middle),
            (middle, groups, 0, middle), (0, groups, middle, groups)]


def extent(tiles):
    first, second, third, fourth = zip(*tiles)
    return min(first), max(second), min(third), max(fourth)


def band_kernel(groups, uppers, widths, own_rows, masks, follows, *refs):
    me_ref = refs[0]
    stat_refs = refs[1:1 + groups]
    at = 1 + groups
    shapes = subtiles(groups)
    tiles = len(shapes)
    power_refs, col_refs, row_refs = [refs[at + i * tiles:at + (i + 1) * tiles] for i in range(3)]
    at += 3 * tiles
    w_refs = refs[at:at + 2 * groups]
    at += 2 * groups
    before_ref = None
    if follows:
        before_ref, at = refs[at], at + 1
    out_refs = refs[at:at + groups]
    at += groups
    after_ref = None
    if not follows:
        after_ref, at = refs[at], at + 1
    w_ref, = refs[at:]
    base = 0 if widths[-1] == 0 else uppers[widths[-1] - 1]
    top = uppers[widths[0]]
    for i, ref in enumerate(w_refs):
        w_ref[i * own_rows:(i + 1) * own_rows, :] = ref[:, base:top]

    total = w_ref.shape[0]
    chip_rows = total // groups
    count = len(uppers)
    scales = [logit_gain * m ** -0.5 for m in uppers]
    me = me_ref[0]
    lead = (me & 1) == 0
    parts, partners = [], []
    for j, ref in enumerate(stat_refs):
        parts.append(jnp.concatenate(
            [ref[:, (i ^ j) * chip_rows:((i ^ j) + 1) * chip_rows] for i in range(groups)], axis=1))
        partners.append(ref[count:count + 1, :chip_rows])
    peak = functools.reduce(jnp.maximum, parts)
    mass = functools.reduce(lambda a, b: a + b, [jnp.exp2(part - peak) for part in parts])
    partner_row = jnp.concatenate(partners, axis=1)
    sub = lax.broadcasted_iota(jnp.int32, (STATS, total), 0)
    totals = peak + jnp.log(mass) * LOG2E
    for k in range(count):
        totals = jnp.where(sub == k, totals - math.log2(scales[k]), totals)
    packed = jnp.concatenate(
        [totals[:count], partner_row, jnp.zeros((LANES - count - 1, total), jnp.float32)], axis=0)
    cols = packed.T
    id_row = jnp.where(
        lead, document_ids((1, total), 1, me | 1, own_rows, masks), partner_row)
    id_col = jnp.where(
        lead, cols[:, count:count + 1],
        document_ids((total, 1), 0, me | 1, own_rows, masks))

    segments = segments_of(groups)
    narrow = [k for k in widths if uppers[k] <= LANES]
    for block in (segments[1:], segments[:1]):
        first = block[0][0] * chip_rows
        rows = slice(first, block[-1][1] * chip_rows)
        height = rows.stop - first
        hit = id_col[rows] == id_row
        strips = []
        for s0, s1 in block:
            strip = []
            for (r0, r1, c0, c1), power, col_peak, row_peak in zip(
                    shapes, power_refs, col_refs, row_refs):
                if r0 <= s0 and s1 <= r1:
                    inner = slice((s0 - r0) * chip_rows, (s1 - r0) * chip_rows)
                    outer = slice(s0 * chip_rows, s1 * chip_rows)
                    across = slice(c0 * chip_rows, c1 * chip_rows)
                    strip.append((
                        c0, power, inner,
                        jnp.where(lead, jnp.exp2(col_peak[inner, :] - cols[outer]), 1.0),
                        jnp.where(lead, 1.0, jnp.exp2(row_peak[...] - totals[:, across]))))
            strips.append(sorted(strip, key=lambda item: item[0]))
        running = before_ref[rows, :] if follows else None
        stack = []
        for k in widths:
            weight = jnp.concatenate([
                jnp.concatenate([
                    power[k, inner] * col_gain[:, k:k + 1] * row_gain[k:k + 1, :]
                    for _, power, inner, col_gain, row_gain in strip], axis=1)
                for strip in strips], axis=0)
            weight = weight - jnp.where(hit, scales[k], 0.0)
            running = weight if running is None else running + weight
            band = running.astype(jnp.bfloat16)
            if k not in narrow:
                lower, upper = uppers[k - 1] - base, uppers[k] - base
                product = jnp.dot(band, w_ref[:, lower:upper], preferred_element_type=jnp.float32)
                store(out_refs, product, first, lower, upper, chip_rows)
            else:
                stack.append(band)
        if not follows:
            after_ref[rows, :] = running
        if narrow:
            product = jnp.dot(
                jnp.concatenate(stack, axis=0), w_ref[:, :LANES],
                preferred_element_type=jnp.float32)
            lane = lax.broadcasted_iota(jnp.int32, (height, LANES), 1)
            chosen = product[:height]
            for i in range(1, len(stack)):
                chosen = jnp.where(
                    lane < uppers[narrow[i]], product[i * height:(i + 1) * height], chosen)
            store(out_refs, chosen, first, 0, LANES, chip_rows)


def store(out_refs, value, first_row, lower, upper, chip_rows):
    for at in range(0, value.shape[0], chip_rows):
        ref = out_refs[(first_row + at) // chip_rows]
        ref[:, lower:upper] = value[at:at + chip_rows].astype(ref.dtype)


def on_device(queries, documents, partner):
    own_rows, feature_dim = queries.shape
    uppers = width_list(feature_dim)
    dp_size, rep_size = lax.axis_size("dp"), lax.axis_size("rep")
    devices = dp_size * rep_size
    bits = devices.bit_length() - 1
    assert rep_size == 2 and devices == 1 << bits and bits % 2 == 1
    stages = (bits - 1) // 2
    groups = 1 << stages
    pieces = 2 * groups
    query_masks = [1 << (2 * s + 1) for s in range(stages)]
    document_masks = [1 << (2 * s + 2) for s in range(stages)]
    total = pieces * own_rows
    chip_rows = 2 * own_rows

    role = lax.axis_index("rep")
    me = (lax.axis_index("dp") * rep_size + role).astype(jnp.int32).reshape(1)
    lead = role == 0

    def exchange(x, masks_of):
        return lax.ppermute(x, AXES, [(i, i ^ masks_of(i)) for i in range(devices)])

    def swap(x):
        return exchange(x, lambda i: 1)

    def along(x, stage):
        return exchange(x, lambda i: document_masks[stage] if i & 1 else query_masks[stage])

    mine = jnp.where(lead, queries, documents)
    other = jnp.where(lead, documents, queries)
    v = {(0, 0): mine, (0, 1): swap(other)}
    w = {(0, 0): swap(mine), (0, 1): other}
    for stage in reversed(range(stages)):
        for j in [j for j in range(groups) if (j, 0) in v]:
            for t in range(2):
                v[j | 1 << stage, t] = along(v[j, t], stage)
    for j, t in sorted(v):
        if j:
            w[j, t] = swap(v[j, t])
    order = [(j, t) for j in range(groups) for t in range(2)]
    v_list, w_list = [v[key] for key in order], [w[key] for key in order]

    own_partner = partner.astype(jnp.float32).reshape(1, own_rows)
    far_partner = swap(own_partner)
    chip_partner = jnp.where(
        lead,
        jnp.concatenate([own_partner, far_partner], axis=1),
        jnp.concatenate([far_partner, own_partner], axis=1))

    vmem = pl.BlockSpec(memory_space=pltpu.VMEM)
    smem = pl.BlockSpec(memory_space=pltpu.SMEM)

    def query_mask(j):
        return sum(mask for s, mask in enumerate(query_masks) if j >> s & 1)

    def gathered(stats):
        return [stats] + [exchange(stats, lambda i: query_mask(j)) for j in range(1, groups)]

    shape = lambda *dims: jax.ShapeDtypeStruct(dims, jnp.float32)

    def gradient_shapes(columns):
        return [
            jax.ShapeDtypeStruct((chip_rows, columns), jnp.bfloat16 if j & 1 else jnp.float32)
            for j in range(groups)]

    if WIDTHS * total * total * 4 > 16 << 20:
        limit = 60 << 20
        stats = pl.pallas_call(
            functools.partial(stats_kernel, pieces, uppers),
            out_shape=shape(STATS, total),
            in_specs=[smem] + [vmem] * (1 + 2 * pieces),
            out_specs=vmem,
            scratch_shapes=[
                pltpu.VMEM((total, feature_dim), jnp.bfloat16),
                pltpu.VMEM((total, feature_dim), jnp.bfloat16),
                pltpu.VMEM((total, LANES), jnp.float32),
            ],
            compiler_params=pltpu.CompilerParams(vmem_limit_bytes=limit),
            name="tile_stats",
        )(me, chip_partner, *v_list, *w_list)
        whole = pl.pallas_call(
            functools.partial(grads_kernel, pieces, uppers, own_rows, document_masks),
            out_shape=gradient_shapes(feature_dim),
            in_specs=[smem] + [vmem] * (groups + 2 * pieces),
            out_specs=[vmem] * groups,
            scratch_shapes=[
                pltpu.VMEM((total, feature_dim), jnp.bfloat16),
                pltpu.VMEM((total, feature_dim), jnp.bfloat16),
                pltpu.VMEM((WIDTHS, block_of(total), total), jnp.float32),
                pltpu.VMEM((total, LANES), jnp.float32),
            ],
            compiler_params=pltpu.CompilerParams(vmem_limit_bytes=limit),
            name="tile_grads",
        )(me, *gathered(stats), *v_list, *w_list)
        chunks = [whole]
    else:
        shapes = subtiles(groups)
        limit = 20 << 20
        params = pltpu.CompilerParams(vmem_limit_bytes=limit)

        def tile(span, partner_row, earlier=()):
            first, end, left, right = extent([shapes[i] for i in span])
            operands = v_list[2 * first:2 * end] + w_list[2 * left:2 * right]
            stat_shapes = [shape(STATS, total)] if earlier else [shape(1, chip_rows)]
            result, area = [], 0
            for i in span:
                r0, r1, c0, c1 = shapes[i]
                tall, wide = (r1 - r0) * chip_rows, (c1 - c0) * chip_rows
                area += tall * wide
                result += [shape(WIDTHS, tall, wide), shape(tall, LANES), shape(tall, LANES),
                           shape(STATS, wide), shape(STATS, wide)]
            *arrays, last_array = pl.pallas_call(
                functools.partial(
                    tile_kernel, span, groups, uppers, own_rows, len(earlier)),
                out_shape=result + stat_shapes,
                in_specs=[smem] + [vmem] * (1 + len(operands) + 4 * len(earlier)),
                out_specs=[vmem] * (len(result) + 1),
                compiler_params=params,
                cost_estimate=pl.CostEstimate(
                    flops=6 * area * feature_dim, transcendentals=0,
                    bytes_accessed=2 * total * feature_dim),
            )(me, partner_row, *operands, *[a for one in earlier for a in one[1:]])
            return [arrays[5 * i:5 * i + 5] for i in range(len(span))], last_array

        done, chip_partner = tile([0], chip_partner)
        more, chip_partner = tile([1, 2], chip_partner)
        done += more
        more, chip_partner = tile([3], chip_partner)
        done += more
        more, stats = tile([4], chip_partner, done)
        done += more
        common = [me, *gathered(stats), *[t[0] for t in done], *[t[1] for t in done],
                  *[t[3] for t in done], *w_list]
        last = WIDTHS - 1

        def bands(widths, more, follows):
            base = 0 if widths[-1] == 0 else uppers[widths[-1] - 1]
            columns = uppers[widths[0]] - base
            return pl.pallas_call(
                functools.partial(
                    band_kernel, groups, uppers, widths, own_rows, document_masks, follows),
                out_shape=gradient_shapes(columns) + ([] if follows else [shape(total, total)]),
                in_specs=[smem] + [vmem] * (len(common) - 1 + len(more)),
                out_specs=[vmem] * (groups + (not follows)),
                scratch_shapes=[pltpu.VMEM((total, columns), jnp.bfloat16)],
                compiler_params=params,
                cost_estimate=pl.CostEstimate(
                    flops=2 * total * total * feature_dim, transcendentals=0,
                    bytes_accessed=4 * total * feature_dim),
            )(*common, *more)

        *widest, running = bands([last], [], False)
        others = bands(list(reversed(range(last))), [running], True)
        chunks = [widest, others]

    mine_parts, other_parts = [], []
    for c, chunk in enumerate(chunks):
        partial = dict(enumerate(chunk))
        for stage in range(stages - 1):
            step = 1 << stage
            for j in sorted([j for j in partial if j & step], reverse=True):
                arrived = along(partial.pop(j).astype(jnp.bfloat16), stage)
                partial[j ^ step] = partial[j ^ step] + arrived.astype(jnp.float32)
                if stage == stages - 2 and j ^ step:
                    partial[j ^ step] = partial[j ^ step].astype(jnp.bfloat16)
        stage = stages - 1
        outgoing = partial[1 << stage]
        kept = partial[0]
        if c < len(chunks) - 1:
            arrived = along(outgoing, stage)
            kept = kept + arrived.astype(jnp.float32)
            mine_parts.append(kept[:own_rows])
            other_parts.append(swap(kept[own_rows:]))
        else:
            far = lambda i: document_masks[stage] ^ 1 if i & 1 else query_masks[stage] ^ 1
            near_arrived = along(outgoing[:own_rows], stage)
            far_arrived = exchange(outgoing[own_rows:], far)
            ours, theirs = lax.optimization_barrier((kept[:own_rows], kept[own_rows:]))
            mine_parts.append(ours + near_arrived.astype(jnp.float32))
            other_parts.append(swap(theirs) + far_arrived.astype(jnp.float32))
    mine_parts, other_parts = mine_parts[::-1], other_parts[::-1]
    ours = jnp.concatenate(mine_parts, axis=1)
    theirs = jnp.concatenate(other_parts, axis=1)
    return jnp.where(lead, ours, theirs), jnp.where(lead, theirs, ours)


def solution(mesh):
    return jax.shard_map(
        on_device,
        mesh=mesh,
        in_specs=(P(AXES, None), P(AXES, None), P(AXES)),
        out_specs=(P(AXES, None), P(AXES, None)),
        check_vma=False,
    )
```

```python
import functools
import math

import jax
import jax.numpy as jnp
from jax import lax
from jax.experimental import pallas as pl
from jax.experimental.pallas import tpu as pltpu
from jax.sharding import PartitionSpec as P


WIDTHS = 9
AXES = ("dp", "rep")
LOG2E = 1.4426950408889634
STATS = 16
LANES = 128


logit_gain = 3.0


def width_list(feature_dim):
    return [feature_dim >> WIDTHS - 1 - nested for nested in range(WIDTHS)]


def transposed_dot(a, b):
    return lax.dot_general(a, b, (((1,), (1,)), ((), ())), preferred_element_type=jnp.float32)


def prefix_scores(v_ref, w_ref, rows, uppers):
    narrow = [m for m in uppers if m <= LANES]
    count = rows.size
    head = v_ref[rows, :LANES]
    lane = lax.broadcasted_iota(jnp.int32, head.shape, 1)
    masked = [jnp.where(lane < m, head, jnp.zeros_like(head)) for m in narrow]
    stacked = transposed_dot(jnp.concatenate(masked, axis=0), w_ref[:, :LANES])
    result = [stacked[k * count:(k + 1) * count] for k in range(len(narrow))]
    lower = narrow[-1]
    for upper in uppers[len(narrow):]:
        part = transposed_dot(v_ref[rows, lower:upper], w_ref[:, lower:upper])
        result.append(result[-1] + part)
        lower = upper
    return result


def block_of(total):
    return min(total, 256)


def load_tile(refs, scratch):
    at = 0
    for ref in refs:
        scratch[at:at + ref.shape[0], :] = ref[...]
        at += ref.shape[0]


def stats_kernel(pieces, uppers, *refs):
    role_ref, partner_ref = refs[:2]
    v_refs, w_refs = refs[2:2 + pieces], refs[2 + pieces:2 + 2 * pieces]
    out_ref, v_ref, w_ref, col_ref = refs[2 + 2 * pieces:]
    load_tile(v_refs, v_ref)
    load_tile(w_refs, w_ref)
    total = v_ref.shape[0]
    block = block_of(total)
    steps = total // block
    gains = [logit_gain * m ** -0.5 * LOG2E for m in uppers]
    own = partner_ref.shape[1]
    out_ref[...] = jnp.zeros_like(out_ref)

    @pl.when((role_ref[0] & 1) == 0)
    def _():
        for step in range(steps):
            rows = pl.ds(step * block, block)
            col_ref[rows, :] = jnp.zeros((block, LANES), jnp.float32)
            for k, s in enumerate(prefix_scores(v_ref, w_ref, rows, uppers)):
                logits = s * gains[k]
                peak = jnp.max(logits, axis=1, keepdims=True)
                mass = jnp.sum(jnp.exp2(logits - peak), axis=1, keepdims=True)
                col_ref[rows, k:k + 1] = peak + jnp.log(mass) * LOG2E
        out_ref[...] = col_ref[...].T[:STATS]

    @pl.when((role_ref[0] & 1) != 0)
    def _():
        peaks, masses = [None] * len(uppers), [None] * len(uppers)
        for step in range(steps):
            rows = pl.ds(step * block, block)
            for k, s in enumerate(prefix_scores(v_ref, w_ref, rows, uppers)):
                logits = s * gains[k]
                peak = jnp.max(logits, axis=0, keepdims=True)
                mass = jnp.sum(jnp.exp2(logits - peak), axis=0, keepdims=True)
                if step:
                    top = jnp.maximum(peak, peaks[k])
                    mass = mass * jnp.exp2(peak - top) + masses[k] * jnp.exp2(peaks[k] - top)
                    peak = top
                peaks[k], masses[k] = peak, mass
        for k in range(len(uppers)):
            out_ref[k:k + 1, :] = peaks[k] + jnp.log(masses[k]) * LOG2E

    out_ref[len(uppers):len(uppers) + 1, :own] = partner_ref[...]


def document_ids(shape, axis, first, own_rows, masks, start=0):
    at = lax.broadcasted_iota(jnp.int32, shape, axis) + start
    shift = own_rows.bit_length() - 1
    piece = at >> shift
    device = first ^ (piece & 1)
    for s, mask in enumerate(masks):
        device = device ^ (((piece >> (1 + s)) & 1) * mask)
    return (device * own_rows + (at & (own_rows - 1))).astype(jnp.float32)


def grads_kernel(pieces, uppers, own_rows, masks, *refs):
    me_ref = refs[0]
    groups = pieces // 2
    stat_refs = refs[1:1 + groups]
    v_refs = refs[1 + groups:1 + groups + pieces]
    w_refs = refs[1 + groups + pieces:1 + groups + 2 * pieces]
    out_refs = refs[1 + groups + 2 * pieces:1 + 2 * groups + 2 * pieces]
    v_ref, w_ref, score_ref, col_ref = refs[1 + 2 * groups + 2 * pieces:]
    load_tile(v_refs, v_ref)
    load_tile(w_refs, w_ref)
    total = v_ref.shape[0]
    block = block_of(total)
    chip_rows = total // groups
    count = len(uppers)
    scales = [logit_gain * m ** -0.5 for m in uppers]
    me = me_ref[0]
    lead = (me & 1) == 0

    parts = []
    partners = []
    for j, ref in enumerate(stat_refs):
        parts.append(jnp.concatenate(
            [ref[:, (i ^ j) * chip_rows:((i ^ j) + 1) * chip_rows] for i in range(groups)], axis=1))
        partners.append(ref[count:count + 1, :chip_rows])
    peak = functools.reduce(jnp.maximum, parts)
    mass = functools.reduce(lambda a, b: a + b, [jnp.exp2(part - peak) for part in parts])
    totals = peak + jnp.log(mass) * LOG2E
    partner_row = jnp.concatenate(partners, axis=1)
    packed = jnp.concatenate(
        [totals[:count], partner_row, jnp.zeros((LANES - count - 1, total), jnp.float32)], axis=0)
    col_ref[...] = packed.T
    zero_or = lambda keep, x: jnp.where(keep, x, jnp.zeros_like(x))
    document_row = document_ids((1, total), 1, me | 1, own_rows, masks)
    id_row = jnp.where(lead, document_row, partner_row)
    shifts = [math.log2(s) for s in scales]
    total_rows = [zero_or(jnp.logical_not(lead), totals[k:k + 1]) - shifts[k] for k in range(count)]

    narrow = [m for m in uppers if m <= LANES]
    for step in range(total // block):
        rows = pl.ds(step * block, block)
        document_col = document_ids((block, 1), 0, me | 1, own_rows, masks, step * block)
        id_col = jnp.where(lead, col_ref[rows, count:count + 1], document_col)
        hit = id_col == id_row
        for k, s in enumerate(prefix_scores(v_ref, w_ref, rows, uppers)):
            score_ref[k] = s
        running = None
        stack = []
        for k in reversed(range(count)):
            gain = scales[k] * LOG2E
            total_col = zero_or(lead, col_ref[rows, k:k + 1])
            weight = jnp.exp2(score_ref[k] * gain - total_col - total_rows[k])
            weight = weight - jnp.where(hit, scales[k], 0.0)
            running = weight if running is None else running + weight
            band = running.astype(jnp.bfloat16)
            if k >= len(narrow):
                lower, upper = uppers[k - 1], uppers[k]
                product = jnp.dot(band, w_ref[:, lower:upper], preferred_element_type=jnp.float32)
                store(out_refs, product, step * block, lower, upper, chip_rows)
            else:
                stack.append(band)
        product = jnp.dot(
            jnp.concatenate(stack, axis=0), w_ref[:, :LANES], preferred_element_type=jnp.float32)
        lane = lax.broadcasted_iota(jnp.int32, (block, LANES), 1)
        chosen = product[:block]
        for at_stack in range(1, len(stack)):
            k = len(narrow) - 1 - at_stack
            chosen = jnp.where(
                lane < uppers[k], product[at_stack * block:(at_stack + 1) * block], chosen)
        store(out_refs, chosen, step * block, 0, LANES, chip_rows)


def rows_of(refs, lower, upper):
    return jnp.concatenate([ref[:, lower:upper] for ref in refs], axis=0)


def subtile_scores(v_refs, w_refs, uppers):
    narrow = [m for m in uppers if m <= LANES]
    left, right = rows_of(v_refs, 0, LANES), rows_of(w_refs, 0, LANES)
    slim = right.shape[0] < 2 * LANES
    head = right if slim else left
    count = head.shape[0]
    lane = lax.broadcasted_iota(jnp.int32, head.shape, 1)
    masked = jnp.concatenate(
        [jnp.where(lane < m, head, jnp.zeros_like(head)) for m in narrow], axis=0)
    if slim:
        stacked = transposed_dot(left, masked)
        parts = [stacked[:, k * count:(k + 1) * count] for k in range(len(narrow))]
    else:
        stacked = transposed_dot(masked, right)
        parts = [stacked[k * count:(k + 1) * count] for k in range(len(narrow))]
    yield from parts
    lower, running = narrow[-1], parts[-1]
    for upper in uppers[len(narrow):]:
        running = running + transposed_dot(
            rows_of(v_refs, lower, upper), rows_of(w_refs, lower, upper))
        yield running
        lower = upper


def subtile(lead, v_refs, w_refs, uppers, refs):
    power_ref, col_peak, col_mass, row_peak, row_mass = refs
    gains = [logit_gain * m ** -0.5 * LOG2E for m in uppers]
    count = power_ref.shape[1]

    @pl.when(lead)
    def _():
        lane = lax.broadcasted_iota(jnp.int32, (count, LANES), 1)
        peaks = jnp.zeros((count, LANES), jnp.float32)
        masses = jnp.ones((count, LANES), jnp.float32)
        for k, s in enumerate(subtile_scores(v_refs, w_refs, uppers)):
            logits = s * gains[k]
            peak = jnp.max(logits, axis=1, keepdims=True)
            power = jnp.exp2(logits - peak)
            power_ref[k] = power
            peaks = jnp.where(lane == k, peak, peaks)
            masses = jnp.where(lane == k, jnp.sum(power, axis=1, keepdims=True), masses)
        col_peak[...] = peaks
        col_mass[...] = masses

    @pl.when(jnp.logical_not(lead))
    def _():
        row_peak[...] = jnp.zeros_like(row_peak)
        row_mass[...] = jnp.ones_like(row_mass)
        for k, s in enumerate(subtile_scores(v_refs, w_refs, uppers)):
            logits = s * gains[k]
            peak = jnp.max(logits, axis=0, keepdims=True)
            power = jnp.exp2(logits - peak)
            power_ref[k] = power
            row_peak[k:k + 1, :] = peak
            row_mass[k:k + 1, :] = jnp.sum(power, axis=0, keepdims=True)


def log_sum(pairs):
    top = functools.reduce(jnp.maximum, [peak for peak, _ in pairs])
    mass = functools.reduce(
        lambda a, b: a + b, [mass * jnp.exp2(peak - top) for peak, mass in pairs])
    return top + jnp.log(mass) * LOG2E


def tile_kernel(span, counts, uppers, own_rows, finish, *refs):
    groups = len(counts)
    shapes = subtiles(groups)
    tiles = [shapes[i] for i in span]
    r0, r1, c0, c1 = extent(tiles)
    me_ref, partner_ref = refs[:2]
    at = 2 + sum(counts[r0:r1])
    v_refs, w_refs = refs[2:at], refs[at:at + sum(counts[c0:c1])]
    at += sum(counts[c0:c1])
    earlier = refs[at:at + 4 * finish]
    outs = refs[at + 4 * finish:]
    lead = (me_ref[0] & 1) == 0
    for i, (t0, t1, u0, u1) in enumerate(tiles):
        subtile(
            lead, v_refs[sum(counts[r0:t0]):sum(counts[r0:t1])],
            w_refs[sum(counts[c0:u0]):sum(counts[c0:u1])], uppers, outs[5 * i:5 * i + 5])
    if not finish:
        outs[-1][...] = partner_ref[...]
        return
    stats_ref = outs[-1]
    every = [earlier[4 * i:4 * i + 4] for i in range(finish)]
    every += [outs[5 * i + 1:5 * i + 5] for i in range(len(tiles))]
    segments = segments_of(groups)
    chip_rows = 2 * own_rows

    @pl.when(lead)
    def _():
        merged = []
        for s0, s1 in segments:
            pairs = []
            for (r0, r1, _, _), tile in zip(shapes, every):
                if r0 <= s0 and s1 <= r1:
                    rows = slice((s0 - r0) * chip_rows, (s1 - r0) * chip_rows)
                    pairs.append((tile[0][rows, :], tile[1][rows, :]))
            merged.append(log_sum(pairs))
        stats_ref[...] = jnp.concatenate(merged, axis=0).T[:STATS]

    @pl.when(jnp.logical_not(lead))
    def _():
        for s0, s1 in segments:
            pairs = []
            for (_, _, c0, c1), tile in zip(shapes, every):
                if c0 <= s0 and s1 <= c1:
                    across = slice((s0 - c0) * chip_rows, (s1 - c0) * chip_rows)
                    pairs.append((tile[2][:, across], tile[3][:, across]))
            stats_ref[:, s0 * chip_rows:s1 * chip_rows] = log_sum(pairs)

    count = len(uppers)
    stats_ref[count:count + 1, :chip_rows] = partner_ref[...]


def segments_of(groups):
    low, middle = groups // 2, groups // 2 + groups // 4
    return [(0, low), (low, middle), (middle, groups)]


def subtiles(groups):
    (_, low), (_, middle), _ = segments_of(groups)
    return [(0, low, 0, low), (low, middle, 0, low), (0, middle, low, middle),
            (middle, groups, 0, middle), (0, groups, middle, groups)]


def extent(tiles):
    first, second, third, fourth = zip(*tiles)
    return min(first), max(second), min(third), max(fourth)


def band_setup(groups, uppers, own_rows, masks, me_ref, stat_refs):
    count = len(uppers)
    total = stat_refs[0].shape[1]
    chip_rows = total // groups
    me = me_ref[0]
    lead = (me & 1) == 0
    parts, partners = [], []
    for j, ref in enumerate(stat_refs):
        parts.append(jnp.concatenate(
            [ref[:, (i ^ j) * chip_rows:((i ^ j) + 1) * chip_rows] for i in range(groups)], axis=1))
        partners.append(ref[count:count + 1, :chip_rows])
    peak = functools.reduce(jnp.maximum, parts)
    mass = functools.reduce(lambda a, b: a + b, [jnp.exp2(part - peak) for part in parts])
    partner_row = jnp.concatenate(partners, axis=1)
    sub = lax.broadcasted_iota(jnp.int32, (STATS, total), 0)
    totals = peak + jnp.log(mass) * LOG2E
    for k in range(count):
        totals = jnp.where(sub == k, totals - math.log2(logit_gain * uppers[k] ** -0.5), totals)
    packed = jnp.concatenate(
        [totals[:count], partner_row, jnp.zeros((LANES - count - 1, total), jnp.float32)], axis=0)
    cols = packed.T
    id_row = jnp.where(
        lead, document_ids((1, total), 1, me | 1, own_rows, masks), partner_row)
    id_col = jnp.where(
        lead, cols[:, count:count + 1],
        document_ids((total, 1), 0, me | 1, own_rows, masks))
    return lead, totals, cols, id_row, id_col


def weights_of(segment, groups, setup, power_refs, col_refs, row_refs):
    lead, totals, cols, _, _ = setup
    chip_rows = totals.shape[1] // groups
    s0, s1 = segment
    strip = []
    for (r0, r1, c0, c1), power, col_peak, row_peak in zip(
            subtiles(groups), power_refs, col_refs, row_refs):
        if r0 <= s0 and s1 <= r1:
            inner = slice((s0 - r0) * chip_rows, (s1 - r0) * chip_rows)
            outer = slice(s0 * chip_rows, s1 * chip_rows)
            across = slice(c0 * chip_rows, c1 * chip_rows)
            strip.append((
                c0, power, inner,
                jnp.where(lead, jnp.exp2(col_peak[inner, :] - cols[outer]), 1.0),
                jnp.where(lead, 1.0, jnp.exp2(row_peak[...] - totals[:, across]))))
    strip.sort(key=lambda item: item[0])
    return lambda k: jnp.concatenate([
        power[k, inner] * col_gain[:, k:k + 1] * row_gain[k:k + 1, :]
        for _, power, inner, col_gain, row_gain in strip], axis=1)


def last_band_kernel(groups, uppers, own_rows, masks, *refs):
    tiles = len(subtiles(groups))
    setup = band_setup(groups, uppers, own_rows, masks, refs[0], refs[1:1 + groups])
    at = 1 + groups
    power_refs, col_refs, row_refs = [refs[at + i * tiles:at + (i + 1) * tiles] for i in range(3)]
    segment = segments_of(groups)[-1]
    farthest = segment[1] - segment[0]
    w_refs, out_refs, after_ref = refs[at + 3 * tiles:-farthest - 1], refs[-farthest - 1:-1], refs[-1]
    _, totals, _, id_row, id_col = setup
    chip_rows = totals.shape[1] // groups
    k = len(uppers) - 1
    rows = slice(segment[0] * chip_rows, segment[1] * chip_rows)
    weight = weights_of(segment, groups, setup, power_refs, col_refs, row_refs)(k)
    weight = weight - jnp.where(id_col[rows] == id_row, logit_gain * uppers[k] ** -0.5, 0.0)
    after_ref[...] = weight
    product = jnp.dot(
        weight.astype(jnp.bfloat16), rows_of(w_refs, uppers[k - 1], uppers[k]),
        preferred_element_type=jnp.float32)
    store(out_refs, product, 0, 0, uppers[k] - uppers[k - 1], chip_rows)


def bands_kernel(groups, uppers, own_rows, masks, *refs):
    tiles = len(subtiles(groups))
    setup = band_setup(groups, uppers, own_rows, masks, refs[0], refs[1:1 + groups])
    at = 1 + groups
    power_refs, col_refs, row_refs = [refs[at + i * tiles:at + (i + 1) * tiles] for i in range(3)]
    segments = segments_of(groups)
    outs = groups + segments[-1][0]
    before_ref = refs[-outs - 1]
    w_refs, others, widest = refs[at + 3 * tiles:-outs - 1], refs[-outs:-outs + groups], refs[-outs + groups:]
    _, totals, _, id_row, id_col = setup
    chip_rows = totals.shape[1] // groups
    scales = [logit_gain * m ** -0.5 for m in uppers]
    last = len(uppers) - 1
    narrow = [k for k in range(last, -1, -1) if uppers[k] <= LANES]
    for block in (segments[1:], segments[:1]):
        first = block[0][0] * chip_rows
        rows = slice(first, block[-1][1] * chip_rows)
        height = rows.stop - first
        hit = id_col[rows] == id_row
        weights = [
            weights_of(segment, groups, setup, power_refs, col_refs, row_refs) for segment in block]
        tall = (block[0][1] - block[0][0]) * chip_rows
        running = weights[0](last) - jnp.where(hit[:tall], scales[last], 0.0)
        lower, upper = uppers[last - 1], uppers[last]
        product = jnp.dot(
            running.astype(jnp.bfloat16), rows_of(w_refs, lower, upper),
            preferred_element_type=jnp.float32)
        store(widest, product, first, 0, upper - lower, chip_rows)
        if len(block) > 1:
            running = jnp.concatenate([running, before_ref[...]], axis=0)
        stack = []
        for k in range(last - 1, -1, -1):
            weight = jnp.concatenate([part(k) for part in weights], axis=0)
            running = running + (weight - jnp.where(hit, scales[k], 0.0))
            band = running.astype(jnp.bfloat16)
            if k in narrow:
                stack.append(band)
                continue
            lower, upper = uppers[k - 1], uppers[k]
            product = jnp.dot(
                band, rows_of(w_refs, lower, upper), preferred_element_type=jnp.float32)
            store(others, product, first, lower, upper, chip_rows)
        product = jnp.dot(
            jnp.concatenate(stack, axis=0), rows_of(w_refs, 0, LANES),
            preferred_element_type=jnp.float32)
        lane = lax.broadcasted_iota(jnp.int32, (height, LANES), 1)
        chosen = product[:height]
        for i in range(1, len(stack)):
            chosen = jnp.where(
                lane < uppers[narrow[i]], product[i * height:(i + 1) * height], chosen)
        store(others, chosen, first, 0, LANES, chip_rows)


def store(out_refs, value, first_row, lower, upper, chip_rows):
    for at in range(0, value.shape[0], chip_rows):
        ref = out_refs[(first_row + at) // chip_rows]
        ref[:, lower:upper] = value[at:at + chip_rows].astype(ref.dtype)


def on_device(queries, documents, partner):
    own_rows, feature_dim = queries.shape
    uppers = width_list(feature_dim)
    dp_size, rep_size = lax.axis_size("dp"), lax.axis_size("rep")
    devices = dp_size * rep_size
    bits = devices.bit_length() - 1
    assert rep_size == 2 and devices == 1 << bits and bits % 2 == 1
    stages = (bits - 1) // 2
    groups = 1 << stages
    pieces = 2 * groups
    query_masks = [1 << (2 * s + 1) for s in range(stages)]
    document_masks = [1 << (2 * s + 2) for s in range(stages)]
    total = pieces * own_rows
    chip_rows = 2 * own_rows

    role = lax.axis_index("rep")
    me = (lax.axis_index("dp") * rep_size + role).astype(jnp.int32).reshape(1)
    lead = role == 0

    def exchange(x, masks_of):
        return lax.ppermute(x, AXES, [(i, i ^ masks_of(i)) for i in range(devices)])

    def swap(x):
        return exchange(x, lambda i: 1)

    def along(x, stage):
        return exchange(x, lambda i: document_masks[stage] if i & 1 else query_masks[stage])

    mine = jnp.where(lead, queries, documents)
    other = jnp.where(lead, documents, queries)
    got = swap(other)
    small = WIDTHS * total * total * 4 <= 16 << 20
    cut = own_rows - 16 if small and own_rows >= 32 else own_rows
    v = {0: [mine, got]}
    w = {0: [swap(mine), other]}
    for stage in reversed(range(stages)):
        for j in sorted(v):
            parts = v[j]
            if j == 0 and stage == stages - 1 and cut < own_rows:
                parts = [mine, got[:cut], got[cut:]]
            v[j | 1 << stage] = [
                along(part, stage) for part in parts]
    for j in range(1, groups):
        w[j] = [swap(part) for part in v[j]]
    counts = [len(v[j]) for j in range(groups)]
    v_list = [part for j in range(groups) for part in v[j]]
    w_list = [part for j in range(groups) for part in w[j]]

    own_partner = partner.astype(jnp.float32).reshape(1, own_rows)
    far_partner = swap(own_partner)
    chip_partner = jnp.where(
        lead,
        jnp.concatenate([own_partner, far_partner], axis=1),
        jnp.concatenate([far_partner, own_partner], axis=1))

    vmem = pl.BlockSpec(memory_space=pltpu.VMEM)
    smem = pl.BlockSpec(memory_space=pltpu.SMEM)

    def query_mask(j):
        return sum(mask for s, mask in enumerate(query_masks) if j >> s & 1)

    def gathered(stats):
        return [stats] + [exchange(stats, lambda i: query_mask(j)) for j in range(1, groups)]

    shape = lambda *dims: jax.ShapeDtypeStruct(dims, jnp.float32)

    def gradient_shapes(columns):
        return [
            jax.ShapeDtypeStruct((chip_rows, columns), jnp.bfloat16 if j & 1 else jnp.float32)
            for j in range(groups)]

    if not small:
        limit = 60 << 20
        stats = pl.pallas_call(
            functools.partial(stats_kernel, pieces, uppers),
            out_shape=shape(STATS, total),
            in_specs=[smem] + [vmem] * (1 + 2 * pieces),
            out_specs=vmem,
            scratch_shapes=[
                pltpu.VMEM((total, feature_dim), jnp.bfloat16),
                pltpu.VMEM((total, feature_dim), jnp.bfloat16),
                pltpu.VMEM((total, LANES), jnp.float32),
            ],
            compiler_params=pltpu.CompilerParams(vmem_limit_bytes=limit),
            name="tile_stats",
        )(me, chip_partner, *v_list, *w_list)
        whole = pl.pallas_call(
            functools.partial(grads_kernel, pieces, uppers, own_rows, document_masks),
            out_shape=gradient_shapes(feature_dim),
            in_specs=[smem] + [vmem] * (groups + 2 * pieces),
            out_specs=[vmem] * groups,
            scratch_shapes=[
                pltpu.VMEM((total, feature_dim), jnp.bfloat16),
                pltpu.VMEM((total, feature_dim), jnp.bfloat16),
                pltpu.VMEM((WIDTHS, block_of(total), total), jnp.float32),
                pltpu.VMEM((total, LANES), jnp.float32),
            ],
            compiler_params=pltpu.CompilerParams(vmem_limit_bytes=limit),
            name="tile_grads",
        )(me, *gathered(stats), *v_list, *w_list)
        chunks = [whole]
    else:
        shapes = subtiles(groups)
        limit = 20 << 20
        params = pltpu.CompilerParams(vmem_limit_bytes=limit)

        def tile(span, partner_row, earlier=()):
            first, end, left, right = extent([shapes[i] for i in span])
            operands = v_list[sum(counts[:first]):sum(counts[:end])]
            operands += w_list[sum(counts[:left]):sum(counts[:right])]
            stat_shapes = [shape(STATS, total)] if earlier else [shape(1, chip_rows)]
            result, area = [], 0
            for i in span:
                r0, r1, c0, c1 = shapes[i]
                tall, wide = (r1 - r0) * chip_rows, (c1 - c0) * chip_rows
                area += tall * wide
                result += [shape(WIDTHS, tall, wide), shape(tall, LANES), shape(tall, LANES),
                           shape(STATS, wide), shape(STATS, wide)]
            *arrays, last_array = pl.pallas_call(
                functools.partial(
                    tile_kernel, span, counts, uppers, own_rows, len(earlier)),
                out_shape=result + stat_shapes,
                in_specs=[smem] + [vmem] * (1 + len(operands) + 4 * len(earlier)),
                out_specs=[vmem] * (len(result) + 1),
                compiler_params=params,
                cost_estimate=pl.CostEstimate(
                    flops=6 * area * feature_dim, transcendentals=0,
                    bytes_accessed=2 * total * feature_dim),
            )(me, partner_row, *operands, *[a for one in earlier for a in one[1:]])
            return [arrays[5 * i:5 * i + 5] for i in range(len(span))], last_array

        done, chip_partner = tile([0], chip_partner)
        for at in (1, 2, 3):
            more, chip_partner = tile([at], chip_partner)
            done += more
        more, stats = tile([4], chip_partner, done)
        done += more
        common = [me, *gathered(stats), *[t[0] for t in done], *[t[1] for t in done],
                  *[t[3] for t in done], *w_list]
        near = segments_of(groups)[-1][0]
        widest = feature_dim - uppers[-2]

        def bands(kernel, more, outs):
            return pl.pallas_call(
                functools.partial(kernel, groups, uppers, own_rows, document_masks),
                out_shape=outs,
                in_specs=[smem] + [vmem] * (len(common) - 1 + len(more)),
                out_specs=[vmem] * len(outs),
                compiler_params=params,
                cost_estimate=pl.CostEstimate(
                    flops=2 * total * total * feature_dim, transcendentals=0,
                    bytes_accessed=4 * total * feature_dim),
            )(*common, *more)

        *far_ones, running = bands(
            last_band_kernel, [],
            gradient_shapes(widest)[near:] + [shape((groups - near) * chip_rows, total)])
        rest = bands(
            bands_kernel, [running], gradient_shapes(uppers[-2]) + gradient_shapes(widest)[:near])
        chunks = [[*rest[groups:], *far_ones], rest[:groups]]

    mine_parts, other_parts = [], []
    for c, chunk in enumerate(chunks):
        partial = dict(enumerate(chunk))
        for stage in range(stages - 1):
            step = 1 << stage
            for j in sorted([j for j in partial if j & step], reverse=True):
                arrived = along(partial.pop(j).astype(jnp.bfloat16), stage)
                partial[j ^ step] = partial[j ^ step] + arrived.astype(jnp.float32)
                if stage == stages - 2 and j ^ step:
                    partial[j ^ step] = partial[j ^ step].astype(jnp.bfloat16)
        stage = stages - 1
        outgoing = partial[1 << stage]
        kept = partial[0]
        if c < len(chunks) - 1:
            arrived = along(outgoing, stage)
            kept = kept + arrived.astype(jnp.float32)
            mine_parts.append(kept[:own_rows])
            other_parts.append(swap(kept[own_rows:]))
        else:
            far = lambda i: document_masks[stage] ^ 1 if i & 1 else query_masks[stage] ^ 1
            near_arrived = along(outgoing[:own_rows], stage)
            far_arrived = exchange(outgoing[own_rows:], far)
            ours, theirs = lax.optimization_barrier((kept[:own_rows], kept[own_rows:]))
            mine_parts.append(ours + near_arrived.astype(jnp.float32))
            other_parts.append(swap(theirs) + far_arrived.astype(jnp.float32))
    mine_parts, other_parts = mine_parts[::-1], other_parts[::-1]
    ours = jnp.concatenate(mine_parts, axis=1)
    theirs = jnp.concatenate(other_parts, axis=1)
    return jnp.where(lead, ours, theirs), jnp.where(lead, theirs, ours)


def solution(mesh):
    return jax.shard_map(
        on_device,
        mesh=mesh,
        in_specs=(P(AXES, None), P(AXES, None), P(AXES)),
        out_specs=(P(AXES, None), P(AXES, None)),
        check_vma=False,
    )
```

```python
import functools
import math

import jax
import jax.numpy as jnp
from jax import lax
from jax.experimental import pallas as pl
from jax.experimental.pallas import tpu as pltpu
from jax.sharding import PartitionSpec as P


WIDTHS = 9
AXES = ("dp", "rep")
LOG2E = 1.4426950408889634
STATS = 16
LANES = 128


logit_gain = 3.0


def width_list(feature_dim):
    return [feature_dim >> WIDTHS - 1 - nested for nested in range(WIDTHS)]


def transposed_dot(a, b):
    return lax.dot_general(a, b, (((1,), (1,)), ((), ())), preferred_element_type=jnp.float32)


def prefix_scores(v_ref, w_ref, rows, uppers):
    narrow = [m for m in uppers if m <= LANES]
    count = rows.size
    head = v_ref[rows, :LANES]
    lane = lax.broadcasted_iota(jnp.int32, head.shape, 1)
    masked = [jnp.where(lane < m, head, jnp.zeros_like(head)) for m in narrow]
    stacked = transposed_dot(jnp.concatenate(masked, axis=0), w_ref[:, :LANES])
    result = [stacked[k * count:(k + 1) * count] for k in range(len(narrow))]
    lower = narrow[-1]
    for upper in uppers[len(narrow):]:
        part = transposed_dot(v_ref[rows, lower:upper], w_ref[:, lower:upper])
        result.append(result[-1] + part)
        lower = upper
    return result


def block_of(total):
    return min(total, 256)


def load_tile(refs, scratch):
    at = 0
    for ref in refs:
        scratch[at:at + ref.shape[0], :] = ref[...]
        at += ref.shape[0]


def stats_kernel(pieces, uppers, *refs):
    role_ref, partner_ref = refs[:2]
    v_refs, w_refs = refs[2:2 + pieces], refs[2 + pieces:2 + 2 * pieces]
    out_ref, v_ref, w_ref, col_ref = refs[2 + 2 * pieces:]
    load_tile(v_refs, v_ref)
    load_tile(w_refs, w_ref)
    total = v_ref.shape[0]
    block = block_of(total)
    steps = total // block
    gains = [logit_gain * m ** -0.5 * LOG2E for m in uppers]
    own = partner_ref.shape[1]
    out_ref[...] = jnp.zeros_like(out_ref)

    @pl.when((role_ref[0] & 1) == 0)
    def _():
        for step in range(steps):
            rows = pl.ds(step * block, block)
            col_ref[rows, :] = jnp.zeros((block, LANES), jnp.float32)
            for k, s in enumerate(prefix_scores(v_ref, w_ref, rows, uppers)):
                logits = s * gains[k]
                peak = jnp.max(logits, axis=1, keepdims=True)
                mass = jnp.sum(jnp.exp2(logits - peak), axis=1, keepdims=True)
                col_ref[rows, k:k + 1] = peak + jnp.log(mass) * LOG2E
        out_ref[...] = col_ref[...].T[:STATS]

    @pl.when((role_ref[0] & 1) != 0)
    def _():
        peaks, masses = [None] * len(uppers), [None] * len(uppers)
        for step in range(steps):
            rows = pl.ds(step * block, block)
            for k, s in enumerate(prefix_scores(v_ref, w_ref, rows, uppers)):
                logits = s * gains[k]
                peak = jnp.max(logits, axis=0, keepdims=True)
                mass = jnp.sum(jnp.exp2(logits - peak), axis=0, keepdims=True)
                if step:
                    top = jnp.maximum(peak, peaks[k])
                    mass = mass * jnp.exp2(peak - top) + masses[k] * jnp.exp2(peaks[k] - top)
                    peak = top
                peaks[k], masses[k] = peak, mass
        for k in range(len(uppers)):
            out_ref[k:k + 1, :] = peaks[k] + jnp.log(masses[k]) * LOG2E

    out_ref[len(uppers):len(uppers) + 1, :own] = partner_ref[...]


def document_ids(shape, axis, first, own_rows, masks, start=0):
    at = lax.broadcasted_iota(jnp.int32, shape, axis) + start
    shift = own_rows.bit_length() - 1
    piece = at >> shift
    device = first ^ (piece & 1)
    for s, mask in enumerate(masks):
        device = device ^ (((piece >> (1 + s)) & 1) * mask)
    return (device * own_rows + (at & (own_rows - 1))).astype(jnp.float32)


def grads_kernel(pieces, uppers, own_rows, masks, *refs):
    me_ref = refs[0]
    groups = pieces // 2
    stat_refs = refs[1:1 + groups]
    v_refs = refs[1 + groups:1 + groups + pieces]
    w_refs = refs[1 + groups + pieces:1 + groups + 2 * pieces]
    out_refs = refs[1 + groups + 2 * pieces:1 + 2 * groups + 2 * pieces]
    v_ref, w_ref, score_ref, col_ref = refs[1 + 2 * groups + 2 * pieces:]
    load_tile(v_refs, v_ref)
    load_tile(w_refs, w_ref)
    total = v_ref.shape[0]
    block = block_of(total)
    chip_rows = total // groups
    count = len(uppers)
    scales = [logit_gain * m ** -0.5 for m in uppers]
    me = me_ref[0]
    lead = (me & 1) == 0

    parts = []
    partners = []
    for j, ref in enumerate(stat_refs):
        parts.append(jnp.concatenate(
            [ref[:, (i ^ j) * chip_rows:((i ^ j) + 1) * chip_rows] for i in range(groups)], axis=1))
        partners.append(ref[count:count + 1, :chip_rows])
    peak = functools.reduce(jnp.maximum, parts)
    mass = functools.reduce(lambda a, b: a + b, [jnp.exp2(part - peak) for part in parts])
    totals = peak + jnp.log(mass) * LOG2E
    partner_row = jnp.concatenate(partners, axis=1)
    packed = jnp.concatenate(
        [totals[:count], partner_row, jnp.zeros((LANES - count - 1, total), jnp.float32)], axis=0)
    col_ref[...] = packed.T
    zero_or = lambda keep, x: jnp.where(keep, x, jnp.zeros_like(x))
    document_row = document_ids((1, total), 1, me | 1, own_rows, masks)
    id_row = jnp.where(lead, document_row, partner_row)
    shifts = [math.log2(s) for s in scales]
    total_rows = [zero_or(jnp.logical_not(lead), totals[k:k + 1]) - shifts[k] for k in range(count)]

    narrow = [m for m in uppers if m <= LANES]
    for step in range(total // block):
        rows = pl.ds(step * block, block)
        document_col = document_ids((block, 1), 0, me | 1, own_rows, masks, step * block)
        id_col = jnp.where(lead, col_ref[rows, count:count + 1], document_col)
        hit = id_col == id_row
        for k, s in enumerate(prefix_scores(v_ref, w_ref, rows, uppers)):
            score_ref[k] = s
        running = None
        stack = []
        for k in reversed(range(count)):
            gain = scales[k] * LOG2E
            total_col = zero_or(lead, col_ref[rows, k:k + 1])
            weight = jnp.exp2(score_ref[k] * gain - total_col - total_rows[k])
            weight = weight - jnp.where(hit, scales[k], 0.0)
            running = weight if running is None else running + weight
            band = running.astype(jnp.bfloat16)
            if k >= len(narrow):
                lower, upper = uppers[k - 1], uppers[k]
                product = jnp.dot(band, w_ref[:, lower:upper], preferred_element_type=jnp.float32)
                store(out_refs, product, step * block, lower, upper, chip_rows)
            else:
                stack.append(band)
        product = jnp.dot(
            jnp.concatenate(stack, axis=0), w_ref[:, :LANES], preferred_element_type=jnp.float32)
        lane = lax.broadcasted_iota(jnp.int32, (block, LANES), 1)
        chosen = product[:block]
        for at_stack in range(1, len(stack)):
            k = len(narrow) - 1 - at_stack
            chosen = jnp.where(
                lane < uppers[k], product[at_stack * block:(at_stack + 1) * block], chosen)
        store(out_refs, chosen, step * block, 0, LANES, chip_rows)


def rows_of(refs, lower, upper):
    return jnp.concatenate([ref[:, lower:upper] for ref in refs], axis=0)


def subtile_scores(v_refs, w_refs, uppers):
    narrow = [m for m in uppers if m <= LANES]
    left, right = rows_of(v_refs, 0, LANES), rows_of(w_refs, 0, LANES)
    slim = right.shape[0] < 2 * LANES
    head = right if slim else left
    count = head.shape[0]
    lane = lax.broadcasted_iota(jnp.int32, head.shape, 1)
    masked = jnp.concatenate(
        [jnp.where(lane < m, head, jnp.zeros_like(head)) for m in narrow], axis=0)
    if slim:
        stacked = transposed_dot(left, masked)
        parts = [stacked[:, k * count:(k + 1) * count] for k in range(len(narrow))]
    else:
        stacked = transposed_dot(masked, right)
        parts = [stacked[k * count:(k + 1) * count] for k in range(len(narrow))]
    yield from parts
    lower, running = narrow[-1], parts[-1]
    for upper in uppers[len(narrow):]:
        running = running + transposed_dot(
            rows_of(v_refs, lower, upper), rows_of(w_refs, lower, upper))
        yield running
        lower = upper


def subtile(lead, v_refs, w_refs, uppers, refs):
    power_ref, col_ref, line_ref = refs
    gains = [logit_gain * m ** -0.5 * LOG2E for m in uppers]
    count, across = power_ref.shape[1:]

    @pl.when(lead)
    def _():
        lane = lax.broadcasted_iota(jnp.int32, (count, LANES), 1)
        both = jnp.where(lane < STATS, 0.0, 1.0)
        for k, s in enumerate(subtile_scores(v_refs, w_refs, uppers)):
            logits = s * gains[k]
            peak = jnp.max(logits, axis=1, keepdims=True)
            power = jnp.exp2(logits - peak)
            power_ref[k] = power
            both = jnp.where(lane == k, peak, both)
            both = jnp.where(lane == STATS + k, jnp.sum(power, axis=1, keepdims=True), both)
        col_ref[...] = both
        line_ref[:, :count] = both.T[:2 * STATS]

    @pl.when(jnp.logical_not(lead))
    def _():
        line_ref[:STATS, :] = jnp.zeros((STATS, line_ref.shape[1]), jnp.float32)
        line_ref[STATS:, :] = jnp.ones((STATS, line_ref.shape[1]), jnp.float32)
        for k, s in enumerate(subtile_scores(v_refs, w_refs, uppers)):
            logits = s * gains[k]
            peak = jnp.max(logits, axis=0, keepdims=True)
            power = jnp.exp2(logits - peak)
            power_ref[k] = power
            line_ref[k:k + 1, :across] = peak
            line_ref[STATS + k:STATS + k + 1, :across] = jnp.sum(power, axis=0, keepdims=True)


def log_sum(pairs):
    top = functools.reduce(jnp.maximum, [peak for peak, _ in pairs])
    mass = functools.reduce(
        lambda a, b: a + b, [mass * jnp.exp2(peak - top) for peak, mass in pairs])
    return top + jnp.log(mass) * LOG2E


def tile_kernel(span, counts, uppers, own_rows, finish, *refs):
    groups = len(counts)
    shapes = subtiles(groups)
    tiles = [shapes[i] for i in span]
    r0, r1, c0, c1 = extent(tiles)
    me_ref, partner_ref = refs[:2]
    at = 2 + sum(counts[r0:r1])
    v_refs, w_refs = refs[2:at], refs[at:at + sum(counts[c0:c1])]
    at += sum(counts[c0:c1])
    earlier = refs[at:at + finish]
    outs = refs[at + finish:]
    lead = (me_ref[0] & 1) == 0
    for i, (t0, t1, u0, u1) in enumerate(tiles):
        subtile(
            lead, v_refs[sum(counts[r0:t0]):sum(counts[r0:t1])],
            w_refs[sum(counts[c0:u0]):sum(counts[c0:u1])], uppers, outs[3 * i:3 * i + 3])
    if not finish:
        outs[-1][...] = partner_ref[...]
        return
    stats_ref = outs[-1]
    every = [*earlier, *outs[2:3 * len(tiles):3]]
    segments = segments_of(groups)
    chip_rows = 2 * own_rows

    def merge(axis):
        for s0, s1 in segments:
            pairs = []
            for shape, line in zip(shapes, every):
                low, high = shape[axis:axis + 2]
                if low <= s0 and s1 <= high:
                    at = slice((s0 - low) * chip_rows, (s1 - low) * chip_rows)
                    pairs.append((line[:STATS, at], line[STATS:, at]))
            stats_ref[:, s0 * chip_rows:s1 * chip_rows] = log_sum(pairs)

    pl.when(lead)(lambda: merge(0))
    pl.when(jnp.logical_not(lead))(lambda: merge(2))

    count = len(uppers)
    stats_ref[count:count + 1, :chip_rows] = partner_ref[...]


def segments_of(groups):
    low, middle = groups // 2, groups // 2 + groups // 4
    return [(0, low), (low, middle), (middle, groups)]


def subtiles(groups):
    (_, low), (_, middle), _ = segments_of(groups)
    return [(0, low, 0, low), (low, middle, 0, low), (0, middle, low, middle),
            (middle, groups, 0, middle), (0, groups, middle, groups)]


def extent(tiles):
    first, second, third, fourth = zip(*tiles)
    return min(first), max(second), min(third), max(fourth)


def band_setup(groups, uppers, own_rows, masks, me_ref, stat_refs):
    count = len(uppers)
    total = stat_refs[0].shape[1]
    chip_rows = total // groups
    me = me_ref[0]
    lead = (me & 1) == 0
    parts, partners = [], []
    for j, ref in enumerate(stat_refs):
        parts.append(jnp.concatenate(
            [ref[:, (i ^ j) * chip_rows:((i ^ j) + 1) * chip_rows] for i in range(groups)], axis=1))
        partners.append(ref[count:count + 1, :chip_rows])
    peak = functools.reduce(jnp.maximum, parts)
    mass = functools.reduce(lambda a, b: a + b, [jnp.exp2(part - peak) for part in parts])
    partner_row = jnp.concatenate(partners, axis=1)
    sub = lax.broadcasted_iota(jnp.int32, (STATS, total), 0)
    totals = peak + jnp.log(mass) * LOG2E
    for k in range(count):
        totals = jnp.where(sub == k, totals - math.log2(logit_gain * uppers[k] ** -0.5), totals)
    packed = jnp.concatenate(
        [totals[:count], partner_row, jnp.zeros((LANES - count - 1, total), jnp.float32)], axis=0)
    cols = packed.T
    id_row = jnp.where(
        lead, document_ids((1, total), 1, me | 1, own_rows, masks), partner_row)
    id_col = jnp.where(
        lead, cols[:, count:count + 1],
        document_ids((total, 1), 0, me | 1, own_rows, masks))
    return lead, totals, cols, id_row, id_col


def weights_of(segment, groups, setup, power_refs, col_refs, row_refs):
    lead, totals, cols, _, _ = setup
    chip_rows = totals.shape[1] // groups
    s0, s1 = segment
    strip = []
    for (r0, r1, c0, c1), power, col_peak, line in zip(
            subtiles(groups), power_refs, col_refs, row_refs):
        if r0 <= s0 and s1 <= r1:
            inner = slice((s0 - r0) * chip_rows, (s1 - r0) * chip_rows)
            outer = slice(s0 * chip_rows, s1 * chip_rows)
            across = slice(c0 * chip_rows, c1 * chip_rows)
            strip.append((
                c0, power, inner,
                jnp.where(lead, jnp.exp2(col_peak[inner, :] - cols[outer]), 1.0),
                jnp.where(lead, 1.0, jnp.exp2(line[:STATS, :(c1 - c0) * chip_rows] - totals[:, across]))))
    strip.sort(key=lambda item: item[0])
    return lambda k: jnp.concatenate([
        power[k, inner] * col_gain[:, k:k + 1] * row_gain[k:k + 1, :]
        for _, power, inner, col_gain, row_gain in strip], axis=1)


def last_band_kernel(groups, uppers, own_rows, masks, *refs):
    tiles = len(subtiles(groups))
    setup = band_setup(groups, uppers, own_rows, masks, refs[0], refs[1:1 + groups])
    at = 1 + groups
    power_refs, col_refs, row_refs = [refs[at + i * tiles:at + (i + 1) * tiles] for i in range(3)]
    segment = segments_of(groups)[-1]
    farthest = segment[1] - segment[0]
    w_refs, out_refs, after_ref = refs[at + 3 * tiles:-farthest - 1], refs[-farthest - 1:-1], refs[-1]
    _, totals, _, id_row, id_col = setup
    chip_rows = totals.shape[1] // groups
    k = len(uppers) - 1
    rows = slice(segment[0] * chip_rows, segment[1] * chip_rows)
    weight = weights_of(segment, groups, setup, power_refs, col_refs, row_refs)(k)
    weight = weight - jnp.where(id_col[rows] == id_row, logit_gain * uppers[k] ** -0.5, 0.0)
    after_ref[...] = weight
    product = jnp.dot(
        weight.astype(jnp.bfloat16), rows_of(w_refs, uppers[k - 1], uppers[k]),
        preferred_element_type=jnp.float32)
    store(out_refs, product, 0, 0, uppers[k] - uppers[k - 1], chip_rows)


def bands_kernel(groups, uppers, own_rows, masks, *refs):
    tiles = len(subtiles(groups))
    setup = band_setup(groups, uppers, own_rows, masks, refs[0], refs[1:1 + groups])
    at = 1 + groups
    power_refs, col_refs, row_refs = [refs[at + i * tiles:at + (i + 1) * tiles] for i in range(3)]
    segments = segments_of(groups)
    outs = groups + segments[-1][0]
    before_ref = refs[-outs - 1]
    w_refs, others, widest = refs[at + 3 * tiles:-outs - 1], refs[-outs:-outs + groups], refs[-outs + groups:]
    _, totals, _, id_row, id_col = setup
    chip_rows = totals.shape[1] // groups
    scales = [logit_gain * m ** -0.5 for m in uppers]
    last = len(uppers) - 1
    narrow = [k for k in range(last, -1, -1) if uppers[k] <= LANES]
    for block in (segments[1:], segments[:1]):
        first = block[0][0] * chip_rows
        rows = slice(first, block[-1][1] * chip_rows)
        height = rows.stop - first
        hit = id_col[rows] == id_row
        weights = [
            weights_of(segment, groups, setup, power_refs, col_refs, row_refs) for segment in block]
        tall = (block[0][1] - block[0][0]) * chip_rows
        running = weights[0](last) - jnp.where(hit[:tall], scales[last], 0.0)
        lower, upper = uppers[last - 1], uppers[last]
        product = jnp.dot(
            running.astype(jnp.bfloat16), rows_of(w_refs, lower, upper),
            preferred_element_type=jnp.float32)
        store(widest, product, first, 0, upper - lower, chip_rows)
        if len(block) > 1:
            running = jnp.concatenate([running, before_ref[...]], axis=0)
        stack = []
        for k in range(last - 1, -1, -1):
            weight = jnp.concatenate([part(k) for part in weights], axis=0)
            running = running + (weight - jnp.where(hit, scales[k], 0.0))
            band = running.astype(jnp.bfloat16)
            if k in narrow:
                stack.append(band)
                continue
            lower, upper = uppers[k - 1], uppers[k]
            product = jnp.dot(
                band, rows_of(w_refs, lower, upper), preferred_element_type=jnp.float32)
            store(others, product, first, lower, upper, chip_rows)
        product = jnp.dot(
            jnp.concatenate(stack, axis=0), rows_of(w_refs, 0, LANES),
            preferred_element_type=jnp.float32)
        lane = lax.broadcasted_iota(jnp.int32, (height, LANES), 1)
        chosen = product[:height]
        for i in range(1, len(stack)):
            chosen = jnp.where(
                lane < uppers[narrow[i]], product[i * height:(i + 1) * height], chosen)
        store(others, chosen, first, 0, LANES, chip_rows)


def store(out_refs, value, first_row, lower, upper, chip_rows):
    for at in range(0, value.shape[0], chip_rows):
        ref = out_refs[(first_row + at) // chip_rows]
        ref[:, lower:upper] = value[at:at + chip_rows].astype(ref.dtype)


def on_device(queries, documents, partner):
    own_rows, feature_dim = queries.shape
    uppers = width_list(feature_dim)
    dp_size, rep_size = lax.axis_size("dp"), lax.axis_size("rep")
    devices = dp_size * rep_size
    bits = devices.bit_length() - 1
    assert rep_size == 2 and devices == 1 << bits and bits % 2 == 1
    stages = (bits - 1) // 2
    groups = 1 << stages
    pieces = 2 * groups
    query_masks = [1 << (2 * s + 1) for s in range(stages)]
    document_masks = [1 << (2 * s + 2) for s in range(stages)]
    total = pieces * own_rows
    chip_rows = 2 * own_rows

    role = lax.axis_index("rep")
    me = (lax.axis_index("dp") * rep_size + role).astype(jnp.int32).reshape(1)
    lead = role == 0

    def exchange(x, masks_of):
        return lax.ppermute(x, AXES, [(i, i ^ masks_of(i)) for i in range(devices)])

    def swap(x):
        return exchange(x, lambda i: 1)

    def along(x, stage):
        return exchange(x, lambda i: document_masks[stage] if i & 1 else query_masks[stage])

    mine = jnp.where(lead, queries, documents)
    other = jnp.where(lead, documents, queries)
    got = swap(other)
    small = WIDTHS * total * total * 4 <= 16 << 20
    cut = own_rows - 16 if small and own_rows >= 32 else own_rows
    v = {0: [mine, got]}
    w = {0: [swap(mine), other]}
    for stage in reversed(range(stages)):
        for j in sorted(v):
            parts = v[j]
            if j == 0 and stage == stages - 1 and cut < own_rows:
                parts = [mine, got[:cut], got[cut:]]
            v[j | 1 << stage] = [
                along(part, stage) for part in parts]
    for j in range(1, groups):
        w[j] = [swap(part) for part in v[j]]
    counts = [len(v[j]) for j in range(groups)]
    v_list = [part for j in range(groups) for part in v[j]]
    w_list = [part for j in range(groups) for part in w[j]]

    own_partner = partner.astype(jnp.float32).reshape(1, own_rows)
    far_partner = swap(own_partner)
    chip_partner = jnp.where(
        lead,
        jnp.concatenate([own_partner, far_partner], axis=1),
        jnp.concatenate([far_partner, own_partner], axis=1))

    vmem = pl.BlockSpec(memory_space=pltpu.VMEM)
    smem = pl.BlockSpec(memory_space=pltpu.SMEM)

    def query_mask(j):
        return sum(mask for s, mask in enumerate(query_masks) if j >> s & 1)

    def gathered(stats):
        return [stats] + [exchange(stats, lambda i: query_mask(j)) for j in range(1, groups)]

    shape = lambda *dims: jax.ShapeDtypeStruct(dims, jnp.float32)

    def gradient_shapes(columns):
        return [
            jax.ShapeDtypeStruct((chip_rows, columns), jnp.bfloat16 if j & 1 else jnp.float32)
            for j in range(groups)]

    if not small:
        limit = 60 << 20
        stats = pl.pallas_call(
            functools.partial(stats_kernel, pieces, uppers),
            out_shape=shape(STATS, total),
            in_specs=[smem] + [vmem] * (1 + 2 * pieces),
            out_specs=vmem,
            scratch_shapes=[
                pltpu.VMEM((total, feature_dim), jnp.bfloat16),
                pltpu.VMEM((total, feature_dim), jnp.bfloat16),
                pltpu.VMEM((total, LANES), jnp.float32),
            ],
            compiler_params=pltpu.CompilerParams(vmem_limit_bytes=limit),
            name="tile_stats",
        )(me, chip_partner, *v_list, *w_list)
        whole = pl.pallas_call(
            functools.partial(grads_kernel, pieces, uppers, own_rows, document_masks),
            out_shape=gradient_shapes(feature_dim),
            in_specs=[smem] + [vmem] * (groups + 2 * pieces),
            out_specs=[vmem] * groups,
            scratch_shapes=[
                pltpu.VMEM((total, feature_dim), jnp.bfloat16),
                pltpu.VMEM((total, feature_dim), jnp.bfloat16),
                pltpu.VMEM((WIDTHS, block_of(total), total), jnp.float32),
                pltpu.VMEM((total, LANES), jnp.float32),
            ],
            compiler_params=pltpu.CompilerParams(vmem_limit_bytes=limit),
            name="tile_grads",
        )(me, *gathered(stats), *v_list, *w_list)
        chunks = [whole]
    else:
        shapes = subtiles(groups)
        limit = 20 << 20
        params = pltpu.CompilerParams(vmem_limit_bytes=limit)

        def tile(span, partner_row, earlier=()):
            first, end, left, right = extent([shapes[i] for i in span])
            operands = v_list[sum(counts[:first]):sum(counts[:end])]
            operands += w_list[sum(counts[:left]):sum(counts[:right])]
            stat_shapes = [shape(STATS, total)] if earlier else [shape(1, chip_rows)]
            result, area = [], 0
            for i in span:
                r0, r1, c0, c1 = shapes[i]
                tall, wide = (r1 - r0) * chip_rows, (c1 - c0) * chip_rows
                area += tall * wide
                result += [shape(WIDTHS, tall, wide), shape(tall, LANES),
                           shape(2 * STATS, max(tall, wide))]
            *arrays, last_array = pl.pallas_call(
                functools.partial(
                    tile_kernel, span, counts, uppers, own_rows, len(earlier)),
                out_shape=result + stat_shapes,
                in_specs=[smem] + [vmem] * (1 + len(operands) + len(earlier)),
                out_specs=[vmem] * (len(result) + 1),
                compiler_params=params,
                cost_estimate=pl.CostEstimate(
                    flops=6 * area * feature_dim, transcendentals=0,
                    bytes_accessed=2 * total * feature_dim),
            )(me, partner_row, *operands, *[one[2] for one in earlier])
            return [arrays[3 * i:3 * i + 3] for i in range(len(span))], last_array

        done, chip_partner = tile([0], chip_partner)
        for at in (1, 2, 3):
            more, chip_partner = tile([at], chip_partner)
            done += more
        more, stats = tile([4], chip_partner, done)
        done += more
        common = [me, *gathered(stats), *[t[0] for t in done], *[t[1] for t in done],
                  *[t[2] for t in done], *w_list]
        near = segments_of(groups)[-1][0]
        widest = feature_dim - uppers[-2]

        def bands(kernel, more, outs):
            return pl.pallas_call(
                functools.partial(kernel, groups, uppers, own_rows, document_masks),
                out_shape=outs,
                in_specs=[smem] + [vmem] * (len(common) - 1 + len(more)),
                out_specs=[vmem] * len(outs),
                compiler_params=params,
                cost_estimate=pl.CostEstimate(
                    flops=2 * total * total * feature_dim, transcendentals=0,
                    bytes_accessed=4 * total * feature_dim),
            )(*common, *more)

        *far_ones, running = bands(
            last_band_kernel, [],
            gradient_shapes(widest)[near:] + [shape((groups - near) * chip_rows, total)])
        rest = bands(
            bands_kernel, [running], gradient_shapes(uppers[-2]) + gradient_shapes(widest)[:near])
        chunks = [[*rest[groups:], *far_ones], rest[:groups]]

    mine_parts, other_parts = [], []
    for c, chunk in enumerate(chunks):
        partial = dict(enumerate(chunk))
        for stage in range(stages - 1):
            step = 1 << stage
            for j in sorted([j for j in partial if j & step], reverse=True):
                arrived = along(partial.pop(j).astype(jnp.bfloat16), stage)
                partial[j ^ step] = partial[j ^ step] + arrived.astype(jnp.float32)
                if stage == stages - 2 and j ^ step:
                    partial[j ^ step] = partial[j ^ step].astype(jnp.bfloat16)
        stage = stages - 1
        outgoing = partial[1 << stage]
        kept = partial[0]
        if c < len(chunks) - 1:
            arrived = along(outgoing, stage)
            kept = kept + arrived.astype(jnp.float32)
            mine_parts.append(kept[:own_rows])
            other_parts.append(swap(kept[own_rows:]))
        else:
            far = lambda i: document_masks[stage] ^ 1 if i & 1 else query_masks[stage] ^ 1
            near_arrived = along(outgoing[:own_rows], stage)
            far_arrived = exchange(outgoing[own_rows:], far)
            ours, theirs = lax.optimization_barrier((kept[:own_rows], kept[own_rows:]))
            mine_parts.append(ours + near_arrived.astype(jnp.float32))
            other_parts.append(swap(theirs) + far_arrived.astype(jnp.float32))
    mine_parts, other_parts = mine_parts[::-1], other_parts[::-1]
    ours = jnp.concatenate(mine_parts, axis=1)
    theirs = jnp.concatenate(other_parts, axis=1)
    return jnp.where(lead, ours, theirs), jnp.where(lead, theirs, ours)


def solution(mesh):
    return jax.shard_map(
        on_device,
        mesh=mesh,
        in_specs=(P(AXES, None), P(AXES, None), P(AXES)),
        out_specs=(P(AXES, None), P(AXES, None)),
        check_vma=False,
    )
```

```python
import functools
import math

import jax
import jax.numpy as jnp
from jax import lax
from jax.experimental import pallas as pl
from jax.experimental.pallas import tpu as pltpu
from jax.sharding import PartitionSpec as P


WIDTHS = 9
AXES = ("dp", "rep")
LOG2E = 1.4426950408889634
STATS = 16
LANES = 128


logit_gain = 3.0


def width_list(feature_dim):
    return [feature_dim >> WIDTHS - 1 - nested for nested in range(WIDTHS)]


def transposed_dot(a, b):
    return lax.dot_general(a, b, (((1,), (1,)), ((), ())), preferred_element_type=jnp.float32)


def prefix_scores(v_ref, w_ref, rows, uppers):
    narrow = [m for m in uppers if m <= LANES]
    count = rows.size
    head = v_ref[rows, :LANES]
    lane = lax.broadcasted_iota(jnp.int32, head.shape, 1)
    masked = [jnp.where(lane < m, head, jnp.zeros_like(head)) for m in narrow]
    stacked = transposed_dot(jnp.concatenate(masked, axis=0), w_ref[:, :LANES])
    result = [stacked[k * count:(k + 1) * count] for k in range(len(narrow))]
    lower = narrow[-1]
    for upper in uppers[len(narrow):]:
        part = transposed_dot(v_ref[rows, lower:upper], w_ref[:, lower:upper])
        result.append(result[-1] + part)
        lower = upper
    return result


def block_of(total):
    return min(total, 256)


def load_tile(refs, scratch):
    at = 0
    for ref in refs:
        scratch[at:at + ref.shape[0], :] = ref[...]
        at += ref.shape[0]


def stats_kernel(pieces, uppers, *refs):
    role_ref, partner_ref = refs[:2]
    v_refs, w_refs = refs[2:2 + pieces], refs[2 + pieces:2 + 2 * pieces]
    out_ref, v_ref, w_ref, col_ref = refs[2 + 2 * pieces:]
    load_tile(v_refs, v_ref)
    load_tile(w_refs, w_ref)
    total = v_ref.shape[0]
    block = block_of(total)
    steps = total // block
    gains = [logit_gain * m ** -0.5 * LOG2E for m in uppers]
    own = partner_ref.shape[1]
    out_ref[...] = jnp.zeros_like(out_ref)

    @pl.when((role_ref[0] & 1) == 0)
    def _():
        for step in range(steps):
            rows = pl.ds(step * block, block)
            col_ref[rows, :] = jnp.zeros((block, LANES), jnp.float32)
            for k, s in enumerate(prefix_scores(v_ref, w_ref, rows, uppers)):
                logits = s * gains[k]
                peak = jnp.max(logits, axis=1, keepdims=True)
                mass = jnp.sum(jnp.exp2(logits - peak), axis=1, keepdims=True)
                col_ref[rows, k:k + 1] = peak + jnp.log(mass) * LOG2E
        out_ref[...] = col_ref[...].T[:STATS]

    @pl.when((role_ref[0] & 1) != 0)
    def _():
        peaks, masses = [None] * len(uppers), [None] * len(uppers)
        for step in range(steps):
            rows = pl.ds(step * block, block)
            for k, s in enumerate(prefix_scores(v_ref, w_ref, rows, uppers)):
                logits = s * gains[k]
                peak = jnp.max(logits, axis=0, keepdims=True)
                mass = jnp.sum(jnp.exp2(logits - peak), axis=0, keepdims=True)
                if step:
                    top = jnp.maximum(peak, peaks[k])
                    mass = mass * jnp.exp2(peak - top) + masses[k] * jnp.exp2(peaks[k] - top)
                    peak = top
                peaks[k], masses[k] = peak, mass
        for k in range(len(uppers)):
            out_ref[k:k + 1, :] = peaks[k] + jnp.log(masses[k]) * LOG2E

    out_ref[len(uppers):len(uppers) + 1, :own] = partner_ref[...]


def document_ids(shape, axis, first, own_rows, masks, start=0):
    at = lax.broadcasted_iota(jnp.int32, shape, axis) + start
    shift = own_rows.bit_length() - 1
    piece = at >> shift
    device = first ^ (piece & 1)
    for s, mask in enumerate(masks):
        device = device ^ (((piece >> (1 + s)) & 1) * mask)
    return (device * own_rows + (at & (own_rows - 1))).astype(jnp.float32)


def grads_kernel(pieces, uppers, own_rows, masks, *refs):
    me_ref = refs[0]
    groups = pieces // 2
    stat_refs = refs[1:1 + groups]
    v_refs = refs[1 + groups:1 + groups + pieces]
    w_refs = refs[1 + groups + pieces:1 + groups + 2 * pieces]
    out_refs = refs[1 + groups + 2 * pieces:1 + 2 * groups + 2 * pieces]
    v_ref, w_ref, score_ref, col_ref = refs[1 + 2 * groups + 2 * pieces:]
    load_tile(v_refs, v_ref)
    load_tile(w_refs, w_ref)
    total = v_ref.shape[0]
    block = block_of(total)
    chip_rows = total // groups
    count = len(uppers)
    scales = [logit_gain * m ** -0.5 for m in uppers]
    me = me_ref[0]
    lead = (me & 1) == 0

    parts = []
    partners = []
    for j, ref in enumerate(stat_refs):
        parts.append(jnp.concatenate(
            [ref[:, (i ^ j) * chip_rows:((i ^ j) + 1) * chip_rows] for i in range(groups)], axis=1))
        partners.append(ref[count:count + 1, :chip_rows])
    peak = functools.reduce(jnp.maximum, parts)
    mass = functools.reduce(lambda a, b: a + b, [jnp.exp2(part - peak) for part in parts])
    totals = peak + jnp.log(mass) * LOG2E
    partner_row = jnp.concatenate(partners, axis=1)
    packed = jnp.concatenate(
        [totals[:count], partner_row, jnp.zeros((LANES - count - 1, total), jnp.float32)], axis=0)
    col_ref[...] = packed.T
    zero_or = lambda keep, x: jnp.where(keep, x, jnp.zeros_like(x))
    document_row = document_ids((1, total), 1, me | 1, own_rows, masks)
    id_row = jnp.where(lead, document_row, partner_row)
    shifts = [math.log2(s) for s in scales]
    total_rows = [zero_or(jnp.logical_not(lead), totals[k:k + 1]) - shifts[k] for k in range(count)]

    narrow = [m for m in uppers if m <= LANES]
    for step in range(total // block):
        rows = pl.ds(step * block, block)
        document_col = document_ids((block, 1), 0, me | 1, own_rows, masks, step * block)
        id_col = jnp.where(lead, col_ref[rows, count:count + 1], document_col)
        hit = id_col == id_row
        for k, s in enumerate(prefix_scores(v_ref, w_ref, rows, uppers)):
            score_ref[k] = s
        running = None
        stack = []
        for k in reversed(range(count)):
            gain = scales[k] * LOG2E
            total_col = zero_or(lead, col_ref[rows, k:k + 1])
            weight = jnp.exp2(score_ref[k] * gain - total_col - total_rows[k])
            weight = weight - jnp.where(hit, scales[k], 0.0)
            running = weight if running is None else running + weight
            band = running.astype(jnp.bfloat16)
            if k >= len(narrow):
                lower, upper = uppers[k - 1], uppers[k]
                product = jnp.dot(band, w_ref[:, lower:upper], preferred_element_type=jnp.float32)
                store(out_refs, product, step * block, lower, upper, chip_rows)
            else:
                stack.append(band)
        product = jnp.dot(
            jnp.concatenate(stack, axis=0), w_ref[:, :LANES], preferred_element_type=jnp.float32)
        lane = lax.broadcasted_iota(jnp.int32, (block, LANES), 1)
        chosen = product[:block]
        for at_stack in range(1, len(stack)):
            k = len(narrow) - 1 - at_stack
            chosen = jnp.where(
                lane < uppers[k], product[at_stack * block:(at_stack + 1) * block], chosen)
        store(out_refs, chosen, step * block, 0, LANES, chip_rows)


def rows_of(refs, lower, upper):
    return jnp.concatenate([ref[:, lower:upper] for ref in refs], axis=0)


def subtile_scores(v_refs, w_refs, uppers):
    narrow = [m for m in uppers if m <= LANES]
    left, right = rows_of(v_refs, 0, LANES), rows_of(w_refs, 0, LANES)
    slim = right.shape[0] < 2 * LANES
    head = right if slim else left
    count = head.shape[0]
    lane = lax.broadcasted_iota(jnp.int32, head.shape, 1)
    masked = jnp.concatenate(
        [jnp.where(lane < m, head, jnp.zeros_like(head)) for m in narrow], axis=0)
    if slim:
        stacked = transposed_dot(left, masked)
        parts = [stacked[:, k * count:(k + 1) * count] for k in range(len(narrow))]
    else:
        stacked = transposed_dot(masked, right)
        parts = [stacked[k * count:(k + 1) * count] for k in range(len(narrow))]
    yield from parts
    lower, running = narrow[-1], parts[-1]
    for upper in uppers[len(narrow):]:
        running = running + transposed_dot(
            rows_of(v_refs, lower, upper), rows_of(w_refs, lower, upper))
        yield running
        lower = upper


def subtile(lead, v_refs, w_refs, uppers, refs):
    power_ref, col_ref, line_ref = refs
    gains = [logit_gain * m ** -0.5 * LOG2E for m in uppers]
    count, across = power_ref.shape[1:]

    @pl.when(lead)
    def _():
        lane = lax.broadcasted_iota(jnp.int32, (count, LANES), 1)
        both = jnp.where(lane < STATS, 0.0, 1.0)
        for k, s in enumerate(subtile_scores(v_refs, w_refs, uppers)):
            logits = s * gains[k]
            peak = jnp.max(logits, axis=1, keepdims=True)
            power = jnp.exp2(logits - peak)
            power_ref[k] = power
            both = jnp.where(lane == k, peak, both)
            both = jnp.where(lane == STATS + k, jnp.sum(power, axis=1, keepdims=True), both)
        col_ref[...] = both
        line_ref[:, :count] = both.T[:2 * STATS]

    @pl.when(jnp.logical_not(lead))
    def _():
        line_ref[:STATS, :] = jnp.zeros((STATS, line_ref.shape[1]), jnp.float32)
        line_ref[STATS:, :] = jnp.ones((STATS, line_ref.shape[1]), jnp.float32)
        for k, s in enumerate(subtile_scores(v_refs, w_refs, uppers)):
            logits = s * gains[k]
            peak = jnp.max(logits, axis=0, keepdims=True)
            power = jnp.exp2(logits - peak)
            power_ref[k] = power
            line_ref[k:k + 1, :across] = peak
            line_ref[STATS + k:STATS + k + 1, :across] = jnp.sum(power, axis=0, keepdims=True)


def log_sum(pairs):
    top = functools.reduce(jnp.maximum, [peak for peak, _ in pairs])
    mass = functools.reduce(
        lambda a, b: a + b, [mass * jnp.exp2(peak - top) for peak, mass in pairs])
    return top + jnp.log(mass) * LOG2E


def tile_kernel(span, counts, uppers, own_rows, finish, *refs):
    groups = len(counts)
    shapes = subtiles(groups)
    tiles = [shapes[i] for i in span]
    r0, r1, c0, c1 = extent(tiles)
    me_ref, partner_ref, far_ref = refs[:3]
    at = 3 + sum(counts[r0:r1])
    v_refs, w_refs = refs[3:at], refs[at:at + sum(counts[c0:c1])]
    at += sum(counts[c0:c1])
    earlier = refs[at:at + finish]
    outs = refs[at + finish:]
    lead = (me_ref[0] & 1) == 0
    for i, (t0, t1, u0, u1) in enumerate(tiles):
        subtile(
            lead, v_refs[sum(counts[r0:t0]):sum(counts[r0:t1])],
            w_refs[sum(counts[c0:u0]):sum(counts[c0:u1])], uppers, outs[3 * i:3 * i + 3])
    if not finish:
        if span[0] == 0:
            near, far = partner_ref[...].astype(jnp.float32), far_ref[...].astype(jnp.float32)
            outs[-1][:, :own_rows] = jnp.where(lead, near, far)
            outs[-1][:, own_rows:] = jnp.where(lead, far, near)
        else:
            outs[-1][...] = partner_ref[...]
        return
    stats_ref = outs[-1]
    every = [*earlier, *outs[2:3 * len(tiles):3]]
    segments = segments_of(groups)
    chip_rows = 2 * own_rows

    def merge(axis):
        for s0, s1 in segments:
            pairs = []
            for shape, line in zip(shapes, every):
                low, high = shape[axis:axis + 2]
                if low <= s0 and s1 <= high:
                    at = slice((s0 - low) * chip_rows, (s1 - low) * chip_rows)
                    pairs.append((line[:STATS, at], line[STATS:, at]))
            stats_ref[:, s0 * chip_rows:s1 * chip_rows] = log_sum(pairs)

    pl.when(lead)(lambda: merge(0))
    pl.when(jnp.logical_not(lead))(lambda: merge(2))

    count = len(uppers)
    stats_ref[count:count + 1, :chip_rows] = partner_ref[...]


def segments_of(groups):
    low, middle = groups // 2, groups // 2 + groups // 4
    return [(0, low), (low, middle), (middle, groups)]


def subtiles(groups):
    (_, low), (_, middle), _ = segments_of(groups)
    return [(0, low, 0, low), (low, middle, 0, low), (0, middle, low, middle),
            (middle, groups, 0, middle), (0, groups, middle, groups)]


def extent(tiles):
    first, second, third, fourth = zip(*tiles)
    return min(first), max(second), min(third), max(fourth)


def band_setup(groups, uppers, own_rows, masks, me_ref, stat_refs):
    count = len(uppers)
    total = stat_refs[0].shape[1]
    chip_rows = total // groups
    me = me_ref[0]
    lead = (me & 1) == 0
    own, first, second, swapped = [ref[...] for ref in stat_refs]
    values = [own, jnp.where(lead, swapped, first), second, jnp.where(lead, first, swapped)]
    parts, partners = [], []
    for j, value in enumerate(values):
        parts.append(jnp.concatenate(
            [value[:, (i ^ j) * chip_rows:((i ^ j) + 1) * chip_rows] for i in range(groups)], axis=1))
        partners.append(value[count:count + 1, :chip_rows])
    peak = functools.reduce(jnp.maximum, parts)
    mass = functools.reduce(lambda a, b: a + b, [jnp.exp2(part - peak) for part in parts])
    partner_row = jnp.concatenate(partners, axis=1)
    sub = lax.broadcasted_iota(jnp.int32, (STATS, total), 0)
    totals = peak + jnp.log(mass) * LOG2E
    for k in range(count):
        totals = jnp.where(sub == k, totals - math.log2(logit_gain * uppers[k] ** -0.5), totals)
    packed = jnp.concatenate(
        [totals[:count], partner_row, jnp.zeros((LANES - count - 1, total), jnp.float32)], axis=0)
    cols = packed.T
    id_row = jnp.where(
        lead, document_ids((1, total), 1, me | 1, own_rows, masks), partner_row)
    id_col = jnp.where(
        lead, cols[:, count:count + 1],
        document_ids((total, 1), 0, me | 1, own_rows, masks))
    return lead, totals, cols, id_row, id_col


def weights_of(segment, groups, setup, power_refs, col_refs, row_refs):
    lead, totals, cols, _, _ = setup
    chip_rows = totals.shape[1] // groups
    s0, s1 = segment
    strip = []
    for (r0, r1, c0, c1), power, col_peak, line in zip(
            subtiles(groups), power_refs, col_refs, row_refs):
        if r0 <= s0 and s1 <= r1:
            inner = slice((s0 - r0) * chip_rows, (s1 - r0) * chip_rows)
            outer = slice(s0 * chip_rows, s1 * chip_rows)
            across = slice(c0 * chip_rows, c1 * chip_rows)
            strip.append((
                c0, power, inner,
                jnp.where(lead, jnp.exp2(col_peak[inner, :] - cols[outer]), 1.0),
                jnp.where(lead, 1.0, jnp.exp2(line[:STATS, :(c1 - c0) * chip_rows] - totals[:, across]))))
    strip.sort(key=lambda item: item[0])
    return lambda k: jnp.concatenate([
        power[k, inner] * col_gain[:, k:k + 1] * row_gain[k:k + 1, :]
        for _, power, inner, col_gain, row_gain in strip], axis=1)


def last_band_kernel(groups, uppers, own_rows, masks, *refs):
    tiles = len(subtiles(groups))
    setup = band_setup(groups, uppers, own_rows, masks, refs[0], refs[1:1 + groups])
    at = 1 + groups
    power_refs, col_refs, row_refs = [refs[at + i * tiles:at + (i + 1) * tiles] for i in range(3)]
    segment = segments_of(groups)[-1]
    farthest = segment[1] - segment[0]
    w_refs, out_refs, after_ref = refs[at + 3 * tiles:-farthest - 1], refs[-farthest - 1:-1], refs[-1]
    _, totals, _, id_row, id_col = setup
    chip_rows = totals.shape[1] // groups
    k = len(uppers) - 1
    rows = slice(segment[0] * chip_rows, segment[1] * chip_rows)
    weight = weights_of(segment, groups, setup, power_refs, col_refs, row_refs)(k)
    weight = weight - jnp.where(id_col[rows] == id_row, logit_gain * uppers[k] ** -0.5, 0.0)
    after_ref[...] = weight
    product = jnp.dot(
        weight.astype(jnp.bfloat16), rows_of(w_refs, uppers[k - 1], uppers[k]),
        preferred_element_type=jnp.float32)
    store(out_refs, product, 0, 0, uppers[k] - uppers[k - 1], chip_rows)


def bands_kernel(groups, uppers, own_rows, masks, *refs):
    tiles = len(subtiles(groups))
    setup = band_setup(groups, uppers, own_rows, masks, refs[0], refs[1:1 + groups])
    at = 1 + groups
    power_refs, col_refs, row_refs = [refs[at + i * tiles:at + (i + 1) * tiles] for i in range(3)]
    segments = segments_of(groups)
    outs = groups + segments[-1][0]
    before_ref = refs[-outs - 1]
    w_refs, others, widest = refs[at + 3 * tiles:-outs - 1], refs[-outs:-outs + groups], refs[-outs + groups:]
    _, totals, _, id_row, id_col = setup
    chip_rows = totals.shape[1] // groups
    scales = [logit_gain * m ** -0.5 for m in uppers]
    last = len(uppers) - 1
    narrow = [k for k in range(last, -1, -1) if uppers[k] <= LANES]
    for block in (segments[1:], segments[:1]):
        first = block[0][0] * chip_rows
        rows = slice(first, block[-1][1] * chip_rows)
        height = rows.stop - first
        hit = id_col[rows] == id_row
        weights = [
            weights_of(segment, groups, setup, power_refs, col_refs, row_refs) for segment in block]
        tall = (block[0][1] - block[0][0]) * chip_rows
        running = weights[0](last) - jnp.where(hit[:tall], scales[last], 0.0)
        lower, upper = uppers[last - 1], uppers[last]
        product = jnp.dot(
            running.astype(jnp.bfloat16), rows_of(w_refs, lower, upper),
            preferred_element_type=jnp.float32)
        store(widest, product, first, 0, upper - lower, chip_rows)
        if len(block) > 1:
            running = jnp.concatenate([running, before_ref[...]], axis=0)
        stack = []
        for k in range(last - 1, -1, -1):
            weight = jnp.concatenate([part(k) for part in weights], axis=0)
            running = running + (weight - jnp.where(hit, scales[k], 0.0))
            band = running.astype(jnp.bfloat16)
            if k in narrow:
                stack.append(band)
                continue
            lower, upper = uppers[k - 1], uppers[k]
            product = jnp.dot(
                band, rows_of(w_refs, lower, upper), preferred_element_type=jnp.float32)
            store(others, product, first, lower, upper, chip_rows)
        product = jnp.dot(
            jnp.concatenate(stack, axis=0), rows_of(w_refs, 0, LANES),
            preferred_element_type=jnp.float32)
        lane = lax.broadcasted_iota(jnp.int32, (height, LANES), 1)
        chosen = product[:height]
        for i in range(1, len(stack)):
            chosen = jnp.where(
                lane < uppers[narrow[i]], product[i * height:(i + 1) * height], chosen)
        store(others, chosen, first, 0, LANES, chip_rows)


def store(out_refs, value, first_row, lower, upper, chip_rows):
    for at in range(0, value.shape[0], chip_rows):
        ref = out_refs[(first_row + at) // chip_rows]
        ref[:, lower:upper] = value[at:at + chip_rows].astype(ref.dtype)


def on_device(queries, documents, partner):
    own_rows, feature_dim = queries.shape
    uppers = width_list(feature_dim)
    dp_size, rep_size = lax.axis_size("dp"), lax.axis_size("rep")
    devices = dp_size * rep_size
    bits = devices.bit_length() - 1
    assert rep_size == 2 and devices == 1 << bits and bits % 2 == 1
    stages = (bits - 1) // 2
    groups = 1 << stages
    pieces = 2 * groups
    query_masks = [1 << (2 * s + 1) for s in range(stages)]
    document_masks = [1 << (2 * s + 2) for s in range(stages)]
    total = pieces * own_rows
    chip_rows = 2 * own_rows

    role = lax.axis_index("rep")
    me = (lax.axis_index("dp") * rep_size + role).astype(jnp.int32).reshape(1)
    lead = role == 0

    def exchange(x, masks_of):
        return lax.ppermute(x, AXES, [(i, i ^ masks_of(i)) for i in range(devices)])

    def swap(x):
        return exchange(x, lambda i: 1)

    def along(x, stage):
        return exchange(x, lambda i: document_masks[stage] if i & 1 else query_masks[stage])

    mine = jnp.where(lead, queries, documents)
    other = jnp.where(lead, documents, queries)
    got = swap(other)
    small = groups == 4 and WIDTHS * total * total * 4 <= 16 << 20
    cut = own_rows - 16 if small and own_rows >= 32 else own_rows
    v = {0: [mine, got]}
    w = {0: [swap(mine), other]}
    for stage in reversed(range(stages)):
        for j in sorted(v):
            parts = v[j]
            if small and j == 0:
                parts = [mine, got[:cut], got[cut:]] if stage else [jnp.concatenate(v[0], axis=0)]
            v[j | 1 << stage] = [
                along(part, stage) for part in parts]
    for j in range(1, groups):
        w[j] = [swap(part) for part in v[j]]
    counts = [len(v[j]) for j in range(groups)]
    v_list = [part for j in range(groups) for part in v[j]]
    w_list = [part for j in range(groups) for part in w[j]]

    own_partner = partner.reshape(1, own_rows)
    far_partner = swap(own_partner)

    vmem = pl.BlockSpec(memory_space=pltpu.VMEM)
    smem = pl.BlockSpec(memory_space=pltpu.SMEM)

    def query_mask(j):
        return sum(mask for s, mask in enumerate(query_masks) if j >> s & 1)

    def gathered(stats):
        return [stats] + [exchange(stats, lambda i: query_mask(j)) for j in range(1, groups)]

    shape = lambda *dims: jax.ShapeDtypeStruct(dims, jnp.float32)

    def gradient_shapes(columns):
        return [
            jax.ShapeDtypeStruct((chip_rows, columns), jnp.bfloat16 if j & 1 else jnp.float32)
            for j in range(groups)]

    if not small:
        near, far = own_partner.astype(jnp.float32), far_partner.astype(jnp.float32)
        chip_partner = jnp.where(
            lead, jnp.concatenate([near, far], axis=1), jnp.concatenate([far, near], axis=1))
        limit = 60 << 20
        stats = pl.pallas_call(
            functools.partial(stats_kernel, pieces, uppers),
            out_shape=shape(STATS, total),
            in_specs=[smem] + [vmem] * (1 + 2 * pieces),
            out_specs=vmem,
            scratch_shapes=[
                pltpu.VMEM((total, feature_dim), jnp.bfloat16),
                pltpu.VMEM((total, feature_dim), jnp.bfloat16),
                pltpu.VMEM((total, LANES), jnp.float32),
            ],
            compiler_params=pltpu.CompilerParams(vmem_limit_bytes=limit),
            name="tile_stats",
        )(me, chip_partner, *v_list, *w_list)
        whole = pl.pallas_call(
            functools.partial(grads_kernel, pieces, uppers, own_rows, document_masks),
            out_shape=gradient_shapes(feature_dim),
            in_specs=[smem] + [vmem] * (groups + 2 * pieces),
            out_specs=[vmem] * groups,
            scratch_shapes=[
                pltpu.VMEM((total, feature_dim), jnp.bfloat16),
                pltpu.VMEM((total, feature_dim), jnp.bfloat16),
                pltpu.VMEM((WIDTHS, block_of(total), total), jnp.float32),
                pltpu.VMEM((total, LANES), jnp.float32),
            ],
            compiler_params=pltpu.CompilerParams(vmem_limit_bytes=limit),
            name="tile_grads",
        )(me, *gathered(stats), *v_list, *w_list)
        chunks = [whole]
    else:
        shapes = subtiles(groups)
        limit = 20 << 20
        params = pltpu.CompilerParams(vmem_limit_bytes=limit)

        def tile(span, partner_row, far_row, earlier=()):
            first, end, left, right = extent([shapes[i] for i in span])
            operands = v_list[sum(counts[:first]):sum(counts[:end])]
            operands += w_list[sum(counts[:left]):sum(counts[:right])]
            stat_shapes = [shape(STATS, total)] if earlier else [shape(1, chip_rows)]
            result, area = [], 0
            for i in span:
                r0, r1, c0, c1 = shapes[i]
                tall, wide = (r1 - r0) * chip_rows, (c1 - c0) * chip_rows
                area += tall * wide
                result += [shape(WIDTHS, tall, wide), shape(tall, LANES),
                           shape(2 * STATS, max(tall, wide))]
            *arrays, last_array = pl.pallas_call(
                functools.partial(
                    tile_kernel, span, counts, uppers, own_rows, len(earlier)),
                out_shape=result + stat_shapes,
                in_specs=[smem] + [vmem] * (2 + len(operands) + len(earlier)),
                out_specs=[vmem] * (len(result) + 1),
                compiler_params=params,
                cost_estimate=pl.CostEstimate(
                    flops=6 * area * feature_dim, transcendentals=0,
                    bytes_accessed=2 * total * feature_dim),
            )(me, partner_row, far_row, *operands, *[one[2] for one in earlier])
            return [arrays[3 * i:3 * i + 3] for i in range(len(span))], last_array

        done, chip_partner = tile([0], own_partner, far_partner)
        for at in (1, 2, 3):
            more, chip_partner = tile([at], chip_partner, far_partner)
            done += more
        more, stats = tile([4], chip_partner, far_partner, done)
        done += more
        first = exchange(
            stats, lambda i: query_mask(1) if i & 1 else query_mask(3))
        second = exchange(stats, lambda i: query_mask(2))
        swapped = swap(first)
        common = [me, stats, first, second, swapped, *[t[0] for t in done], *[t[1] for t in done],
                  *[t[2] for t in done], *w_list]
        near = segments_of(groups)[-1][0]
        widest = feature_dim - uppers[-2]

        def bands(kernel, more, outs):
            return pl.pallas_call(
                functools.partial(kernel, groups, uppers, own_rows, document_masks),
                out_shape=outs,
                in_specs=[smem] + [vmem] * (len(common) - 1 + len(more)),
                out_specs=[vmem] * len(outs),
                compiler_params=params,
                cost_estimate=pl.CostEstimate(
                    flops=2 * total * total * feature_dim, transcendentals=0,
                    bytes_accessed=4 * total * feature_dim),
            )(*common, *more)

        *far_ones, running = bands(
            last_band_kernel, [],
            gradient_shapes(widest)[near:] + [shape((groups - near) * chip_rows, total)])
        rest = bands(
            bands_kernel, [running], gradient_shapes(uppers[-2]) + gradient_shapes(widest)[:near])
        chunks = [[*rest[groups:], *far_ones], rest[:groups]]

    mine_parts, other_parts = [], []
    for c, chunk in enumerate(chunks):
        partial = dict(enumerate(chunk))
        for stage in range(stages - 1):
            step = 1 << stage
            for j in sorted([j for j in partial if j & step], reverse=True):
                arrived = along(partial.pop(j).astype(jnp.bfloat16), stage)
                partial[j ^ step] = partial[j ^ step] + arrived.astype(jnp.float32)
                if stage == stages - 2 and j ^ step:
                    partial[j ^ step] = partial[j ^ step].astype(jnp.bfloat16)
        stage = stages - 1
        outgoing = partial[1 << stage]
        kept = partial[0]
        if c < len(chunks) - 1:
            arrived = along(outgoing, stage)
            kept = kept + arrived.astype(jnp.float32)
            mine_parts.append(kept[:own_rows])
            other_parts.append(swap(kept[own_rows:]))
        else:
            far = lambda i: document_masks[stage] ^ 1 if i & 1 else query_masks[stage] ^ 1
            near_arrived = along(outgoing[:own_rows], stage)
            far_arrived = exchange(outgoing[own_rows:], far)
            ours, theirs = lax.optimization_barrier((kept[:own_rows], kept[own_rows:]))
            mine_parts.append(ours + near_arrived.astype(jnp.float32))
            other_parts.append(swap(theirs) + far_arrived.astype(jnp.float32))
    mine_parts, other_parts = mine_parts[::-1], other_parts[::-1]
    ours = jnp.concatenate(mine_parts, axis=1)
    theirs = jnp.concatenate(other_parts, axis=1)
    return jnp.where(lead, ours, theirs), jnp.where(lead, theirs, ours)


def solution(mesh):
    return jax.shard_map(
        on_device,
        mesh=mesh,
        in_specs=(P(AXES, None), P(AXES, None), P(AXES)),
        out_specs=(P(AXES, None), P(AXES, None)),
        check_vma=False,
    )
```

```python
import functools
import math

import jax
import jax.numpy as jnp
from jax import lax
from jax.experimental import pallas as pl
from jax.experimental.pallas import tpu as pltpu
from jax.sharding import PartitionSpec as P


WIDTHS = 9
AXES = ("dp", "rep")
LOG2E = 1.4426950408889634
STATS = 16
LANES = 128


logit_gain = 3.0


def width_list(feature_dim):
    return [feature_dim >> WIDTHS - 1 - nested for nested in range(WIDTHS)]


def transposed_dot(a, b):
    return lax.dot_general(a, b, (((1,), (1,)), ((), ())), preferred_element_type=jnp.float32)


def prefix_scores(v_ref, w_ref, rows, uppers):
    narrow = [m for m in uppers if m <= LANES]
    count = rows.size
    head = v_ref[rows, :LANES]
    lane = lax.broadcasted_iota(jnp.int32, head.shape, 1)
    masked = [jnp.where(lane < m, head, jnp.zeros_like(head)) for m in narrow]
    stacked = transposed_dot(jnp.concatenate(masked, axis=0), w_ref[:, :LANES])
    result = [stacked[k * count:(k + 1) * count] for k in range(len(narrow))]
    lower = narrow[-1]
    for upper in uppers[len(narrow):]:
        part = transposed_dot(v_ref[rows, lower:upper], w_ref[:, lower:upper])
        result.append(result[-1] + part)
        lower = upper
    return result


def block_of(total):
    return min(total, 256)


def load_tile(refs, scratch):
    at = 0
    for ref in refs:
        scratch[at:at + ref.shape[0], :] = ref[...]
        at += ref.shape[0]


def stats_kernel(pieces, uppers, *refs):
    role_ref, partner_ref = refs[:2]
    v_refs, w_refs = refs[2:2 + pieces], refs[2 + pieces:2 + 2 * pieces]
    out_ref, v_ref, w_ref, col_ref = refs[2 + 2 * pieces:]
    load_tile(v_refs, v_ref)
    load_tile(w_refs, w_ref)
    total = v_ref.shape[0]
    block = block_of(total)
    steps = total // block
    gains = [logit_gain * m ** -0.5 * LOG2E for m in uppers]
    own = partner_ref.shape[1]
    out_ref[...] = jnp.zeros_like(out_ref)

    @pl.when((role_ref[0] & 1) == 0)
    def _():
        for step in range(steps):
            rows = pl.ds(step * block, block)
            col_ref[rows, :] = jnp.zeros((block, LANES), jnp.float32)
            for k, s in enumerate(prefix_scores(v_ref, w_ref, rows, uppers)):
                logits = s * gains[k]
                peak = jnp.max(logits, axis=1, keepdims=True)
                mass = jnp.sum(jnp.exp2(logits - peak), axis=1, keepdims=True)
                col_ref[rows, k:k + 1] = peak + jnp.log(mass) * LOG2E
        out_ref[...] = col_ref[...].T[:STATS]

    @pl.when((role_ref[0] & 1) != 0)
    def _():
        peaks, masses = [None] * len(uppers), [None] * len(uppers)
        for step in range(steps):
            rows = pl.ds(step * block, block)
            for k, s in enumerate(prefix_scores(v_ref, w_ref, rows, uppers)):
                logits = s * gains[k]
                peak = jnp.max(logits, axis=0, keepdims=True)
                mass = jnp.sum(jnp.exp2(logits - peak), axis=0, keepdims=True)
                if step:
                    top = jnp.maximum(peak, peaks[k])
                    mass = mass * jnp.exp2(peak - top) + masses[k] * jnp.exp2(peaks[k] - top)
                    peak = top
                peaks[k], masses[k] = peak, mass
        for k in range(len(uppers)):
            out_ref[k:k + 1, :] = peaks[k] + jnp.log(masses[k]) * LOG2E

    out_ref[len(uppers):len(uppers) + 1, :own] = partner_ref[...]


def document_ids(shape, axis, first, own_rows, masks, start=0):
    at = lax.broadcasted_iota(jnp.int32, shape, axis) + start
    shift = own_rows.bit_length() - 1
    piece = at >> shift
    device = first ^ (piece & 1)
    for s, mask in enumerate(masks):
        device = device ^ (((piece >> (1 + s)) & 1) * mask)
    return (device * own_rows + (at & (own_rows - 1))).astype(jnp.float32)


def grads_kernel(pieces, uppers, own_rows, masks, *refs):
    me_ref = refs[0]
    groups = pieces // 2
    stat_refs = refs[1:1 + groups]
    v_refs = refs[1 + groups:1 + groups + pieces]
    w_refs = refs[1 + groups + pieces:1 + groups + 2 * pieces]
    out_refs = refs[1 + groups + 2 * pieces:1 + 2 * groups + 2 * pieces]
    v_ref, w_ref, score_ref, col_ref = refs[1 + 2 * groups + 2 * pieces:]
    load_tile(v_refs, v_ref)
    load_tile(w_refs, w_ref)
    total = v_ref.shape[0]
    block = block_of(total)
    chip_rows = total // groups
    count = len(uppers)
    scales = [logit_gain * m ** -0.5 for m in uppers]
    me = me_ref[0]
    lead = (me & 1) == 0

    parts = []
    partners = []
    for j, ref in enumerate(stat_refs):
        parts.append(jnp.concatenate(
            [ref[:, (i ^ j) * chip_rows:((i ^ j) + 1) * chip_rows] for i in range(groups)], axis=1))
        partners.append(ref[count:count + 1, :chip_rows])
    peak = functools.reduce(jnp.maximum, parts)
    mass = functools.reduce(lambda a, b: a + b, [jnp.exp2(part - peak) for part in parts])
    totals = peak + jnp.log(mass) * LOG2E
    partner_row = jnp.concatenate(partners, axis=1)
    packed = jnp.concatenate(
        [totals[:count], partner_row, jnp.zeros((LANES - count - 1, total), jnp.float32)], axis=0)
    col_ref[...] = packed.T
    zero_or = lambda keep, x: jnp.where(keep, x, jnp.zeros_like(x))
    document_row = document_ids((1, total), 1, me | 1, own_rows, masks)
    id_row = jnp.where(lead, document_row, partner_row)
    shifts = [math.log2(s) for s in scales]
    total_rows = [zero_or(jnp.logical_not(lead), totals[k:k + 1]) - shifts[k] for k in range(count)]

    narrow = [m for m in uppers if m <= LANES]
    for step in range(total // block):
        rows = pl.ds(step * block, block)
        document_col = document_ids((block, 1), 0, me | 1, own_rows, masks, step * block)
        id_col = jnp.where(lead, col_ref[rows, count:count + 1], document_col)
        hit = id_col == id_row
        for k, s in enumerate(prefix_scores(v_ref, w_ref, rows, uppers)):
            score_ref[k] = s
        running = None
        stack = []
        for k in reversed(range(count)):
            gain = scales[k] * LOG2E
            total_col = zero_or(lead, col_ref[rows, k:k + 1])
            weight = jnp.exp2(score_ref[k] * gain - total_col - total_rows[k])
            weight = weight - jnp.where(hit, scales[k], 0.0)
            running = weight if running is None else running + weight
            band = running.astype(jnp.bfloat16)
            if k >= len(narrow):
                lower, upper = uppers[k - 1], uppers[k]
                product = jnp.dot(band, w_ref[:, lower:upper], preferred_element_type=jnp.float32)
                store(out_refs, product, step * block, lower, upper, chip_rows)
            else:
                stack.append(band)
        product = jnp.dot(
            jnp.concatenate(stack, axis=0), w_ref[:, :LANES], preferred_element_type=jnp.float32)
        lane = lax.broadcasted_iota(jnp.int32, (block, LANES), 1)
        chosen = product[:block]
        for at_stack in range(1, len(stack)):
            k = len(narrow) - 1 - at_stack
            chosen = jnp.where(
                lane < uppers[k], product[at_stack * block:(at_stack + 1) * block], chosen)
        store(out_refs, chosen, step * block, 0, LANES, chip_rows)


def rows_of(refs, lower, upper):
    return jnp.concatenate([ref[:, lower:upper] for ref in refs], axis=0)


def subtile_scores(v_refs, w_refs, uppers):
    narrow = [m for m in uppers if m <= LANES]
    left, right = rows_of(v_refs, 0, LANES), rows_of(w_refs, 0, LANES)
    slim = right.shape[0] < 2 * LANES
    head = right if slim else left
    count = head.shape[0]
    lane = lax.broadcasted_iota(jnp.int32, head.shape, 1)
    masked = jnp.concatenate(
        [jnp.where(lane < m, head, jnp.zeros_like(head)) for m in narrow], axis=0)
    if slim:
        stacked = transposed_dot(left, masked)
        parts = [stacked[:, k * count:(k + 1) * count] for k in range(len(narrow))]
    else:
        stacked = transposed_dot(masked, right)
        parts = [stacked[k * count:(k + 1) * count] for k in range(len(narrow))]
    yield from parts
    lower, running = narrow[-1], parts[-1]
    for upper in uppers[len(narrow):]:
        running = running + transposed_dot(
            rows_of(v_refs, lower, upper), rows_of(w_refs, lower, upper))
        yield running
        lower = upper


def subtile(lead, v_refs, w_refs, uppers, refs):
    power_ref, col_ref, line_ref = refs
    gains = [logit_gain * m ** -0.5 * LOG2E for m in uppers]
    count, across = power_ref.shape[1:]

    @pl.when(lead)
    def _():
        lane = lax.broadcasted_iota(jnp.int32, (count, LANES), 1)
        both = jnp.where(lane < STATS, 0.0, 1.0)
        for k, s in enumerate(subtile_scores(v_refs, w_refs, uppers)):
            logits = s * gains[k]
            peak = jnp.max(logits, axis=1, keepdims=True)
            power = jnp.exp2(logits - peak)
            power_ref[k] = power
            both = jnp.where(lane == k, peak, both)
            both = jnp.where(lane == STATS + k, jnp.sum(power, axis=1, keepdims=True), both)
        col_ref[...] = both
        line_ref[:, :count] = both.T[:2 * STATS]

    @pl.when(jnp.logical_not(lead))
    def _():
        line_ref[:STATS, :] = jnp.zeros((STATS, line_ref.shape[1]), jnp.float32)
        line_ref[STATS:, :] = jnp.ones((STATS, line_ref.shape[1]), jnp.float32)
        for k, s in enumerate(subtile_scores(v_refs, w_refs, uppers)):
            logits = s * gains[k]
            peak = jnp.max(logits, axis=0, keepdims=True)
            power = jnp.exp2(logits - peak)
            power_ref[k] = power
            line_ref[k:k + 1, :across] = peak
            line_ref[STATS + k:STATS + k + 1, :across] = jnp.sum(power, axis=0, keepdims=True)


def log_sum(pairs):
    top = functools.reduce(jnp.maximum, [peak for peak, _ in pairs])
    mass = functools.reduce(
        lambda a, b: a + b, [mass * jnp.exp2(peak - top) for peak, mass in pairs])
    return top + jnp.log(mass) * LOG2E


def tile_kernel(span, counts, uppers, own_rows, finish, *refs):
    groups = len(counts)
    shapes = subtiles(groups)
    tiles = [shapes[i] for i in span]
    r0, r1, c0, c1 = extent(tiles)
    me_ref, partner_ref, far_ref = refs[:3]
    at = 3 + sum(counts[r0:r1])
    v_refs, w_refs = refs[3:at], refs[at:at + sum(counts[c0:c1])]
    at += sum(counts[c0:c1])
    earlier = refs[at:at + finish]
    outs = refs[at + finish:]
    lead = (me_ref[0] & 1) == 0
    for i, (t0, t1, u0, u1) in enumerate(tiles):
        subtile(
            lead, v_refs[sum(counts[r0:t0]):sum(counts[r0:t1])],
            w_refs[sum(counts[c0:u0]):sum(counts[c0:u1])], uppers, outs[3 * i:3 * i + 3])
    if not finish:
        if span[0] == 0:
            near, far = partner_ref[...].astype(jnp.float32), far_ref[...].astype(jnp.float32)
            outs[-1][:, :own_rows] = jnp.where(lead, near, far)
            outs[-1][:, own_rows:] = jnp.where(lead, far, near)
        else:
            outs[-1][...] = partner_ref[...]
        return
    stats_ref = outs[-1]
    every = [*earlier, *outs[2:3 * len(tiles):3]]
    segments = segments_of(groups)
    chip_rows = 2 * own_rows

    def merge(axis):
        for s0, s1 in segments:
            pairs = []
            for shape, line in zip(shapes, every):
                low, high = shape[axis:axis + 2]
                if low <= s0 and s1 <= high:
                    at = slice((s0 - low) * chip_rows, (s1 - low) * chip_rows)
                    pairs.append((line[:STATS, at], line[STATS:, at]))
            stats_ref[:, s0 * chip_rows:s1 * chip_rows] = log_sum(pairs)

    pl.when(lead)(lambda: merge(0))
    pl.when(jnp.logical_not(lead))(lambda: merge(2))

    count = len(uppers)
    stats_ref[count:count + 1, :chip_rows] = partner_ref[...]


def segments_of(groups):
    low, middle = groups // 2, groups // 2 + groups // 4
    return [(0, low), (low, middle), (middle, groups)]


def subtiles(groups):
    (_, low), (_, middle), _ = segments_of(groups)
    return [(0, low, 0, low), (low, middle, 0, low), (0, middle, low, middle),
            (middle, groups, 0, middle), (0, groups, middle, groups)]


def extent(tiles):
    first, second, third, fourth = zip(*tiles)
    return min(first), max(second), min(third), max(fourth)


def band_setup(groups, uppers, own_rows, masks, me_ref, stat_refs):
    count = len(uppers)
    total = stat_refs[0].shape[1]
    chip_rows = total // groups
    me = me_ref[0]
    lead = (me & 1) == 0
    own, first, second, swapped = [ref[...] for ref in stat_refs]
    values = [own, jnp.where(lead, first, swapped), second, jnp.where(lead, swapped, first)]
    parts, partners = [], []
    for j, value in enumerate(values):
        parts.append(jnp.concatenate(
            [value[:, (i ^ j) * chip_rows:((i ^ j) + 1) * chip_rows] for i in range(groups)], axis=1))
        partners.append(value[count:count + 1, :chip_rows])
    peak = functools.reduce(jnp.maximum, parts)
    mass = functools.reduce(lambda a, b: a + b, [jnp.exp2(part - peak) for part in parts])
    partner_row = jnp.concatenate(partners, axis=1)
    sub = lax.broadcasted_iota(jnp.int32, (STATS, total), 0)
    totals = peak + jnp.log(mass) * LOG2E
    for k in range(count):
        totals = jnp.where(sub == k, totals - math.log2(logit_gain * uppers[k] ** -0.5), totals)
    packed = jnp.concatenate(
        [totals[:count], partner_row, jnp.zeros((LANES - count - 1, total), jnp.float32)], axis=0)
    cols = packed.T
    id_row = jnp.where(
        lead, document_ids((1, total), 1, me | 1, own_rows, masks), partner_row)
    id_col = jnp.where(
        lead, cols[:, count:count + 1],
        document_ids((total, 1), 0, me | 1, own_rows, masks))
    return lead, totals, cols, id_row, id_col


def weights_of(segment, groups, setup, power_refs, col_refs, row_refs):
    lead, totals, cols, _, _ = setup
    chip_rows = totals.shape[1] // groups
    s0, s1 = segment
    strip = []
    for (r0, r1, c0, c1), power, col_peak, line in zip(
            subtiles(groups), power_refs, col_refs, row_refs):
        if r0 <= s0 and s1 <= r1:
            inner = slice((s0 - r0) * chip_rows, (s1 - r0) * chip_rows)
            outer = slice(s0 * chip_rows, s1 * chip_rows)
            across = slice(c0 * chip_rows, c1 * chip_rows)
            strip.append((
                c0, power, inner,
                jnp.where(lead, jnp.exp2(col_peak[inner, :] - cols[outer]), 1.0),
                jnp.where(lead, 1.0, jnp.exp2(line[:STATS, :(c1 - c0) * chip_rows] - totals[:, across]))))
    strip.sort(key=lambda item: item[0])
    return lambda k: jnp.concatenate([
        power[k, inner] * col_gain[:, k:k + 1] * row_gain[k:k + 1, :]
        for _, power, inner, col_gain, row_gain in strip], axis=1)


def last_band_kernel(groups, uppers, own_rows, masks, *refs):
    tiles = len(subtiles(groups))
    setup = band_setup(groups, uppers, own_rows, masks, refs[0], refs[1:1 + groups])
    at = 1 + groups
    power_refs, col_refs, row_refs = [refs[at + i * tiles:at + (i + 1) * tiles] for i in range(3)]
    segment = segments_of(groups)[-1]
    farthest = segment[1] - segment[0]
    w_refs, out_refs, after_ref = refs[at + 3 * tiles:-farthest - 1], refs[-farthest - 1:-1], refs[-1]
    _, totals, _, id_row, id_col = setup
    chip_rows = totals.shape[1] // groups
    k = len(uppers) - 1
    rows = slice(segment[0] * chip_rows, segment[1] * chip_rows)
    weight = weights_of(segment, groups, setup, power_refs, col_refs, row_refs)(k)
    weight = weight - jnp.where(id_col[rows] == id_row, logit_gain * uppers[k] ** -0.5, 0.0)
    after_ref[...] = weight
    product = jnp.dot(
        weight.astype(jnp.bfloat16), rows_of(w_refs, uppers[k - 1], uppers[k]),
        preferred_element_type=jnp.float32)
    store(out_refs, product, 0, 0, uppers[k] - uppers[k - 1], chip_rows)


def bands_kernel(groups, uppers, own_rows, masks, *refs):
    tiles = len(subtiles(groups))
    setup = band_setup(groups, uppers, own_rows, masks, refs[0], refs[1:1 + groups])
    at = 1 + groups
    power_refs, col_refs, row_refs = [refs[at + i * tiles:at + (i + 1) * tiles] for i in range(3)]
    segments = segments_of(groups)
    outs = groups + segments[-1][0]
    before_ref = refs[-outs - 1]
    w_refs, others, widest = refs[at + 3 * tiles:-outs - 1], refs[-outs:-outs + groups], refs[-outs + groups:]
    _, totals, _, id_row, id_col = setup
    chip_rows = totals.shape[1] // groups
    scales = [logit_gain * m ** -0.5 for m in uppers]
    last = len(uppers) - 1
    narrow = [k for k in range(last, -1, -1) if uppers[k] <= LANES]
    for block in (segments[1:], segments[:1]):
        first = block[0][0] * chip_rows
        rows = slice(first, block[-1][1] * chip_rows)
        height = rows.stop - first
        hit = id_col[rows] == id_row
        weights = [
            weights_of(segment, groups, setup, power_refs, col_refs, row_refs) for segment in block]
        tall = (block[0][1] - block[0][0]) * chip_rows
        running = weights[0](last) - jnp.where(hit[:tall], scales[last], 0.0)
        lower, upper = uppers[last - 1], uppers[last]
        product = jnp.dot(
            running.astype(jnp.bfloat16), rows_of(w_refs, lower, upper),
            preferred_element_type=jnp.float32)
        store(widest, product, first, 0, upper - lower, chip_rows)
        if len(block) > 1:
            running = jnp.concatenate([running, before_ref[...]], axis=0)
        stack = []
        for k in range(last - 1, -1, -1):
            weight = jnp.concatenate([part(k) for part in weights], axis=0)
            running = running + (weight - jnp.where(hit, scales[k], 0.0))
            band = running.astype(jnp.bfloat16)
            if k in narrow:
                stack.append(band)
                continue
            lower, upper = uppers[k - 1], uppers[k]
            product = jnp.dot(
                band, rows_of(w_refs, lower, upper), preferred_element_type=jnp.float32)
            store(others, product, first, lower, upper, chip_rows)
        product = jnp.dot(
            jnp.concatenate(stack, axis=0), rows_of(w_refs, 0, LANES),
            preferred_element_type=jnp.float32)
        lane = lax.broadcasted_iota(jnp.int32, (height, LANES), 1)
        chosen = product[:height]
        for i in range(1, len(stack)):
            chosen = jnp.where(
                lane < uppers[narrow[i]], product[i * height:(i + 1) * height], chosen)
        store(others, chosen, first, 0, LANES, chip_rows)


def store(out_refs, value, first_row, lower, upper, chip_rows):
    for at in range(0, value.shape[0], chip_rows):
        ref = out_refs[(first_row + at) // chip_rows]
        ref[:, lower:upper] = value[at:at + chip_rows].astype(ref.dtype)


def on_device(queries, documents, partner):
    own_rows, feature_dim = queries.shape
    uppers = width_list(feature_dim)
    dp_size, rep_size = lax.axis_size("dp"), lax.axis_size("rep")
    devices = dp_size * rep_size
    bits = devices.bit_length() - 1
    assert rep_size == 2 and devices == 1 << bits and bits % 2 == 1
    stages = (bits - 1) // 2
    groups = 1 << stages
    pieces = 2 * groups
    query_masks = [1 << (2 * s + 1) for s in range(stages)]
    document_masks = [1 << (2 * s + 2) for s in range(stages)]
    total = pieces * own_rows
    chip_rows = 2 * own_rows

    role = lax.axis_index("rep")
    me = (lax.axis_index("dp") * rep_size + role).astype(jnp.int32).reshape(1)
    lead = role == 0

    def exchange(x, masks_of):
        return lax.ppermute(x, AXES, [(i, i ^ masks_of(i)) for i in range(devices)])

    def swap(x):
        return exchange(x, lambda i: 1)

    def along(x, stage):
        return exchange(x, lambda i: document_masks[stage] if i & 1 else query_masks[stage])

    mine = jnp.where(lead, queries, documents)
    other = jnp.where(lead, documents, queries)
    got = swap(other)
    small = groups == 4 and WIDTHS * total * total * 4 <= 16 << 20
    cut = own_rows - 16 if small and own_rows >= 32 else own_rows
    v = {0: [mine, got]}
    w = {0: [swap(mine), other]}
    for stage in reversed(range(stages)):
        for j in sorted(v):
            parts = v[j]
            if small and j == 0 and stage:
                parts = [mine, got[:cut], got[cut:]]
            v[j | 1 << stage] = [
                along(part, stage) for part in parts]
    for j in range(1, groups):
        w[j] = [swap(part) for part in v[j]]
    counts = [len(v[j]) for j in range(groups)]
    v_list = [part for j in range(groups) for part in v[j]]
    w_list = [part for j in range(groups) for part in w[j]]

    own_partner = partner.reshape(1, own_rows)
    far_partner = swap(own_partner)

    vmem = pl.BlockSpec(memory_space=pltpu.VMEM)
    smem = pl.BlockSpec(memory_space=pltpu.SMEM)

    def query_mask(j):
        return sum(mask for s, mask in enumerate(query_masks) if j >> s & 1)

    def gathered(stats):
        return [stats] + [exchange(stats, lambda i: query_mask(j)) for j in range(1, groups)]

    shape = lambda *dims: jax.ShapeDtypeStruct(dims, jnp.float32)

    def gradient_shapes(columns):
        return [
            jax.ShapeDtypeStruct((chip_rows, columns), jnp.bfloat16 if j & 1 else jnp.float32)
            for j in range(groups)]

    if not small:
        near, far = own_partner.astype(jnp.float32), far_partner.astype(jnp.float32)
        chip_partner = jnp.where(
            lead, jnp.concatenate([near, far], axis=1), jnp.concatenate([far, near], axis=1))
        limit = 60 << 20
        stats = pl.pallas_call(
            functools.partial(stats_kernel, pieces, uppers),
            out_shape=shape(STATS, total),
            in_specs=[smem] + [vmem] * (1 + 2 * pieces),
            out_specs=vmem,
            scratch_shapes=[
                pltpu.VMEM((total, feature_dim), jnp.bfloat16),
                pltpu.VMEM((total, feature_dim), jnp.bfloat16),
                pltpu.VMEM((total, LANES), jnp.float32),
            ],
            compiler_params=pltpu.CompilerParams(vmem_limit_bytes=limit),
            name="tile_stats",
        )(me, chip_partner, *v_list, *w_list)
        whole = pl.pallas_call(
            functools.partial(grads_kernel, pieces, uppers, own_rows, document_masks),
            out_shape=gradient_shapes(feature_dim),
            in_specs=[smem] + [vmem] * (groups + 2 * pieces),
            out_specs=[vmem] * groups,
            scratch_shapes=[
                pltpu.VMEM((total, feature_dim), jnp.bfloat16),
                pltpu.VMEM((total, feature_dim), jnp.bfloat16),
                pltpu.VMEM((WIDTHS, block_of(total), total), jnp.float32),
                pltpu.VMEM((total, LANES), jnp.float32),
            ],
            compiler_params=pltpu.CompilerParams(vmem_limit_bytes=limit),
            name="tile_grads",
        )(me, *gathered(stats), *v_list, *w_list)
        chunks = [whole]
    else:
        shapes = subtiles(groups)
        limit = 20 << 20
        params = pltpu.CompilerParams(vmem_limit_bytes=limit)

        def tile(span, partner_row, far_row, earlier=()):
            first, end, left, right = extent([shapes[i] for i in span])
            operands = v_list[sum(counts[:first]):sum(counts[:end])]
            operands += w_list[sum(counts[:left]):sum(counts[:right])]
            stat_shapes = [shape(STATS, total)] if earlier else [shape(1, chip_rows)]
            result, area = [], 0
            for i in span:
                r0, r1, c0, c1 = shapes[i]
                tall, wide = (r1 - r0) * chip_rows, (c1 - c0) * chip_rows
                area += tall * wide
                result += [shape(WIDTHS, tall, wide), shape(tall, LANES),
                           shape(2 * STATS, max(tall, wide))]
            *arrays, last_array = pl.pallas_call(
                functools.partial(
                    tile_kernel, span, counts, uppers, own_rows, len(earlier)),
                out_shape=result + stat_shapes,
                in_specs=[smem] + [vmem] * (2 + len(operands) + len(earlier)),
                out_specs=[vmem] * (len(result) + 1),
                compiler_params=params,
                cost_estimate=pl.CostEstimate(
                    flops=6 * area * feature_dim, transcendentals=0,
                    bytes_accessed=2 * total * feature_dim),
            )(me, partner_row, far_row, *operands, *[one[2] for one in earlier])
            return [arrays[3 * i:3 * i + 3] for i in range(len(span))], last_array

        done, chip_partner = tile([0], own_partner, far_partner)
        for at in (1, 2, 3):
            more, chip_partner = tile([at], chip_partner, far_partner)
            done += more
        more, stats = tile([4], chip_partner, far_partner, done)
        done += more
        first = exchange(
            stats, lambda i: query_mask(3) if i & 1 else query_mask(1))
        second = exchange(stats, lambda i: query_mask(2))
        swapped = swap(first)
        common = [me, stats, first, second, swapped, *[t[0] for t in done], *[t[1] for t in done],
                  *[t[2] for t in done], *w_list]
        near = segments_of(groups)[-1][0]
        widest = feature_dim - uppers[-2]

        def bands(kernel, more, outs):
            return pl.pallas_call(
                functools.partial(kernel, groups, uppers, own_rows, document_masks),
                out_shape=outs,
                in_specs=[smem] + [vmem] * (len(common) - 1 + len(more)),
                out_specs=[vmem] * len(outs),
                compiler_params=params,
                cost_estimate=pl.CostEstimate(
                    flops=2 * total * total * feature_dim, transcendentals=0,
                    bytes_accessed=4 * total * feature_dim),
            )(*common, *more)

        *far_ones, running = bands(
            last_band_kernel, [],
            gradient_shapes(widest)[near:] + [shape((groups - near) * chip_rows, total)])
        rest = bands(
            bands_kernel, [running], gradient_shapes(uppers[-2]) + gradient_shapes(widest)[:near])
        chunks = [[*rest[groups:], *far_ones], rest[:groups]]

    mine_parts, other_parts = [], []
    for c, chunk in enumerate(chunks):
        partial = dict(enumerate(chunk))
        for stage in range(stages - 1):
            step = 1 << stage
            for j in sorted([j for j in partial if j & step], reverse=True):
                arrived = along(partial.pop(j).astype(jnp.bfloat16), stage)
                partial[j ^ step] = partial[j ^ step] + arrived.astype(jnp.float32)
                if stage == stages - 2 and j ^ step:
                    partial[j ^ step] = partial[j ^ step].astype(jnp.bfloat16)
        stage = stages - 1
        outgoing = partial[1 << stage]
        kept = partial[0]
        if c < len(chunks) - 1:
            arrived = along(outgoing, stage)
            kept = kept + arrived.astype(jnp.float32)
            mine_parts.append(kept[:own_rows])
            other_parts.append(swap(kept[own_rows:]))
        else:
            far = lambda i: document_masks[stage] ^ 1 if i & 1 else query_masks[stage] ^ 1
            near_arrived = along(outgoing[:own_rows], stage)
            far_arrived = exchange(outgoing[own_rows:], far)
            ours, theirs = lax.optimization_barrier((kept[:own_rows], kept[own_rows:]))
            mine_parts.append(ours + near_arrived.astype(jnp.float32))
            other_parts.append(swap(theirs) + far_arrived.astype(jnp.float32))
    mine_parts, other_parts = mine_parts[::-1], other_parts[::-1]
    ours = jnp.concatenate(mine_parts, axis=1)
    theirs = jnp.concatenate(other_parts, axis=1)
    return jnp.where(lead, ours, theirs), jnp.where(lead, theirs, ours)


def solution(mesh):
    return jax.shard_map(
        on_device,
        mesh=mesh,
        in_specs=(P(AXES, None), P(AXES, None), P(AXES)),
        out_specs=(P(AXES, None), P(AXES, None)),
        check_vma=False,
    )
```

```python
import functools
import math

import jax
import jax.numpy as jnp
from jax import lax
from jax.experimental import pallas as pl
from jax.experimental.pallas import tpu as pltpu
from jax.sharding import PartitionSpec as P


WIDTHS = 9
AXES = ("dp", "rep")
LOG2E = 1.4426950408889634
STATS = 16
LANES = 128


logit_gain = 3.0


def width_list(feature_dim):
    return [feature_dim >> WIDTHS - 1 - nested for nested in range(WIDTHS)]


def transposed_dot(a, b):
    return lax.dot_general(a, b, (((1,), (1,)), ((), ())), preferred_element_type=jnp.float32)


def prefix_scores(v_ref, w_ref, rows, uppers):
    narrow = [m for m in uppers if m <= LANES]
    count = rows.size
    head = v_ref[rows, :LANES]
    lane = lax.broadcasted_iota(jnp.int32, head.shape, 1)
    masked = [jnp.where(lane < m, head, jnp.zeros_like(head)) for m in narrow]
    stacked = transposed_dot(jnp.concatenate(masked, axis=0), w_ref[:, :LANES])
    result = [stacked[k * count:(k + 1) * count] for k in range(len(narrow))]
    lower = narrow[-1]
    for upper in uppers[len(narrow):]:
        part = transposed_dot(v_ref[rows, lower:upper], w_ref[:, lower:upper])
        result.append(result[-1] + part)
        lower = upper
    return result


def block_of(total):
    return min(total, 256)


def load_tile(refs, scratch):
    at = 0
    for ref in refs:
        scratch[at:at + ref.shape[0], :] = ref[...]
        at += ref.shape[0]


def stats_kernel(pieces, uppers, *refs):
    role_ref, partner_ref = refs[:2]
    v_refs, w_refs = refs[2:2 + pieces], refs[2 + pieces:2 + 2 * pieces]
    out_ref, v_ref, w_ref, col_ref = refs[2 + 2 * pieces:]
    load_tile(v_refs, v_ref)
    load_tile(w_refs, w_ref)
    total = v_ref.shape[0]
    block = block_of(total)
    steps = total // block
    gains = [logit_gain * m ** -0.5 * LOG2E for m in uppers]
    own = partner_ref.shape[1]
    out_ref[...] = jnp.zeros_like(out_ref)

    @pl.when((role_ref[0] & 1) == 0)
    def _():
        for step in range(steps):
            rows = pl.ds(step * block, block)
            col_ref[rows, :] = jnp.zeros((block, LANES), jnp.float32)
            for k, s in enumerate(prefix_scores(v_ref, w_ref, rows, uppers)):
                logits = s * gains[k]
                peak = jnp.max(logits, axis=1, keepdims=True)
                mass = jnp.sum(jnp.exp2(logits - peak), axis=1, keepdims=True)
                col_ref[rows, k:k + 1] = peak + jnp.log(mass) * LOG2E
        out_ref[...] = col_ref[...].T[:STATS]

    @pl.when((role_ref[0] & 1) != 0)
    def _():
        peaks, masses = [None] * len(uppers), [None] * len(uppers)
        for step in range(steps):
            rows = pl.ds(step * block, block)
            for k, s in enumerate(prefix_scores(v_ref, w_ref, rows, uppers)):
                logits = s * gains[k]
                peak = jnp.max(logits, axis=0, keepdims=True)
                mass = jnp.sum(jnp.exp2(logits - peak), axis=0, keepdims=True)
                if step:
                    top = jnp.maximum(peak, peaks[k])
                    mass = mass * jnp.exp2(peak - top) + masses[k] * jnp.exp2(peaks[k] - top)
                    peak = top
                peaks[k], masses[k] = peak, mass
        for k in range(len(uppers)):
            out_ref[k:k + 1, :] = peaks[k] + jnp.log(masses[k]) * LOG2E

    out_ref[len(uppers):len(uppers) + 1, :own] = partner_ref[...]


def document_ids(shape, axis, first, own_rows, masks, start=0):
    at = lax.broadcasted_iota(jnp.int32, shape, axis) + start
    shift = own_rows.bit_length() - 1
    piece = at >> shift
    device = first ^ (piece & 1)
    for s, mask in enumerate(masks):
        device = device ^ (((piece >> (1 + s)) & 1) * mask)
    return (device * own_rows + (at & (own_rows - 1))).astype(jnp.float32)


def grads_kernel(pieces, uppers, own_rows, masks, *refs):
    me_ref = refs[0]
    groups = pieces // 2
    stat_refs = refs[1:1 + groups]
    v_refs = refs[1 + groups:1 + groups + pieces]
    w_refs = refs[1 + groups + pieces:1 + groups + 2 * pieces]
    out_refs = refs[1 + groups + 2 * pieces:1 + 2 * groups + 2 * pieces]
    v_ref, w_ref, score_ref, col_ref = refs[1 + 2 * groups + 2 * pieces:]
    load_tile(v_refs, v_ref)
    load_tile(w_refs, w_ref)
    total = v_ref.shape[0]
    block = block_of(total)
    chip_rows = total // groups
    count = len(uppers)
    scales = [logit_gain * m ** -0.5 for m in uppers]
    me = me_ref[0]
    lead = (me & 1) == 0

    parts = []
    partners = []
    for j, ref in enumerate(stat_refs):
        parts.append(jnp.concatenate(
            [ref[:, (i ^ j) * chip_rows:((i ^ j) + 1) * chip_rows] for i in range(groups)], axis=1))
        partners.append(ref[count:count + 1, :chip_rows])
    peak = functools.reduce(jnp.maximum, parts)
    mass = functools.reduce(lambda a, b: a + b, [jnp.exp2(part - peak) for part in parts])
    totals = peak + jnp.log(mass) * LOG2E
    partner_row = jnp.concatenate(partners, axis=1)
    packed = jnp.concatenate(
        [totals[:count], partner_row, jnp.zeros((LANES - count - 1, total), jnp.float32)], axis=0)
    col_ref[...] = packed.T
    zero_or = lambda keep, x: jnp.where(keep, x, jnp.zeros_like(x))
    document_row = document_ids((1, total), 1, me | 1, own_rows, masks)
    id_row = jnp.where(lead, document_row, partner_row)
    shifts = [math.log2(s) for s in scales]
    total_rows = [zero_or(jnp.logical_not(lead), totals[k:k + 1]) - shifts[k] for k in range(count)]

    narrow = [m for m in uppers if m <= LANES]
    for step in range(total // block):
        rows = pl.ds(step * block, block)
        document_col = document_ids((block, 1), 0, me | 1, own_rows, masks, step * block)
        id_col = jnp.where(lead, col_ref[rows, count:count + 1], document_col)
        hit = id_col == id_row
        for k, s in enumerate(prefix_scores(v_ref, w_ref, rows, uppers)):
            score_ref[k] = s
        running = None
        stack = []
        for k in reversed(range(count)):
            gain = scales[k] * LOG2E
            total_col = zero_or(lead, col_ref[rows, k:k + 1])
            weight = jnp.exp2(score_ref[k] * gain - total_col - total_rows[k])
            weight = weight - jnp.where(hit, scales[k], 0.0)
            running = weight if running is None else running + weight
            band = running.astype(jnp.bfloat16)
            if k >= len(narrow):
                lower, upper = uppers[k - 1], uppers[k]
                product = jnp.dot(band, w_ref[:, lower:upper], preferred_element_type=jnp.float32)
                store(out_refs, product, step * block, lower, upper, chip_rows)
            else:
                stack.append(band)
        product = jnp.dot(
            jnp.concatenate(stack, axis=0), w_ref[:, :LANES], preferred_element_type=jnp.float32)
        lane = lax.broadcasted_iota(jnp.int32, (block, LANES), 1)
        chosen = product[:block]
        for at_stack in range(1, len(stack)):
            k = len(narrow) - 1 - at_stack
            chosen = jnp.where(
                lane < uppers[k], product[at_stack * block:(at_stack + 1) * block], chosen)
        store(out_refs, chosen, step * block, 0, LANES, chip_rows)


def rows_of(refs, lower, upper):
    return jnp.concatenate([ref[:, lower:upper] for ref in refs], axis=0)


def subtile_scores(v_refs, w_refs, uppers):
    narrow = [m for m in uppers if m <= LANES]
    left, right = rows_of(v_refs, 0, LANES), rows_of(w_refs, 0, LANES)
    slim = right.shape[0] < 2 * LANES
    head = right if slim else left
    count = head.shape[0]
    lane = lax.broadcasted_iota(jnp.int32, head.shape, 1)
    masked = jnp.concatenate(
        [jnp.where(lane < m, head, jnp.zeros_like(head)) for m in narrow], axis=0)
    if slim:
        stacked = transposed_dot(left, masked)
        parts = [stacked[:, k * count:(k + 1) * count] for k in range(len(narrow))]
    else:
        stacked = transposed_dot(masked, right)
        parts = [stacked[k * count:(k + 1) * count] for k in range(len(narrow))]
    yield from parts
    lower, running = narrow[-1], parts[-1]
    for upper in uppers[len(narrow):]:
        running = running + transposed_dot(
            rows_of(v_refs, lower, upper), rows_of(w_refs, lower, upper))
        yield running
        lower = upper


def subtile(lead, v_refs, w_refs, uppers, refs):
    power_ref, col_ref, line_ref = refs
    gains = [logit_gain * m ** -0.5 * LOG2E for m in uppers]
    count, across = power_ref.shape[1:]

    @pl.when(lead)
    def _():
        lane = lax.broadcasted_iota(jnp.int32, (count, LANES), 1)
        both = jnp.where(lane < STATS, 0.0, 1.0)
        for k, s in enumerate(subtile_scores(v_refs, w_refs, uppers)):
            logits = s * gains[k]
            peak = jnp.max(logits, axis=1, keepdims=True)
            power = jnp.exp2(logits - peak)
            power_ref[k] = power
            both = jnp.where(lane == k, peak, both)
            both = jnp.where(lane == STATS + k, jnp.sum(power, axis=1, keepdims=True), both)
        col_ref[...] = both
        line_ref[:, :count] = both.T[:2 * STATS]

    @pl.when(jnp.logical_not(lead))
    def _():
        line_ref[:STATS, :] = jnp.zeros((STATS, line_ref.shape[1]), jnp.float32)
        line_ref[STATS:, :] = jnp.ones((STATS, line_ref.shape[1]), jnp.float32)
        for k, s in enumerate(subtile_scores(v_refs, w_refs, uppers)):
            logits = s * gains[k]
            peak = jnp.max(logits, axis=0, keepdims=True)
            power = jnp.exp2(logits - peak)
            power_ref[k] = power
            line_ref[k:k + 1, :across] = peak
            line_ref[STATS + k:STATS + k + 1, :across] = jnp.sum(power, axis=0, keepdims=True)


def log_sum(pairs):
    top = functools.reduce(jnp.maximum, [peak for peak, _ in pairs])
    mass = functools.reduce(
        lambda a, b: a + b, [mass * jnp.exp2(peak - top) for peak, mass in pairs])
    return top + jnp.log(mass) * LOG2E


def tile_kernel(span, counts, uppers, own_rows, finish, *refs):
    groups = len(counts)
    shapes = subtiles(groups)
    tiles = [shapes[i] for i in span]
    r0, r1, c0, c1 = extent(tiles)
    me_ref, partner_ref = refs[:2]
    at = 2 + sum(counts[r0:r1])
    v_refs, w_refs = refs[2:at], refs[at:at + sum(counts[c0:c1])]
    at += sum(counts[c0:c1])
    earlier = refs[at:at + finish]
    outs = refs[at + finish:]
    lead = (me_ref[0] & 1) == 0
    for i, (t0, t1, u0, u1) in enumerate(tiles):
        subtile(
            lead, v_refs[sum(counts[r0:t0]):sum(counts[r0:t1])],
            w_refs[sum(counts[c0:u0]):sum(counts[c0:u1])], uppers, outs[3 * i:3 * i + 3])
    if not finish:
        outs[-1][...] = partner_ref[...]
        return
    stats_ref = outs[-1]
    every = [*earlier, *outs[2:3 * len(tiles):3]]
    segments = segments_of(groups)
    chip_rows = 2 * own_rows

    def merge(axis):
        for s0, s1 in segments:
            pairs = []
            for shape, line in zip(shapes, every):
                low, high = shape[axis:axis + 2]
                if low <= s0 and s1 <= high:
                    at = slice((s0 - low) * chip_rows, (s1 - low) * chip_rows)
                    pairs.append((line[:STATS, at], line[STATS:, at]))
            stats_ref[:, s0 * chip_rows:s1 * chip_rows] = log_sum(pairs)

    pl.when(lead)(lambda: merge(0))
    pl.when(jnp.logical_not(lead))(lambda: merge(2))

    count = len(uppers)
    stats_ref[count:count + 1, :chip_rows] = partner_ref[...]


def segments_of(groups):
    low, middle = groups // 2, groups // 2 + groups // 4
    return [(0, low), (low, middle), (middle, groups)]


def subtiles(groups):
    (_, low), (_, middle), _ = segments_of(groups)
    return [(0, low, 0, low), (low, middle, 0, low), (0, middle, low, middle),
            (middle, groups, 0, middle), (0, groups, middle, groups)]


def extent(tiles):
    first, second, third, fourth = zip(*tiles)
    return min(first), max(second), min(third), max(fourth)


def band_setup(groups, uppers, own_rows, masks, me_ref, stat_refs):
    count = len(uppers)
    total = stat_refs[0].shape[1]
    chip_rows = total // groups
    me = me_ref[0]
    lead = (me & 1) == 0
    own, first, second, swapped = [ref[...] for ref in stat_refs]
    values = [own, jnp.where(lead, first, swapped), second, jnp.where(lead, swapped, first)]
    parts, partners = [], []
    for j, value in enumerate(values):
        parts.append(jnp.concatenate(
            [value[:, (i ^ j) * chip_rows:((i ^ j) + 1) * chip_rows] for i in range(groups)], axis=1))
        partners.append(value[count:count + 1, :chip_rows])
    peak = functools.reduce(jnp.maximum, parts)
    mass = functools.reduce(lambda a, b: a + b, [jnp.exp2(part - peak) for part in parts])
    partner_row = jnp.concatenate(partners, axis=1)
    sub = lax.broadcasted_iota(jnp.int32, (STATS, total), 0)
    totals = peak + jnp.log(mass) * LOG2E
    for k in range(count):
        totals = jnp.where(sub == k, totals - math.log2(logit_gain * uppers[k] ** -0.5), totals)
    packed = jnp.concatenate(
        [totals[:count], partner_row, jnp.zeros((LANES - count - 1, total), jnp.float32)], axis=0)
    cols = packed.T
    id_row = jnp.where(
        lead, document_ids((1, total), 1, me | 1, own_rows, masks), partner_row)
    id_col = jnp.where(
        lead, cols[:, count:count + 1],
        document_ids((total, 1), 0, me | 1, own_rows, masks))
    return lead, totals, cols, id_row, id_col


def weights_of(segment, groups, setup, power_refs, col_refs, row_refs):
    lead, totals, cols, _, _ = setup
    chip_rows = totals.shape[1] // groups
    s0, s1 = segment
    strip = []
    for (r0, r1, c0, c1), power, col_peak, line in zip(
            subtiles(groups), power_refs, col_refs, row_refs):
        if r0 <= s0 and s1 <= r1:
            inner = slice((s0 - r0) * chip_rows, (s1 - r0) * chip_rows)
            outer = slice(s0 * chip_rows, s1 * chip_rows)
            across = slice(c0 * chip_rows, c1 * chip_rows)
            strip.append((
                c0, power, inner,
                jnp.where(lead, jnp.exp2(col_peak[inner, :] - cols[outer]), 1.0),
                jnp.where(lead, 1.0, jnp.exp2(line[:STATS, :(c1 - c0) * chip_rows] - totals[:, across]))))
    strip.sort(key=lambda item: item[0])
    return lambda k: jnp.concatenate([
        power[k, inner] * col_gain[:, k:k + 1] * row_gain[k:k + 1, :]
        for _, power, inner, col_gain, row_gain in strip], axis=1)


def last_band_kernel(groups, uppers, own_rows, masks, *refs):
    tiles = len(subtiles(groups))
    setup = band_setup(groups, uppers, own_rows, masks, refs[0], refs[1:1 + groups])
    at = 1 + groups
    power_refs, col_refs, row_refs = [refs[at + i * tiles:at + (i + 1) * tiles] for i in range(3)]
    segment = segments_of(groups)[-1]
    farthest = segment[1] - segment[0]
    w_refs, out_refs, after_ref = refs[at + 3 * tiles:-farthest - 1], refs[-farthest - 1:-1], refs[-1]
    _, totals, _, id_row, id_col = setup
    chip_rows = totals.shape[1] // groups
    k = len(uppers) - 1
    rows = slice(segment[0] * chip_rows, segment[1] * chip_rows)
    weight = weights_of(segment, groups, setup, power_refs, col_refs, row_refs)(k)
    weight = weight - jnp.where(id_col[rows] == id_row, logit_gain * uppers[k] ** -0.5, 0.0)
    after_ref[...] = weight
    product = jnp.dot(
        weight.astype(jnp.bfloat16), rows_of(w_refs, uppers[k - 1], uppers[k]),
        preferred_element_type=jnp.float32)
    store(out_refs, product, 0, 0, uppers[k] - uppers[k - 1], chip_rows)


def bands_kernel(groups, uppers, own_rows, masks, *refs, block):
    tiles = len(subtiles(groups))
    setup = band_setup(groups, uppers, own_rows, masks, refs[0], refs[1:1 + groups])
    at = 1 + groups
    power_refs, col_refs, row_refs = [refs[at + i * tiles:at + (i + 1) * tiles] for i in range(3)]
    at += 3 * tiles
    far = segments_of(groups)[-1]
    height = block[-1][1] - block[0][0]
    fresh = far[0] - block[0][0] if block[-1] == far else height
    outs = refs[len(refs) - height - fresh:]
    others, widest = outs[:height], outs[height:]
    inputs = refs[at:len(refs) - height - fresh]
    before_ref = inputs[-1] if fresh < height else None
    w_refs = inputs[:-1] if fresh < height else inputs
    _, totals, _, id_row, id_col = setup
    chip_rows = totals.shape[1] // groups
    height, fresh = height * chip_rows, fresh * chip_rows
    first = block[0][0] * chip_rows
    scales = [logit_gain * m ** -0.5 for m in uppers]
    last = len(uppers) - 1
    narrow = [k for k in range(last, -1, -1) if uppers[k] <= LANES]
    hit = id_col[first:first + height] == id_row
    weights = [
        weights_of(segment, groups, setup, power_refs, col_refs, row_refs) for segment in block]
    running = weights[0](last) - jnp.where(hit[:fresh], scales[last], 0.0)
    lower, upper = uppers[last - 1], uppers[last]
    product = jnp.dot(
        running.astype(jnp.bfloat16), rows_of(w_refs, lower, upper),
        preferred_element_type=jnp.float32)
    store(widest, product, 0, 0, upper - lower, chip_rows)
    if before_ref is not None:
        running = jnp.concatenate([running, before_ref[...]], axis=0)
    stack = []
    for k in range(last - 1, -1, -1):
        weight = jnp.concatenate([part(k) for part in weights], axis=0)
        running = running + (weight - jnp.where(hit, scales[k], 0.0))
        band = running.astype(jnp.bfloat16)
        if k in narrow:
            stack.append(band)
            continue
        lower, upper = uppers[k - 1], uppers[k]
        product = jnp.dot(band, rows_of(w_refs, lower, upper), preferred_element_type=jnp.float32)
        store(others, product, 0, lower, upper, chip_rows)
    product = jnp.dot(
        jnp.concatenate(stack, axis=0), rows_of(w_refs, 0, LANES),
        preferred_element_type=jnp.float32)
    lane = lax.broadcasted_iota(jnp.int32, (height, LANES), 1)
    chosen = product[:height]
    for i in range(1, len(stack)):
        chosen = jnp.where(
            lane < uppers[narrow[i]], product[i * height:(i + 1) * height], chosen)
    store(others, chosen, 0, 0, LANES, chip_rows)


def store(out_refs, value, first_row, lower, upper, chip_rows):
    for at in range(0, value.shape[0], chip_rows):
        ref = out_refs[(first_row + at) // chip_rows]
        ref[:, lower:upper] = value[at:at + chip_rows].astype(ref.dtype)


def on_device(queries, documents, partner):
    own_rows, feature_dim = queries.shape
    uppers = width_list(feature_dim)
    dp_size, rep_size = lax.axis_size("dp"), lax.axis_size("rep")
    devices = dp_size * rep_size
    bits = devices.bit_length() - 1
    assert rep_size == 2 and devices == 1 << bits and bits % 2 == 1
    stages = (bits - 1) // 2
    groups = 1 << stages
    pieces = 2 * groups
    query_masks = [1 << (2 * s + 1) for s in range(stages)]
    document_masks = [1 << (2 * s + 2) for s in range(stages)]
    total = pieces * own_rows
    chip_rows = 2 * own_rows

    role = lax.axis_index("rep")
    me = (lax.axis_index("dp") * rep_size + role).astype(jnp.int32).reshape(1)
    lead = role == 0

    def exchange(x, masks_of):
        return lax.ppermute(x, AXES, [(i, i ^ masks_of(i)) for i in range(devices)])

    def swap(x):
        return exchange(x, lambda i: 1)

    def along(x, stage):
        return exchange(x, lambda i: document_masks[stage] if i & 1 else query_masks[stage])

    mine = jnp.where(lead, queries, documents)
    other = jnp.where(lead, documents, queries)
    got = swap(other)
    small = groups == 4 and WIDTHS * total * total * 4 <= 16 << 20
    cut = own_rows // 2 if small and own_rows % 32 == 0 else own_rows
    v = {0: [mine, got]}
    w = {0: [swap(mine), other]}
    for stage in reversed(range(stages)):
        for j in sorted(v):
            parts = v[j]
            if cut < own_rows and j == 0 and stage:
                parts = [mine, got[:cut], got[cut:]]
            v[j | 1 << stage] = [
                along(part, stage) for part in parts]
    for j in range(1, groups):
        w[j] = [swap(part) for part in v[j]]
    counts = [len(v[j]) for j in range(groups)]
    v_list = [part for j in range(groups) for part in v[j]]
    w_list = [part for j in range(groups) for part in w[j]]

    own_partner = partner.astype(jnp.float32).reshape(1, own_rows)
    far_partner = swap(own_partner)
    chip_partner = jnp.where(
        lead,
        jnp.concatenate([own_partner, far_partner], axis=1),
        jnp.concatenate([far_partner, own_partner], axis=1))

    vmem = pl.BlockSpec(memory_space=pltpu.VMEM)
    smem = pl.BlockSpec(memory_space=pltpu.SMEM)

    def query_mask(j):
        return sum(mask for s, mask in enumerate(query_masks) if j >> s & 1)

    def gathered(stats):
        return [stats] + [exchange(stats, lambda i: query_mask(j)) for j in range(1, groups)]

    shape = lambda *dims: jax.ShapeDtypeStruct(dims, jnp.float32)

    def gradient_shapes(columns):
        return [
            jax.ShapeDtypeStruct((chip_rows, columns), jnp.bfloat16 if j & 1 else jnp.float32)
            for j in range(groups)]

    if not small:
        limit = 60 << 20
        stats = pl.pallas_call(
            functools.partial(stats_kernel, pieces, uppers),
            out_shape=shape(STATS, total),
            in_specs=[smem] + [vmem] * (1 + 2 * pieces),
            out_specs=vmem,
            scratch_shapes=[
                pltpu.VMEM((total, feature_dim), jnp.bfloat16),
                pltpu.VMEM((total, feature_dim), jnp.bfloat16),
                pltpu.VMEM((total, LANES), jnp.float32),
            ],
            compiler_params=pltpu.CompilerParams(vmem_limit_bytes=limit),
            name="tile_stats",
        )(me, chip_partner, *v_list, *w_list)
        whole = pl.pallas_call(
            functools.partial(grads_kernel, pieces, uppers, own_rows, document_masks),
            out_shape=gradient_shapes(feature_dim),
            in_specs=[smem] + [vmem] * (groups + 2 * pieces),
            out_specs=[vmem] * groups,
            scratch_shapes=[
                pltpu.VMEM((total, feature_dim), jnp.bfloat16),
                pltpu.VMEM((total, feature_dim), jnp.bfloat16),
                pltpu.VMEM((WIDTHS, block_of(total), total), jnp.float32),
                pltpu.VMEM((total, LANES), jnp.float32),
            ],
            compiler_params=pltpu.CompilerParams(vmem_limit_bytes=limit),
            name="tile_grads",
        )(me, *gathered(stats), *v_list, *w_list)
        chunks = [whole]
    else:
        shapes = subtiles(groups)
        limit = 20 << 20
        params = pltpu.CompilerParams(vmem_limit_bytes=limit)

        def tile(span, partner_row, earlier=()):
            first, end, left, right = extent([shapes[i] for i in span])
            operands = v_list[sum(counts[:first]):sum(counts[:end])]
            operands += w_list[sum(counts[:left]):sum(counts[:right])]
            stat_shapes = [shape(STATS, total)] if earlier else [shape(1, chip_rows)]
            result, area = [], 0
            for i in span:
                r0, r1, c0, c1 = shapes[i]
                tall, wide = (r1 - r0) * chip_rows, (c1 - c0) * chip_rows
                area += tall * wide
                result += [shape(WIDTHS, tall, wide), shape(tall, LANES),
                           shape(2 * STATS, max(tall, wide))]
            *arrays, last_array = pl.pallas_call(
                functools.partial(
                    tile_kernel, span, counts, uppers, own_rows, len(earlier)),
                out_shape=result + stat_shapes,
                in_specs=[smem] + [vmem] * (1 + len(operands) + len(earlier)),
                out_specs=[vmem] * (len(result) + 1),
                compiler_params=params,
                cost_estimate=pl.CostEstimate(
                    flops=6 * area * feature_dim, transcendentals=0,
                    bytes_accessed=2 * total * feature_dim),
            )(me, partner_row, *operands, *[one[2] for one in earlier])
            return [arrays[3 * i:3 * i + 3] for i in range(len(span))], last_array

        done, chip_partner = tile([0], chip_partner)
        for at in (1, 2, 3):
            more, chip_partner = tile([at], chip_partner)
            done += more
        more, stats = tile([4], chip_partner, done)
        done += more
        first = exchange(
            stats, lambda i: query_mask(3) if i & 1 else query_mask(1))
        second = exchange(stats, lambda i: query_mask(2))
        swapped = swap(first)
        common = [me, stats, first, second, swapped, *[t[0] for t in done], *[t[1] for t in done],
                  *[t[2] for t in done], *w_list]
        near = segments_of(groups)[-1][0]
        widest = feature_dim - uppers[-2]

        def bands(kernel, more, outs):
            return pl.pallas_call(
                functools.partial(kernel, groups, uppers, own_rows, document_masks),
                out_shape=outs,
                in_specs=[smem] + [vmem] * (len(common) - 1 + len(more)),
                out_specs=[vmem] * len(outs),
                compiler_params=params,
                cost_estimate=pl.CostEstimate(
                    flops=2 * total * total * feature_dim, transcendentals=0,
                    bytes_accessed=4 * total * feature_dim),
            )(*common, *more)

        *far_ones, running = bands(
            last_band_kernel, [],
            gradient_shapes(widest)[near:] + [shape((groups - near) * chip_rows, total)])
        narrow_ones = gradient_shapes(uppers[-2])
        wide_ones = gradient_shapes(widest)
        middle = segments_of(groups)[1]

        def block_of_bands(block, more):
            span = slice(block[0][0], block[-1][1])
            fresh = slice(block[0][0], min(block[-1][1], near))
            result = bands(
                functools.partial(bands_kernel, block=block), more,
                narrow_ones[span] + wide_ones[fresh])
            return result[:span.stop - span.start], result[span.stop - span.start:]

        far_narrow, middle_wide = block_of_bands([middle, (near, groups)], [running])
        next_narrow, next_wide = block_of_bands([(1, 2)], [])
        own_narrow, own_wide = block_of_bands([(0, 1)], [])
        chunks = [
            [*own_wide, *next_wide, *middle_wide, *far_ones],
            [*own_narrow, *next_narrow, *far_narrow]]

    mine_parts, other_parts = [], []
    for c, chunk in enumerate(chunks):
        partial = dict(enumerate(chunk))
        for stage in range(stages - 1):
            step = 1 << stage
            for j in sorted([j for j in partial if j & step], reverse=True):
                arrived = along(partial.pop(j).astype(jnp.bfloat16), stage)
                partial[j ^ step] = partial[j ^ step] + arrived.astype(jnp.float32)
                if stage == stages - 2 and j ^ step:
                    partial[j ^ step] = partial[j ^ step].astype(jnp.bfloat16)
        stage = stages - 1
        outgoing = partial[1 << stage]
        kept = partial[0]
        if c < len(chunks) - 1:
            arrived = along(outgoing, stage)
            kept = kept + arrived.astype(jnp.float32)
            mine_parts.append(kept[:own_rows])
            other_parts.append(swap(kept[own_rows:]))
        else:
            far = lambda i: document_masks[stage] ^ 1 if i & 1 else query_masks[stage] ^ 1
            near_arrived = along(outgoing[:own_rows], stage)
            far_arrived = exchange(outgoing[own_rows:], far)
            ours, theirs = lax.optimization_barrier((kept[:own_rows], kept[own_rows:]))
            mine_parts.append(ours + near_arrived.astype(jnp.float32))
            other_parts.append(swap(theirs) + far_arrived.astype(jnp.float32))
    mine_parts, other_parts = mine_parts[::-1], other_parts[::-1]
    ours = jnp.concatenate(mine_parts, axis=1)
    theirs = jnp.concatenate(other_parts, axis=1)
    return jnp.where(lead, ours, theirs), jnp.where(lead, theirs, ours)


def solution(mesh):
    return jax.shard_map(
        on_device,
        mesh=mesh,
        in_specs=(P(AXES, None), P(AXES, None), P(AXES)),
        out_specs=(P(AXES, None), P(AXES, None)),
        check_vma=False,
    )
```

```python
import functools
import math

import jax
import jax.numpy as jnp
from jax import lax
from jax.experimental import pallas as pl
from jax.experimental.pallas import tpu as pltpu
from jax.sharding import PartitionSpec as P


WIDTHS = 9
AXES = ("dp", "rep")
LOG2E = 1.4426950408889634
STATS = 16
LANES = 128


logit_gain = 3.0


def width_list(feature_dim):
    return [feature_dim >> WIDTHS - 1 - nested for nested in range(WIDTHS)]


def transposed_dot(a, b):
    return lax.dot_general(a, b, (((1,), (1,)), ((), ())), preferred_element_type=jnp.float32)


def prefix_scores(v_ref, w_ref, rows, uppers):
    narrow = [m for m in uppers if m <= LANES]
    count = rows.size
    head = v_ref[rows, :LANES]
    lane = lax.broadcasted_iota(jnp.int32, head.shape, 1)
    masked = [jnp.where(lane < m, head, jnp.zeros_like(head)) for m in narrow]
    stacked = transposed_dot(jnp.concatenate(masked, axis=0), w_ref[:, :LANES])
    result = [stacked[k * count:(k + 1) * count] for k in range(len(narrow))]
    lower = narrow[-1]
    for upper in uppers[len(narrow):]:
        part = transposed_dot(v_ref[rows, lower:upper], w_ref[:, lower:upper])
        result.append(result[-1] + part)
        lower = upper
    return result


def block_of(total):
    return min(total, 256)


def load_tile(refs, scratch):
    at = 0
    for ref in refs:
        scratch[at:at + ref.shape[0], :] = ref[...]
        at += ref.shape[0]


def stats_kernel(pieces, uppers, *refs):
    role_ref, partner_ref = refs[:2]
    v_refs, w_refs = refs[2:2 + pieces], refs[2 + pieces:2 + 2 * pieces]
    out_ref, v_ref, w_ref, col_ref = refs[2 + 2 * pieces:]
    load_tile(v_refs, v_ref)
    load_tile(w_refs, w_ref)
    total = v_ref.shape[0]
    block = block_of(total)
    steps = total // block
    gains = [logit_gain * m ** -0.5 * LOG2E for m in uppers]
    own = partner_ref.shape[1]
    out_ref[...] = jnp.zeros_like(out_ref)

    @pl.when((role_ref[0] & 1) == 0)
    def _():
        for step in range(steps):
            rows = pl.ds(step * block, block)
            col_ref[rows, :] = jnp.zeros((block, LANES), jnp.float32)
            for k, s in enumerate(prefix_scores(v_ref, w_ref, rows, uppers)):
                logits = s * gains[k]
                peak = jnp.max(logits, axis=1, keepdims=True)
                mass = jnp.sum(jnp.exp2(logits - peak), axis=1, keepdims=True)
                col_ref[rows, k:k + 1] = peak + jnp.log(mass) * LOG2E
        out_ref[...] = col_ref[...].T[:STATS]

    @pl.when((role_ref[0] & 1) != 0)
    def _():
        peaks, masses = [None] * len(uppers), [None] * len(uppers)
        for step in range(steps):
            rows = pl.ds(step * block, block)
            for k, s in enumerate(prefix_scores(v_ref, w_ref, rows, uppers)):
                logits = s * gains[k]
                peak = jnp.max(logits, axis=0, keepdims=True)
                mass = jnp.sum(jnp.exp2(logits - peak), axis=0, keepdims=True)
                if step:
                    top = jnp.maximum(peak, peaks[k])
                    mass = mass * jnp.exp2(peak - top) + masses[k] * jnp.exp2(peaks[k] - top)
                    peak = top
                peaks[k], masses[k] = peak, mass
        for k in range(len(uppers)):
            out_ref[k:k + 1, :] = peaks[k] + jnp.log(masses[k]) * LOG2E

    out_ref[len(uppers):len(uppers) + 1, :own] = partner_ref[...]


def document_ids(shape, axis, first, own_rows, masks, start=0):
    at = lax.broadcasted_iota(jnp.int32, shape, axis) + start
    shift = own_rows.bit_length() - 1
    piece = at >> shift
    device = first ^ (piece & 1)
    for s, mask in enumerate(masks):
        device = device ^ (((piece >> (1 + s)) & 1) * mask)
    return (device * own_rows + (at & (own_rows - 1))).astype(jnp.float32)


def grads_kernel(pieces, uppers, own_rows, masks, *refs):
    me_ref = refs[0]
    groups = pieces // 2
    stat_refs = refs[1:1 + groups]
    v_refs = refs[1 + groups:1 + groups + pieces]
    w_refs = refs[1 + groups + pieces:1 + groups + 2 * pieces]
    out_refs = refs[1 + groups + 2 * pieces:1 + 2 * groups + 2 * pieces]
    v_ref, w_ref, score_ref, col_ref = refs[1 + 2 * groups + 2 * pieces:]
    load_tile(v_refs, v_ref)
    load_tile(w_refs, w_ref)
    total = v_ref.shape[0]
    block = block_of(total)
    chip_rows = total // groups
    count = len(uppers)
    scales = [logit_gain * m ** -0.5 for m in uppers]
    me = me_ref[0]
    lead = (me & 1) == 0

    parts = []
    partners = []
    for j, ref in enumerate(stat_refs):
        parts.append(jnp.concatenate(
            [ref[:, (i ^ j) * chip_rows:((i ^ j) + 1) * chip_rows] for i in range(groups)], axis=1))
        partners.append(ref[count:count + 1, :chip_rows])
    peak = functools.reduce(jnp.maximum, parts)
    mass = functools.reduce(lambda a, b: a + b, [jnp.exp2(part - peak) for part in parts])
    totals = peak + jnp.log(mass) * LOG2E
    partner_row = jnp.concatenate(partners, axis=1)
    packed = jnp.concatenate(
        [totals[:count], partner_row, jnp.zeros((LANES - count - 1, total), jnp.float32)], axis=0)
    col_ref[...] = packed.T
    zero_or = lambda keep, x: jnp.where(keep, x, jnp.zeros_like(x))
    document_row = document_ids((1, total), 1, me | 1, own_rows, masks)
    id_row = jnp.where(lead, document_row, partner_row)
    shifts = [math.log2(s) for s in scales]
    total_rows = [zero_or(jnp.logical_not(lead), totals[k:k + 1]) - shifts[k] for k in range(count)]

    narrow = [m for m in uppers if m <= LANES]
    for step in range(total // block):
        rows = pl.ds(step * block, block)
        document_col = document_ids((block, 1), 0, me | 1, own_rows, masks, step * block)
        id_col = jnp.where(lead, col_ref[rows, count:count + 1], document_col)
        hit = id_col == id_row
        for k, s in enumerate(prefix_scores(v_ref, w_ref, rows, uppers)):
            score_ref[k] = s
        running = None
        stack = []
        for k in reversed(range(count)):
            gain = scales[k] * LOG2E
            total_col = zero_or(lead, col_ref[rows, k:k + 1])
            weight = jnp.exp2(score_ref[k] * gain - total_col - total_rows[k])
            weight = weight - jnp.where(hit, scales[k], 0.0)
            running = weight if running is None else running + weight
            band = running.astype(jnp.bfloat16)
            if k >= len(narrow):
                lower, upper = uppers[k - 1], uppers[k]
                product = jnp.dot(band, w_ref[:, lower:upper], preferred_element_type=jnp.float32)
                store(out_refs, product, step * block, lower, upper, chip_rows)
            else:
                stack.append(band)
        product = jnp.dot(
            jnp.concatenate(stack, axis=0), w_ref[:, :LANES], preferred_element_type=jnp.float32)
        lane = lax.broadcasted_iota(jnp.int32, (block, LANES), 1)
        chosen = product[:block]
        for at_stack in range(1, len(stack)):
            k = len(narrow) - 1 - at_stack
            chosen = jnp.where(
                lane < uppers[k], product[at_stack * block:(at_stack + 1) * block], chosen)
        store(out_refs, chosen, step * block, 0, LANES, chip_rows)


def rows_of(refs, lower, upper):
    return jnp.concatenate([ref[:, lower:upper] for ref in refs], axis=0)


def subtile_scores(v_refs, w_refs, uppers):
    narrow = [m for m in uppers if m <= LANES]
    left, right = rows_of(v_refs, 0, LANES), rows_of(w_refs, 0, LANES)
    slim = right.shape[0] < 2 * LANES
    head = right if slim else left
    count = head.shape[0]
    lane = lax.broadcasted_iota(jnp.int32, head.shape, 1)
    masked = jnp.concatenate(
        [jnp.where(lane < m, head, jnp.zeros_like(head)) for m in narrow], axis=0)
    if slim:
        stacked = transposed_dot(left, masked)
        parts = [stacked[:, k * count:(k + 1) * count] for k in range(len(narrow))]
    else:
        stacked = transposed_dot(masked, right)
        parts = [stacked[k * count:(k + 1) * count] for k in range(len(narrow))]
    yield from parts
    lower, running = narrow[-1], parts[-1]
    for upper in uppers[len(narrow):]:
        running = running + transposed_dot(
            rows_of(v_refs, lower, upper), rows_of(w_refs, lower, upper))
        yield running
        lower = upper


def subtile(lead, v_refs, w_refs, uppers, refs):
    power_ref, col_ref, line_ref = refs
    gains = [logit_gain * m ** -0.5 * LOG2E for m in uppers]
    count, across = power_ref.shape[1:]

    @pl.when(lead)
    def _():
        lane = lax.broadcasted_iota(jnp.int32, (count, LANES), 1)
        both = jnp.where(lane < STATS, 0.0, 1.0)
        for k, s in enumerate(subtile_scores(v_refs, w_refs, uppers)):
            logits = s * gains[k]
            peak = jnp.max(logits, axis=1, keepdims=True)
            power = jnp.exp2(logits - peak)
            power_ref[k] = power
            both = jnp.where(lane == k, peak, both)
            both = jnp.where(lane == STATS + k, jnp.sum(power, axis=1, keepdims=True), both)
        col_ref[...] = both
        line_ref[:, :count] = both.T[:2 * STATS]

    @pl.when(jnp.logical_not(lead))
    def _():
        line_ref[:STATS, :] = jnp.zeros((STATS, line_ref.shape[1]), jnp.float32)
        line_ref[STATS:, :] = jnp.ones((STATS, line_ref.shape[1]), jnp.float32)
        for k, s in enumerate(subtile_scores(v_refs, w_refs, uppers)):
            logits = s * gains[k]
            peak = jnp.max(logits, axis=0, keepdims=True)
            power = jnp.exp2(logits - peak)
            power_ref[k] = power
            line_ref[k:k + 1, :across] = peak
            line_ref[STATS + k:STATS + k + 1, :across] = jnp.sum(power, axis=0, keepdims=True)


def log_sum(pairs):
    top = functools.reduce(jnp.maximum, [peak for peak, _ in pairs])
    mass = functools.reduce(
        lambda a, b: a + b, [mass * jnp.exp2(peak - top) for peak, mass in pairs])
    return top + jnp.log(mass) * LOG2E


def tile_kernel(span, counts, uppers, own_rows, finish, *refs):
    groups = len(counts)
    shapes = subtiles(groups)
    tiles = [shapes[i] for i in span]
    r0, r1, c0, c1 = extent(tiles)
    me_ref, partner_ref = refs[:2]
    at = 2 + sum(counts[r0:r1])
    v_refs, w_refs = refs[2:at], refs[at:at + sum(counts[c0:c1])]
    at += sum(counts[c0:c1])
    earlier = refs[at:at + finish]
    outs = refs[at + finish:]
    lead = (me_ref[0] & 1) == 0
    for i, (t0, t1, u0, u1) in enumerate(tiles):
        subtile(
            lead, v_refs[sum(counts[r0:t0]):sum(counts[r0:t1])],
            w_refs[sum(counts[c0:u0]):sum(counts[c0:u1])], uppers, outs[3 * i:3 * i + 3])
    if not finish:
        outs[-1][...] = partner_ref[...]
        return
    stats_ref = outs[-1]
    every = [*earlier, *outs[2:3 * len(tiles):3]]
    segments = segments_of(groups)
    chip_rows = 2 * own_rows

    def merge(axis):
        for s0, s1 in segments:
            pairs = []
            for shape, line in zip(shapes, every):
                low, high = shape[axis:axis + 2]
                if low <= s0 and s1 <= high:
                    at = slice((s0 - low) * chip_rows, (s1 - low) * chip_rows)
                    pairs.append((line[:STATS, at], line[STATS:, at]))
            stats_ref[:, s0 * chip_rows:s1 * chip_rows] = log_sum(pairs)

    pl.when(lead)(lambda: merge(0))
    pl.when(jnp.logical_not(lead))(lambda: merge(2))

    count = len(uppers)
    stats_ref[count:count + 1, :chip_rows] = partner_ref[...]


def segments_of(groups):
    low, middle = groups // 2, groups // 2 + groups // 4
    return [(0, low), (low, middle), (middle, groups)]


def subtiles(groups):
    (_, low), (_, middle), _ = segments_of(groups)
    return [(0, low, 0, low), (low, middle, 0, low), (0, middle, low, middle),
            (middle, groups, 0, middle), (0, groups, middle, groups)]


def extent(tiles):
    first, second, third, fourth = zip(*tiles)
    return min(first), max(second), min(third), max(fourth)


def band_setup(groups, uppers, own_rows, masks, me_ref, stat_refs):
    count = len(uppers)
    total = stat_refs[0].shape[1]
    chip_rows = total // groups
    me = me_ref[0]
    lead = (me & 1) == 0
    own, first, second, swapped = [ref[...] for ref in stat_refs]
    values = [own, jnp.where(lead, first, swapped), second, jnp.where(lead, swapped, first)]
    parts, partners = [], []
    for j, value in enumerate(values):
        parts.append(jnp.concatenate(
            [value[:, (i ^ j) * chip_rows:((i ^ j) + 1) * chip_rows] for i in range(groups)], axis=1))
        partners.append(value[count:count + 1, :chip_rows])
    peak = functools.reduce(jnp.maximum, parts)
    mass = functools.reduce(lambda a, b: a + b, [jnp.exp2(part - peak) for part in parts])
    partner_row = jnp.concatenate(partners, axis=1)
    sub = lax.broadcasted_iota(jnp.int32, (STATS, total), 0)
    totals = peak + jnp.log(mass) * LOG2E
    for k in range(count):
        totals = jnp.where(sub == k, totals - math.log2(logit_gain * uppers[k] ** -0.5), totals)
    packed = jnp.concatenate(
        [totals[:count], partner_row, jnp.zeros((LANES - count - 1, total), jnp.float32)], axis=0)
    cols = packed.T
    id_row = jnp.where(
        lead, document_ids((1, total), 1, me | 1, own_rows, masks), partner_row)
    id_col = jnp.where(
        lead, cols[:, count:count + 1],
        document_ids((total, 1), 0, me | 1, own_rows, masks))
    return lead, totals, cols, id_row, id_col


def weights_of(segment, groups, setup, power_refs, col_refs, row_refs):
    lead, totals, cols, _, _ = setup
    chip_rows = totals.shape[1] // groups
    s0, s1 = segment
    strip = []
    for (r0, r1, c0, c1), power, col_peak, line in zip(
            subtiles(groups), power_refs, col_refs, row_refs):
        if r0 <= s0 and s1 <= r1:
            inner = slice((s0 - r0) * chip_rows, (s1 - r0) * chip_rows)
            outer = slice(s0 * chip_rows, s1 * chip_rows)
            across = slice(c0 * chip_rows, c1 * chip_rows)
            strip.append((
                c0, power, inner,
                jnp.where(lead, jnp.exp2(col_peak[inner, :] - cols[outer]), 1.0),
                jnp.where(lead, 1.0, jnp.exp2(line[:STATS, :(c1 - c0) * chip_rows] - totals[:, across]))))
    strip.sort(key=lambda item: item[0])
    return lambda k: jnp.concatenate([
        power[k, inner] * col_gain[:, k:k + 1] * row_gain[k:k + 1, :]
        for _, power, inner, col_gain, row_gain in strip], axis=1)


def last_band_kernel(groups, uppers, own_rows, masks, split, *refs):
    tiles = len(subtiles(groups))
    setup = band_setup(groups, uppers, own_rows, masks, refs[0], refs[1:1 + groups])
    at = 1 + groups
    power_refs, col_refs, row_refs = [refs[at + i * tiles:at + (i + 1) * tiles] for i in range(3)]
    segment = segments_of(groups)[-1]
    farthest = segment[1] - segment[0]
    w_refs, out_refs, after_ref = refs[at + 3 * tiles:-farthest - 1], refs[-farthest - 1:-1], refs[-1]
    _, totals, _, id_row, id_col = setup
    chip_rows = totals.shape[1] // groups
    k = len(uppers) - 1
    rows = slice(segment[0] * chip_rows, segment[1] * chip_rows)
    weight = weights_of(segment, groups, setup, power_refs, col_refs, row_refs)(k)
    weight = weight - jnp.where(id_col[rows] == id_row, logit_gain * uppers[k] ** -0.5, 0.0)
    after_ref[...] = weight
    product = jnp.dot(
        weight.astype(jnp.bfloat16), rows_of(w_refs, split, uppers[k]),
        preferred_element_type=jnp.float32)
    store(out_refs, product, 0, 0, uppers[k] - split, chip_rows)


def bands_kernel(groups, uppers, own_rows, masks, split, *refs, block):
    tiles = len(subtiles(groups))
    setup = band_setup(groups, uppers, own_rows, masks, refs[0], refs[1:1 + groups])
    at = 1 + groups
    power_refs, col_refs, row_refs = [refs[at + i * tiles:at + (i + 1) * tiles] for i in range(3)]
    at += 3 * tiles
    far = segments_of(groups)[-1]
    height = block[-1][1] - block[0][0]
    fresh = far[0] - block[0][0] if block[-1] == far else height
    outs = refs[len(refs) - height - fresh:]
    others, widest = outs[:height], outs[height:]
    inputs = refs[at:len(refs) - height - fresh]
    before_ref = inputs[-1] if fresh < height else None
    w_refs = inputs[:-1] if fresh < height else inputs
    _, totals, _, id_row, id_col = setup
    chip_rows = totals.shape[1] // groups
    height, fresh = height * chip_rows, fresh * chip_rows
    first = block[0][0] * chip_rows
    scales = [logit_gain * m ** -0.5 for m in uppers]
    last = len(uppers) - 1
    narrow = [k for k in range(last, -1, -1) if uppers[k] <= LANES]
    hit = id_col[first:first + height] == id_row
    weights = [
        weights_of(segment, groups, setup, power_refs, col_refs, row_refs) for segment in block]
    running = weights[0](last) - jnp.where(hit[:fresh], scales[last], 0.0)
    product = jnp.dot(
        running.astype(jnp.bfloat16), rows_of(w_refs, split, uppers[last]),
        preferred_element_type=jnp.float32)
    store(widest, product, 0, 0, uppers[last] - split, chip_rows)
    if before_ref is not None:
        running = jnp.concatenate([running, before_ref[...]], axis=0)
    product = jnp.dot(
        running.astype(jnp.bfloat16), rows_of(w_refs, uppers[last - 1], split),
        preferred_element_type=jnp.float32)
    store(others, product, 0, uppers[last - 1], split, chip_rows)
    stack = []
    for k in range(last - 1, -1, -1):
        weight = jnp.concatenate([part(k) for part in weights], axis=0)
        running = running + (weight - jnp.where(hit, scales[k], 0.0))
        band = running.astype(jnp.bfloat16)
        if k in narrow:
            stack.append(band)
            continue
        lower, upper = uppers[k - 1], uppers[k]
        product = jnp.dot(band, rows_of(w_refs, lower, upper), preferred_element_type=jnp.float32)
        store(others, product, 0, lower, upper, chip_rows)
    product = jnp.dot(
        jnp.concatenate(stack, axis=0), rows_of(w_refs, 0, LANES),
        preferred_element_type=jnp.float32)
    lane = lax.broadcasted_iota(jnp.int32, (height, LANES), 1)
    chosen = product[:height]
    for i in range(1, len(stack)):
        chosen = jnp.where(
            lane < uppers[narrow[i]], product[i * height:(i + 1) * height], chosen)
    store(others, chosen, 0, 0, LANES, chip_rows)


def store(out_refs, value, first_row, lower, upper, chip_rows):
    for at in range(0, value.shape[0], chip_rows):
        ref = out_refs[(first_row + at) // chip_rows]
        ref[:, lower:upper] = value[at:at + chip_rows].astype(ref.dtype)


def on_device(queries, documents, partner):
    own_rows, feature_dim = queries.shape
    uppers = width_list(feature_dim)
    dp_size, rep_size = lax.axis_size("dp"), lax.axis_size("rep")
    devices = dp_size * rep_size
    bits = devices.bit_length() - 1
    assert rep_size == 2 and devices == 1 << bits and bits % 2 == 1
    stages = (bits - 1) // 2
    groups = 1 << stages
    pieces = 2 * groups
    query_masks = [1 << (2 * s + 1) for s in range(stages)]
    document_masks = [1 << (2 * s + 2) for s in range(stages)]
    total = pieces * own_rows
    chip_rows = 2 * own_rows

    role = lax.axis_index("rep")
    me = (lax.axis_index("dp") * rep_size + role).astype(jnp.int32).reshape(1)
    lead = role == 0

    def exchange(x, masks_of):
        return lax.ppermute(x, AXES, [(i, i ^ masks_of(i)) for i in range(devices)])

    def swap(x):
        return exchange(x, lambda i: 1)

    def along(x, stage):
        return exchange(x, lambda i: document_masks[stage] if i & 1 else query_masks[stage])

    mine = jnp.where(lead, queries, documents)
    other = jnp.where(lead, documents, queries)
    got = swap(other)
    small = groups == 4 and WIDTHS * total * total * 4 <= 16 << 20
    cut = own_rows // 2 if small and own_rows % 32 == 0 else own_rows
    v = {0: [mine, got]}
    w = {0: [swap(mine), other]}
    for stage in reversed(range(stages)):
        for j in sorted(v):
            parts = v[j]
            if cut < own_rows and j == 0 and stage:
                parts = [mine, got[:cut], got[cut:]]
            v[j | 1 << stage] = [
                along(part, stage) for part in parts]
    for j in range(1, groups):
        w[j] = [swap(part) for part in v[j]]
    counts = [len(v[j]) for j in range(groups)]
    v_list = [part for j in range(groups) for part in v[j]]
    w_list = [part for j in range(groups) for part in w[j]]

    own_partner = partner.astype(jnp.float32).reshape(1, own_rows)
    far_partner = swap(own_partner)
    chip_partner = jnp.where(
        lead,
        jnp.concatenate([own_partner, far_partner], axis=1),
        jnp.concatenate([far_partner, own_partner], axis=1))

    vmem = pl.BlockSpec(memory_space=pltpu.VMEM)
    smem = pl.BlockSpec(memory_space=pltpu.SMEM)

    def query_mask(j):
        return sum(mask for s, mask in enumerate(query_masks) if j >> s & 1)

    def gathered(stats):
        return [stats] + [exchange(stats, lambda i: query_mask(j)) for j in range(1, groups)]

    shape = lambda *dims: jax.ShapeDtypeStruct(dims, jnp.float32)

    def gradient_shapes(columns):
        return [
            jax.ShapeDtypeStruct((chip_rows, columns), jnp.bfloat16 if j & 1 else jnp.float32)
            for j in range(groups)]

    if not small:
        limit = 60 << 20
        stats = pl.pallas_call(
            functools.partial(stats_kernel, pieces, uppers),
            out_shape=shape(STATS, total),
            in_specs=[smem] + [vmem] * (1 + 2 * pieces),
            out_specs=vmem,
            scratch_shapes=[
                pltpu.VMEM((total, feature_dim), jnp.bfloat16),
                pltpu.VMEM((total, feature_dim), jnp.bfloat16),
                pltpu.VMEM((total, LANES), jnp.float32),
            ],
            compiler_params=pltpu.CompilerParams(vmem_limit_bytes=limit),
            name="tile_stats",
        )(me, chip_partner, *v_list, *w_list)
        whole = pl.pallas_call(
            functools.partial(grads_kernel, pieces, uppers, own_rows, document_masks),
            out_shape=gradient_shapes(feature_dim),
            in_specs=[smem] + [vmem] * (groups + 2 * pieces),
            out_specs=[vmem] * groups,
            scratch_shapes=[
                pltpu.VMEM((total, feature_dim), jnp.bfloat16),
                pltpu.VMEM((total, feature_dim), jnp.bfloat16),
                pltpu.VMEM((WIDTHS, block_of(total), total), jnp.float32),
                pltpu.VMEM((total, LANES), jnp.float32),
            ],
            compiler_params=pltpu.CompilerParams(vmem_limit_bytes=limit),
            name="tile_grads",
        )(me, *gathered(stats), *v_list, *w_list)
        chunks = [whole]
    else:
        shapes = subtiles(groups)
        limit = 20 << 20
        params = pltpu.CompilerParams(vmem_limit_bytes=limit)

        def tile(span, partner_row, earlier=()):
            first, end, left, right = extent([shapes[i] for i in span])
            operands = v_list[sum(counts[:first]):sum(counts[:end])]
            operands += w_list[sum(counts[:left]):sum(counts[:right])]
            stat_shapes = [shape(STATS, total)] if earlier else [shape(1, chip_rows)]
            result, area = [], 0
            for i in span:
                r0, r1, c0, c1 = shapes[i]
                tall, wide = (r1 - r0) * chip_rows, (c1 - c0) * chip_rows
                area += tall * wide
                result += [shape(WIDTHS, tall, wide), shape(tall, LANES),
                           shape(2 * STATS, max(tall, wide))]
            *arrays, last_array = pl.pallas_call(
                functools.partial(
                    tile_kernel, span, counts, uppers, own_rows, len(earlier)),
                out_shape=result + stat_shapes,
                in_specs=[smem] + [vmem] * (1 + len(operands) + len(earlier)),
                out_specs=[vmem] * (len(result) + 1),
                compiler_params=params,
                cost_estimate=pl.CostEstimate(
                    flops=6 * area * feature_dim, transcendentals=0,
                    bytes_accessed=2 * total * feature_dim),
            )(me, partner_row, *operands, *[one[2] for one in earlier])
            return [arrays[3 * i:3 * i + 3] for i in range(len(span))], last_array

        done, chip_partner = tile([0], chip_partner)
        for at in (1, 2, 3):
            more, chip_partner = tile([at], chip_partner)
            done += more
        more, stats = tile([4], chip_partner, done)
        done += more
        first = exchange(
            stats, lambda i: query_mask(3) if i & 1 else query_mask(1))
        second = exchange(stats, lambda i: query_mask(2))
        swapped = swap(first)
        common = [me, stats, first, second, swapped, *[t[0] for t in done], *[t[1] for t in done],
                  *[t[2] for t in done], *w_list]
        near = segments_of(groups)[-1][0]
        split = uppers[-2] + (feature_dim - uppers[-2]) // 4
        widest = feature_dim - split

        def bands(kernel, more, outs):
            return pl.pallas_call(
                functools.partial(kernel, groups, uppers, own_rows, document_masks, split),
                out_shape=outs,
                in_specs=[smem] + [vmem] * (len(common) - 1 + len(more)),
                out_specs=[vmem] * len(outs),
                compiler_params=params,
                cost_estimate=pl.CostEstimate(
                    flops=2 * total * total * feature_dim, transcendentals=0,
                    bytes_accessed=4 * total * feature_dim),
            )(*common, *more)

        *far_ones, running = bands(
            last_band_kernel, [],
            gradient_shapes(widest)[near:] + [shape((groups - near) * chip_rows, total)])
        narrow_ones = gradient_shapes(split)
        wide_ones = gradient_shapes(widest)
        middle = segments_of(groups)[1]

        def block_of_bands(block, more):
            span = slice(block[0][0], block[-1][1])
            fresh = slice(block[0][0], min(block[-1][1], near))
            result = bands(
                functools.partial(bands_kernel, block=block), more,
                narrow_ones[span] + wide_ones[fresh])
            return result[:span.stop - span.start], result[span.stop - span.start:]

        far_narrow, middle_wide = block_of_bands([middle, (near, groups)], [running])
        next_narrow, next_wide = block_of_bands([(1, 2)], [])
        own_narrow, own_wide = block_of_bands([(0, 1)], [])
        chunks = [
            [*own_wide, *next_wide, *middle_wide, *far_ones],
            [*own_narrow, *next_narrow, *far_narrow]]

    mine_parts, other_parts = [], []
    for c, chunk in enumerate(chunks):
        partial = dict(enumerate(chunk))
        for stage in range(stages - 1):
            step = 1 << stage
            for j in sorted([j for j in partial if j & step], reverse=True):
                arrived = along(partial.pop(j).astype(jnp.bfloat16), stage)
                partial[j ^ step] = partial[j ^ step] + arrived.astype(jnp.float32)
                if stage == stages - 2 and j ^ step:
                    partial[j ^ step] = partial[j ^ step].astype(jnp.bfloat16)
        stage = stages - 1
        outgoing = partial[1 << stage]
        kept = partial[0]
        if c < len(chunks) - 1:
            arrived = along(outgoing, stage)
            kept = kept + arrived.astype(jnp.float32)
            mine_parts.append(kept[:own_rows])
            other_parts.append(swap(kept[own_rows:]))
        else:
            far = lambda i: document_masks[stage] ^ 1 if i & 1 else query_masks[stage] ^ 1
            near_arrived = along(outgoing[:own_rows], stage)
            far_arrived = exchange(outgoing[own_rows:], far)
            ours, theirs = lax.optimization_barrier((kept[:own_rows], kept[own_rows:]))
            mine_parts.append(ours + near_arrived.astype(jnp.float32))
            other_parts.append(swap(theirs) + far_arrived.astype(jnp.float32))
    mine_parts, other_parts = mine_parts[::-1], other_parts[::-1]
    ours = jnp.concatenate(mine_parts, axis=1)
    theirs = jnp.concatenate(other_parts, axis=1)
    return jnp.where(lead, ours, theirs), jnp.where(lead, theirs, ours)


def solution(mesh):
    return jax.shard_map(
        on_device,
        mesh=mesh,
        in_specs=(P(AXES, None), P(AXES, None), P(AXES)),
        out_specs=(P(AXES, None), P(AXES, None)),
        check_vma=False,
    )
```

```python
import functools
import math

import jax
import jax.numpy as jnp
from jax import lax
from jax.experimental import pallas as pl
from jax.experimental.pallas import tpu as pltpu
from jax.sharding import PartitionSpec as P


WIDTHS = 9
AXES = ("dp", "rep")
LOG2E = 1.4426950408889634
STATS = 16
LANES = 128


logit_gain = 3.0


def width_list(feature_dim):
    return [feature_dim >> WIDTHS - 1 - nested for nested in range(WIDTHS)]


def transposed_dot(a, b):
    return lax.dot_general(a, b, (((1,), (1,)), ((), ())), preferred_element_type=jnp.float32)


def prefix_scores(v_ref, w_ref, rows, uppers):
    narrow = [m for m in uppers if m <= LANES]
    count = rows.size
    head = v_ref[rows, :LANES]
    lane = lax.broadcasted_iota(jnp.int32, head.shape, 1)
    masked = [jnp.where(lane < m, head, jnp.zeros_like(head)) for m in narrow]
    stacked = transposed_dot(jnp.concatenate(masked, axis=0), w_ref[:, :LANES])
    result = [stacked[k * count:(k + 1) * count] for k in range(len(narrow))]
    lower = narrow[-1]
    for upper in uppers[len(narrow):]:
        part = transposed_dot(v_ref[rows, lower:upper], w_ref[:, lower:upper])
        result.append(result[-1] + part)
        lower = upper
    return result


def block_of(total):
    return min(total, 256)


def load_tile(refs, scratch):
    at = 0
    for ref in refs:
        scratch[at:at + ref.shape[0], :] = ref[...]
        at += ref.shape[0]


def stats_kernel(pieces, uppers, *refs):
    role_ref, partner_ref = refs[:2]
    v_refs, w_refs = refs[2:2 + pieces], refs[2 + pieces:2 + 2 * pieces]
    out_ref, v_ref, w_ref, col_ref = refs[2 + 2 * pieces:]
    load_tile(v_refs, v_ref)
    load_tile(w_refs, w_ref)
    total = v_ref.shape[0]
    block = block_of(total)
    steps = total // block
    gains = [logit_gain * m ** -0.5 * LOG2E for m in uppers]
    own = partner_ref.shape[1]
    out_ref[...] = jnp.zeros_like(out_ref)

    @pl.when((role_ref[0] & 1) == 0)
    def _():
        for step in range(steps):
            rows = pl.ds(step * block, block)
            col_ref[rows, :] = jnp.zeros((block, LANES), jnp.float32)
            for k, s in enumerate(prefix_scores(v_ref, w_ref, rows, uppers)):
                logits = s * gains[k]
                peak = jnp.max(logits, axis=1, keepdims=True)
                mass = jnp.sum(jnp.exp2(logits - peak), axis=1, keepdims=True)
                col_ref[rows, k:k + 1] = peak + jnp.log(mass) * LOG2E
        out_ref[...] = col_ref[...].T[:STATS]

    @pl.when((role_ref[0] & 1) != 0)
    def _():
        peaks, masses = [None] * len(uppers), [None] * len(uppers)
        for step in range(steps):
            rows = pl.ds(step * block, block)
            for k, s in enumerate(prefix_scores(v_ref, w_ref, rows, uppers)):
                logits = s * gains[k]
                peak = jnp.max(logits, axis=0, keepdims=True)
                mass = jnp.sum(jnp.exp2(logits - peak), axis=0, keepdims=True)
                if step:
                    top = jnp.maximum(peak, peaks[k])
                    mass = mass * jnp.exp2(peak - top) + masses[k] * jnp.exp2(peaks[k] - top)
                    peak = top
                peaks[k], masses[k] = peak, mass
        for k in range(len(uppers)):
            out_ref[k:k + 1, :] = peaks[k] + jnp.log(masses[k]) * LOG2E

    out_ref[len(uppers):len(uppers) + 1, :own] = partner_ref[...]


def document_ids(shape, axis, first, own_rows, masks, start=0):
    at = lax.broadcasted_iota(jnp.int32, shape, axis) + start
    shift = own_rows.bit_length() - 1
    piece = at >> shift
    device = first ^ (piece & 1)
    for s, mask in enumerate(masks):
        device = device ^ (((piece >> (1 + s)) & 1) * mask)
    return (device * own_rows + (at & (own_rows - 1))).astype(jnp.float32)


def grads_kernel(pieces, uppers, own_rows, masks, *refs):
    me_ref = refs[0]
    groups = pieces // 2
    stat_refs = refs[1:1 + groups]
    v_refs = refs[1 + groups:1 + groups + pieces]
    w_refs = refs[1 + groups + pieces:1 + groups + 2 * pieces]
    out_refs = refs[1 + groups + 2 * pieces:1 + 2 * groups + 2 * pieces]
    v_ref, w_ref, score_ref, col_ref = refs[1 + 2 * groups + 2 * pieces:]
    load_tile(v_refs, v_ref)
    load_tile(w_refs, w_ref)
    total = v_ref.shape[0]
    block = block_of(total)
    chip_rows = total // groups
    count = len(uppers)
    scales = [logit_gain * m ** -0.5 for m in uppers]
    me = me_ref[0]
    lead = (me & 1) == 0

    parts = []
    partners = []
    for j, ref in enumerate(stat_refs):
        parts.append(jnp.concatenate(
            [ref[:, (i ^ j) * chip_rows:((i ^ j) + 1) * chip_rows] for i in range(groups)], axis=1))
        partners.append(ref[count:count + 1, :chip_rows])
    peak = functools.reduce(jnp.maximum, parts)
    mass = functools.reduce(lambda a, b: a + b, [jnp.exp2(part - peak) for part in parts])
    totals = peak + jnp.log(mass) * LOG2E
    partner_row = jnp.concatenate(partners, axis=1)
    packed = jnp.concatenate(
        [totals[:count], partner_row, jnp.zeros((LANES - count - 1, total), jnp.float32)], axis=0)
    col_ref[...] = packed.T
    zero_or = lambda keep, x: jnp.where(keep, x, jnp.zeros_like(x))
    document_row = document_ids((1, total), 1, me | 1, own_rows, masks)
    id_row = jnp.where(lead, document_row, partner_row)
    shifts = [math.log2(s) for s in scales]
    total_rows = [zero_or(jnp.logical_not(lead), totals[k:k + 1]) - shifts[k] for k in range(count)]

    narrow = [m for m in uppers if m <= LANES]
    for step in range(total // block):
        rows = pl.ds(step * block, block)
        document_col = document_ids((block, 1), 0, me | 1, own_rows, masks, step * block)
        id_col = jnp.where(lead, col_ref[rows, count:count + 1], document_col)
        hit = id_col == id_row
        for k, s in enumerate(prefix_scores(v_ref, w_ref, rows, uppers)):
            score_ref[k] = s
        running = None
        stack = []
        for k in reversed(range(count)):
            gain = scales[k] * LOG2E
            total_col = zero_or(lead, col_ref[rows, k:k + 1])
            weight = jnp.exp2(score_ref[k] * gain - total_col - total_rows[k])
            weight = weight - jnp.where(hit, scales[k], 0.0)
            running = weight if running is None else running + weight
            band = running.astype(jnp.bfloat16)
            if k >= len(narrow):
                lower, upper = uppers[k - 1], uppers[k]
                product = jnp.dot(band, w_ref[:, lower:upper], preferred_element_type=jnp.float32)
                store(out_refs, product, step * block, lower, upper, chip_rows)
            else:
                stack.append(band)
        product = jnp.dot(
            jnp.concatenate(stack, axis=0), w_ref[:, :LANES], preferred_element_type=jnp.float32)
        lane = lax.broadcasted_iota(jnp.int32, (block, LANES), 1)
        chosen = product[:block]
        for at_stack in range(1, len(stack)):
            k = len(narrow) - 1 - at_stack
            chosen = jnp.where(
                lane < uppers[k], product[at_stack * block:(at_stack + 1) * block], chosen)
        store(out_refs, chosen, step * block, 0, LANES, chip_rows)


def rows_of(refs, lower, upper):
    return jnp.concatenate([ref[:, lower:upper] for ref in refs], axis=0)


def subtile_scores(v_refs, w_refs, uppers):
    narrow = [m for m in uppers if m <= LANES]
    left, right = rows_of(v_refs, 0, LANES), rows_of(w_refs, 0, LANES)
    slim = right.shape[0] < 2 * LANES
    head = right if slim else left
    count = head.shape[0]
    lane = lax.broadcasted_iota(jnp.int32, head.shape, 1)
    masked = jnp.concatenate(
        [jnp.where(lane < m, head, jnp.zeros_like(head)) for m in narrow], axis=0)
    if slim:
        stacked = transposed_dot(left, masked)
        parts = [stacked[:, k * count:(k + 1) * count] for k in range(len(narrow))]
    else:
        stacked = transposed_dot(masked, right)
        parts = [stacked[k * count:(k + 1) * count] for k in range(len(narrow))]
    yield from parts
    lower, running = narrow[-1], parts[-1]
    for upper in uppers[len(narrow):]:
        running = running + transposed_dot(
            rows_of(v_refs, lower, upper), rows_of(w_refs, lower, upper))
        yield running
        lower = upper


def subtile(lead, v_refs, w_refs, uppers, refs):
    power_ref, col_ref, line_ref = refs
    gains = [logit_gain * m ** -0.5 * LOG2E for m in uppers]
    count, across = power_ref.shape[1:]

    @pl.when(lead)
    def _():
        lane = lax.broadcasted_iota(jnp.int32, (count, LANES), 1)
        both = jnp.where(lane < STATS, 0.0, 1.0)
        for k, s in enumerate(subtile_scores(v_refs, w_refs, uppers)):
            logits = s * gains[k]
            peak = jnp.max(logits, axis=1, keepdims=True)
            power = jnp.exp2(logits - peak)
            power_ref[k] = power
            both = jnp.where(lane == k, peak, both)
            both = jnp.where(lane == STATS + k, jnp.sum(power, axis=1, keepdims=True), both)
        col_ref[...] = both
        line_ref[:, :count] = both.T[:2 * STATS]

    @pl.when(jnp.logical_not(lead))
    def _():
        line_ref[:STATS, :] = jnp.zeros((STATS, line_ref.shape[1]), jnp.float32)
        line_ref[STATS:, :] = jnp.ones((STATS, line_ref.shape[1]), jnp.float32)
        for k, s in enumerate(subtile_scores(v_refs, w_refs, uppers)):
            logits = s * gains[k]
            peak = jnp.max(logits, axis=0, keepdims=True)
            power = jnp.exp2(logits - peak)
            power_ref[k] = power
            line_ref[k:k + 1, :across] = peak
            line_ref[STATS + k:STATS + k + 1, :across] = jnp.sum(power, axis=0, keepdims=True)


def log_sum(pairs):
    top = functools.reduce(jnp.maximum, [peak for peak, _ in pairs])
    mass = functools.reduce(
        lambda a, b: a + b, [mass * jnp.exp2(peak - top) for peak, mass in pairs])
    return top + jnp.log(mass) * LOG2E


def tile_kernel(span, counts, uppers, own_rows, finish, *refs):
    groups = len(counts)
    shapes = subtiles(groups)
    tiles = [shapes[i] for i in span]
    r0, r1, c0, c1 = extent(tiles)
    me_ref, partner_ref = refs[:2]
    at = 2 + sum(counts[r0:r1])
    v_refs, w_refs = refs[2:at], refs[at:at + sum(counts[c0:c1])]
    at += sum(counts[c0:c1])
    earlier = refs[at:at + finish]
    outs = refs[at + finish:]
    lead = (me_ref[0] & 1) == 0
    for i, (t0, t1, u0, u1) in enumerate(tiles):
        subtile(
            lead, v_refs[sum(counts[r0:t0]):sum(counts[r0:t1])],
            w_refs[sum(counts[c0:u0]):sum(counts[c0:u1])], uppers, outs[3 * i:3 * i + 3])
    if not finish:
        outs[-1][...] = partner_ref[...]
        return
    stats_ref = outs[-1]
    every = [*earlier, *outs[2:3 * len(tiles):3]]
    segments = segments_of(groups)
    chip_rows = 2 * own_rows

    def merge(axis):
        for s0, s1 in segments:
            pairs = []
            for shape, line in zip(shapes, every):
                low, high = shape[axis:axis + 2]
                if low <= s0 and s1 <= high:
                    at = slice((s0 - low) * chip_rows, (s1 - low) * chip_rows)
                    pairs.append((line[:STATS, at], line[STATS:, at]))
            stats_ref[:, s0 * chip_rows:s1 * chip_rows] = log_sum(pairs)

    pl.when(lead)(lambda: merge(0))
    pl.when(jnp.logical_not(lead))(lambda: merge(2))

    count = len(uppers)
    stats_ref[count:count + 1, :chip_rows] = partner_ref[...]


def segments_of(groups):
    low, middle = groups // 2, groups // 2 + groups // 4
    return [(0, low), (low, middle), (middle, groups)]


def subtiles(groups):
    (_, low), (_, middle), _ = segments_of(groups)
    return [(0, low, 0, low), (low, middle, 0, low), (0, middle, low, middle),
            (middle, groups, 0, middle), (0, groups, middle, groups)]


def extent(tiles):
    first, second, third, fourth = zip(*tiles)
    return min(first), max(second), min(third), max(fourth)


def band_setup(groups, uppers, own_rows, masks, me_ref, stat_refs):
    count = len(uppers)
    total = stat_refs[0].shape[1]
    chip_rows = total // groups
    me = me_ref[0]
    lead = (me & 1) == 0
    own, first, second, swapped = [ref[...] for ref in stat_refs]
    values = [own, jnp.where(lead, first, swapped), second, jnp.where(lead, swapped, first)]
    parts, partners = [], []
    for j, value in enumerate(values):
        parts.append(jnp.concatenate(
            [value[:, (i ^ j) * chip_rows:((i ^ j) + 1) * chip_rows] for i in range(groups)], axis=1))
        partners.append(value[count:count + 1, :chip_rows])
    peak = functools.reduce(jnp.maximum, parts)
    mass = functools.reduce(lambda a, b: a + b, [jnp.exp2(part - peak) for part in parts])
    partner_row = jnp.concatenate(partners, axis=1)
    sub = lax.broadcasted_iota(jnp.int32, (STATS, total), 0)
    totals = peak + jnp.log(mass) * LOG2E
    for k in range(count):
        totals = jnp.where(sub == k, totals - math.log2(logit_gain * uppers[k] ** -0.5), totals)
    packed = jnp.concatenate(
        [totals[:count], partner_row, jnp.zeros((LANES - count - 1, total), jnp.float32)], axis=0)
    cols = packed.T
    id_row = jnp.where(
        lead, document_ids((1, total), 1, me | 1, own_rows, masks), partner_row)
    id_col = jnp.where(
        lead, cols[:, count:count + 1],
        document_ids((total, 1), 0, me | 1, own_rows, masks))
    return lead, totals, cols, id_row, id_col


def weights_of(segment, groups, setup, power_refs, col_refs, row_refs):
    lead, totals, cols, _, _ = setup
    chip_rows = totals.shape[1] // groups
    s0, s1 = segment
    strip = []
    for (r0, r1, c0, c1), power, col_peak, line in zip(
            subtiles(groups), power_refs, col_refs, row_refs):
        if r0 <= s0 and s1 <= r1:
            inner = slice((s0 - r0) * chip_rows, (s1 - r0) * chip_rows)
            outer = slice(s0 * chip_rows, s1 * chip_rows)
            across = slice(c0 * chip_rows, c1 * chip_rows)
            strip.append((
                c0, power, inner,
                jnp.where(lead, jnp.exp2(col_peak[inner, :] - cols[outer]), 1.0),
                jnp.where(lead, 1.0, jnp.exp2(line[:STATS, :(c1 - c0) * chip_rows] - totals[:, across]))))
    strip.sort(key=lambda item: item[0])
    return lambda k: jnp.concatenate([
        power[k, inner] * col_gain[:, k:k + 1] * row_gain[k:k + 1, :]
        for _, power, inner, col_gain, row_gain in strip], axis=1)


def last_band_kernel(groups, uppers, own_rows, masks, *refs):
    tiles = len(subtiles(groups))
    setup = band_setup(groups, uppers, own_rows, masks, refs[0], refs[1:1 + groups])
    at = 1 + groups
    power_refs, col_refs, row_refs = [refs[at + i * tiles:at + (i + 1) * tiles] for i in range(3)]
    segment = segments_of(groups)[-1]
    farthest = segment[1] - segment[0]
    w_refs, out_refs, after_ref = refs[at + 3 * tiles:-farthest - 1], refs[-farthest - 1:-1], refs[-1]
    _, totals, _, id_row, id_col = setup
    chip_rows = totals.shape[1] // groups
    k = len(uppers) - 1
    rows = slice(segment[0] * chip_rows, segment[1] * chip_rows)
    weight = weights_of(segment, groups, setup, power_refs, col_refs, row_refs)(k)
    weight = weight - jnp.where(id_col[rows] == id_row, logit_gain * uppers[k] ** -0.5, 0.0)
    after_ref[...] = weight
    product = jnp.dot(
        weight.astype(jnp.bfloat16), rows_of(w_refs, uppers[k - 1], uppers[k]),
        preferred_element_type=jnp.float32)
    store(out_refs, product, 0, 0, uppers[k] - uppers[k - 1], chip_rows)


def bands_kernel(groups, uppers, own_rows, masks, *refs):
    tiles = len(subtiles(groups))
    setup = band_setup(groups, uppers, own_rows, masks, refs[0], refs[1:1 + groups])
    at = 1 + groups
    power_refs, col_refs, row_refs = [refs[at + i * tiles:at + (i + 1) * tiles] for i in range(3)]
    segments = segments_of(groups)
    outs = groups + segments[-1][0]
    before_ref = refs[-outs - 1]
    w_refs, others, widest = refs[at + 3 * tiles:-outs - 1], refs[-outs:-outs + groups], refs[-outs + groups:]
    _, totals, _, id_row, id_col = setup
    chip_rows = totals.shape[1] // groups
    scales = [logit_gain * m ** -0.5 for m in uppers]
    last = len(uppers) - 1
    narrow = [k for k in range(last, -1, -1) if uppers[k] <= LANES]
    for block in (segments[1:], segments[:1]):
        first = block[0][0] * chip_rows
        rows = slice(first, block[-1][1] * chip_rows)
        height = rows.stop - first
        hit = id_col[rows] == id_row
        weights = [
            weights_of(segment, groups, setup, power_refs, col_refs, row_refs) for segment in block]
        tall = (block[0][1] - block[0][0]) * chip_rows
        running = weights[0](last) - jnp.where(hit[:tall], scales[last], 0.0)
        lower, upper = uppers[last - 1], uppers[last]
        product = jnp.dot(
            running.astype(jnp.bfloat16), rows_of(w_refs, lower, upper),
            preferred_element_type=jnp.float32)
        store(widest, product, first, 0, upper - lower, chip_rows)
        if len(block) > 1:
            running = jnp.concatenate([running, before_ref[...]], axis=0)
        stack = []
        for k in range(last - 1, -1, -1):
            weight = jnp.concatenate([part(k) for part in weights], axis=0)
            running = running + (weight - jnp.where(hit, scales[k], 0.0))
            band = running.astype(jnp.bfloat16)
            if k in narrow:
                stack.append(band)
                continue
            lower, upper = uppers[k - 1], uppers[k]
            product = jnp.dot(
                band, rows_of(w_refs, lower, upper), preferred_element_type=jnp.float32)
            store(others, product, first, lower, upper, chip_rows)
        product = jnp.dot(
            jnp.concatenate(stack, axis=0), rows_of(w_refs, 0, LANES),
            preferred_element_type=jnp.float32)
        lane = lax.broadcasted_iota(jnp.int32, (height, LANES), 1)
        chosen = product[:height]
        for i in range(1, len(stack)):
            chosen = jnp.where(
                lane < uppers[narrow[i]], product[i * height:(i + 1) * height], chosen)
        store(others, chosen, first, 0, LANES, chip_rows)


def store(out_refs, value, first_row, lower, upper, chip_rows):
    for at in range(0, value.shape[0], chip_rows):
        ref = out_refs[(first_row + at) // chip_rows]
        ref[:, lower:upper] = value[at:at + chip_rows].astype(ref.dtype)


def on_device(queries, documents, partner):
    own_rows, feature_dim = queries.shape
    uppers = width_list(feature_dim)
    dp_size, rep_size = lax.axis_size("dp"), lax.axis_size("rep")
    devices = dp_size * rep_size
    bits = devices.bit_length() - 1
    assert rep_size == 2 and devices == 1 << bits and bits % 2 == 1
    stages = (bits - 1) // 2
    groups = 1 << stages
    pieces = 2 * groups
    query_masks = [1 << (2 * s + 1) for s in range(stages)]
    document_masks = [1 << (2 * s + 2) for s in range(stages)]
    total = pieces * own_rows
    chip_rows = 2 * own_rows

    role = lax.axis_index("rep")
    me = (lax.axis_index("dp") * rep_size + role).astype(jnp.int32).reshape(1)
    lead = role == 0

    def exchange(x, masks_of):
        return lax.ppermute(x, AXES, [(i, i ^ masks_of(i)) for i in range(devices)])

    def swap(x):
        return exchange(x, lambda i: 1)

    def along(x, stage):
        return exchange(x, lambda i: document_masks[stage] if i & 1 else query_masks[stage])

    mine = jnp.where(lead, queries, documents)
    other = jnp.where(lead, documents, queries)
    got = swap(other)
    small = groups == 4 and WIDTHS * total * total * 4 <= 16 << 20
    cut = own_rows // 2 if small and own_rows % 32 == 0 else own_rows
    v = {0: [mine, got]}
    w = {0: [swap(mine), other]}
    for stage in reversed(range(stages)):
        for j in sorted(v):
            parts = v[j]
            if cut < own_rows and j == 0 and stage:
                parts = [mine, got[:cut], got[cut:]]
            v[j | 1 << stage] = [
                along(part, stage) for part in parts]
    for j in range(1, groups):
        w[j] = [swap(part) for part in v[j]]
    counts = [len(v[j]) for j in range(groups)]
    v_list = [part for j in range(groups) for part in v[j]]
    w_list = [part for j in range(groups) for part in w[j]]

    own_partner = partner.astype(jnp.float32).reshape(1, own_rows)
    far_partner = swap(own_partner)
    chip_partner = jnp.where(
        lead,
        jnp.concatenate([own_partner, far_partner], axis=1),
        jnp.concatenate([far_partner, own_partner], axis=1))

    vmem = pl.BlockSpec(memory_space=pltpu.VMEM)
    smem = pl.BlockSpec(memory_space=pltpu.SMEM)

    def query_mask(j):
        return sum(mask for s, mask in enumerate(query_masks) if j >> s & 1)

    def gathered(stats):
        return [stats] + [exchange(stats, lambda i: query_mask(j)) for j in range(1, groups)]

    shape = lambda *dims: jax.ShapeDtypeStruct(dims, jnp.float32)

    def gradient_shapes(columns):
        return [
            jax.ShapeDtypeStruct((chip_rows, columns), jnp.bfloat16 if j & 1 else jnp.float32)
            for j in range(groups)]

    if not small:
        limit = 60 << 20
        stats = pl.pallas_call(
            functools.partial(stats_kernel, pieces, uppers),
            out_shape=shape(STATS, total),
            in_specs=[smem] + [vmem] * (1 + 2 * pieces),
            out_specs=vmem,
            scratch_shapes=[
                pltpu.VMEM((total, feature_dim), jnp.bfloat16),
                pltpu.VMEM((total, feature_dim), jnp.bfloat16),
                pltpu.VMEM((total, LANES), jnp.float32),
            ],
            compiler_params=pltpu.CompilerParams(vmem_limit_bytes=limit),
            name="tile_stats",
        )(me, chip_partner, *v_list, *w_list)
        whole = pl.pallas_call(
            functools.partial(grads_kernel, pieces, uppers, own_rows, document_masks),
            out_shape=gradient_shapes(feature_dim),
            in_specs=[smem] + [vmem] * (groups + 2 * pieces),
            out_specs=[vmem] * groups,
            scratch_shapes=[
                pltpu.VMEM((total, feature_dim), jnp.bfloat16),
                pltpu.VMEM((total, feature_dim), jnp.bfloat16),
                pltpu.VMEM((WIDTHS, block_of(total), total), jnp.float32),
                pltpu.VMEM((total, LANES), jnp.float32),
            ],
            compiler_params=pltpu.CompilerParams(vmem_limit_bytes=limit),
            name="tile_grads",
        )(me, *gathered(stats), *v_list, *w_list)
        chunks = [whole]
    else:
        shapes = subtiles(groups)
        limit = 20 << 20
        params = pltpu.CompilerParams(vmem_limit_bytes=limit)

        def tile(span, partner_row, earlier=()):
            first, end, left, right = extent([shapes[i] for i in span])
            operands = v_list[sum(counts[:first]):sum(counts[:end])]
            operands += w_list[sum(counts[:left]):sum(counts[:right])]
            stat_shapes = [shape(STATS, total)] if earlier else [shape(1, chip_rows)]
            result, area = [], 0
            for i in span:
                r0, r1, c0, c1 = shapes[i]
                tall, wide = (r1 - r0) * chip_rows, (c1 - c0) * chip_rows
                area += tall * wide
                result += [shape(WIDTHS, tall, wide), shape(tall, LANES),
                           shape(2 * STATS, max(tall, wide))]
            *arrays, last_array = pl.pallas_call(
                functools.partial(
                    tile_kernel, span, counts, uppers, own_rows, len(earlier)),
                out_shape=result + stat_shapes,
                in_specs=[smem] + [vmem] * (1 + len(operands) + len(earlier)),
                out_specs=[vmem] * (len(result) + 1),
                compiler_params=params,
                cost_estimate=pl.CostEstimate(
                    flops=6 * area * feature_dim, transcendentals=0,
                    bytes_accessed=2 * total * feature_dim),
            )(me, partner_row, *operands, *[one[2] for one in earlier])
            return [arrays[3 * i:3 * i + 3] for i in range(len(span))], last_array

        done, chip_partner = tile([0], chip_partner)
        for at in (1, 2, 3):
            more, chip_partner = tile([at], chip_partner)
            done += more
        more, stats = tile([4], chip_partner, done)
        done += more
        first = exchange(
            stats, lambda i: query_mask(3) if i & 1 else query_mask(1))
        second = exchange(stats, lambda i: query_mask(2))
        swapped = swap(first)
        common = [me, stats, first, second, swapped, *[t[0] for t in done], *[t[1] for t in done],
                  *[t[2] for t in done], *w_list]
        near = segments_of(groups)[-1][0]
        widest = feature_dim - uppers[-2]

        def bands(kernel, more, outs):
            return pl.pallas_call(
                functools.partial(kernel, groups, uppers, own_rows, document_masks),
                out_shape=outs,
                in_specs=[smem] + [vmem] * (len(common) - 1 + len(more)),
                out_specs=[vmem] * len(outs),
                compiler_params=params,
                cost_estimate=pl.CostEstimate(
                    flops=2 * total * total * feature_dim, transcendentals=0,
                    bytes_accessed=4 * total * feature_dim),
            )(*common, *more)

        *far_ones, running = bands(
            last_band_kernel, [],
            gradient_shapes(widest)[near:] + [shape((groups - near) * chip_rows, total)])
        rest = bands(
            bands_kernel, [running], gradient_shapes(uppers[-2]) + gradient_shapes(widest)[:near])
        chunks = [[*rest[groups:], *far_ones], rest[:groups]]

    mine_parts, other_parts = [], []
    for c, chunk in enumerate(chunks):
        partial = dict(enumerate(chunk))
        for stage in range(stages - 1):
            step = 1 << stage
            for j in sorted([j for j in partial if j & step], reverse=True):
                arrived = along(partial.pop(j).astype(jnp.bfloat16), stage)
                partial[j ^ step] = partial[j ^ step] + arrived.astype(jnp.float32)
                if stage == stages - 2 and j ^ step:
                    partial[j ^ step] = partial[j ^ step].astype(jnp.bfloat16)
        stage = stages - 1
        outgoing = partial[1 << stage]
        kept = partial[0]
        if c < len(chunks) - 1:
            arrived = along(outgoing, stage)
            kept = kept + arrived.astype(jnp.float32)
            mine_parts.append(kept[:own_rows])
            other_parts.append(swap(kept[own_rows:]))
        else:
            far = lambda i: document_masks[stage] ^ 1 if i & 1 else query_masks[stage] ^ 1
            near_arrived = along(outgoing[:own_rows], stage)
            far_arrived = exchange(outgoing[own_rows:], far)
            ours, theirs = lax.optimization_barrier((kept[:own_rows], kept[own_rows:]))
            mine_parts.append(ours + near_arrived.astype(jnp.float32))
            other_parts.append(swap(theirs) + far_arrived.astype(jnp.float32))
    mine_parts, other_parts = mine_parts[::-1], other_parts[::-1]
    ours = jnp.concatenate(mine_parts, axis=1)
    theirs = jnp.concatenate(other_parts, axis=1)
    return jnp.where(lead, ours, theirs), jnp.where(lead, theirs, ours)


def solution(mesh):
    return jax.shard_map(
        on_device,
        mesh=mesh,
        in_specs=(P(AXES, None), P(AXES, None), P(AXES)),
        out_specs=(P(AXES, None), P(AXES, None)),
        check_vma=False,
    )
```

```python
import functools
import math

import jax
import jax.numpy as jnp
from jax import lax
from jax.experimental import pallas as pl
from jax.experimental.pallas import tpu as pltpu
from jax.sharding import PartitionSpec as P


WIDTHS = 9
AXES = ("dp", "rep")
LOG2E = 1.4426950408889634
STATS = 16
LANES = 128


logit_gain = 3.0
QUERY_CORE = 1


def leads(device):
    return (device & 1) == QUERY_CORE


def other_core(device):
    return (device & -2) | (1 - QUERY_CORE)


def width_list(feature_dim):
    return [feature_dim >> WIDTHS - 1 - nested for nested in range(WIDTHS)]


def transposed_dot(a, b):
    return lax.dot_general(a, b, (((1,), (1,)), ((), ())), preferred_element_type=jnp.float32)


def prefix_scores(v_ref, w_ref, rows, uppers):
    narrow = [m for m in uppers if m <= LANES]
    count = rows.size
    head = v_ref[rows, :LANES]
    lane = lax.broadcasted_iota(jnp.int32, head.shape, 1)
    masked = [jnp.where(lane < m, head, jnp.zeros_like(head)) for m in narrow]
    stacked = transposed_dot(jnp.concatenate(masked, axis=0), w_ref[:, :LANES])
    result = [stacked[k * count:(k + 1) * count] for k in range(len(narrow))]
    lower = narrow[-1]
    for upper in uppers[len(narrow):]:
        part = transposed_dot(v_ref[rows, lower:upper], w_ref[:, lower:upper])
        result.append(result[-1] + part)
        lower = upper
    return result


def block_of(total):
    return min(total, 256)


def load_tile(refs, scratch):
    at = 0
    for ref in refs:
        scratch[at:at + ref.shape[0], :] = ref[...]
        at += ref.shape[0]


def stats_kernel(pieces, uppers, *refs):
    role_ref, partner_ref = refs[:2]
    v_refs, w_refs = refs[2:2 + pieces], refs[2 + pieces:2 + 2 * pieces]
    out_ref, v_ref, w_ref, col_ref = refs[2 + 2 * pieces:]
    load_tile(v_refs, v_ref)
    load_tile(w_refs, w_ref)
    total = v_ref.shape[0]
    block = block_of(total)
    steps = total // block
    gains = [logit_gain * m ** -0.5 * LOG2E for m in uppers]
    own = partner_ref.shape[1]
    out_ref[...] = jnp.zeros_like(out_ref)

    @pl.when(leads(role_ref[0]))
    def _():
        for step in range(steps):
            rows = pl.ds(step * block, block)
            col_ref[rows, :] = jnp.zeros((block, LANES), jnp.float32)
            for k, s in enumerate(prefix_scores(v_ref, w_ref, rows, uppers)):
                logits = s * gains[k]
                peak = jnp.max(logits, axis=1, keepdims=True)
                mass = jnp.sum(jnp.exp2(logits - peak), axis=1, keepdims=True)
                col_ref[rows, k:k + 1] = peak + jnp.log(mass) * LOG2E
        out_ref[...] = col_ref[...].T[:STATS]

    @pl.when(jnp.logical_not(leads(role_ref[0])))
    def _():
        peaks, masses = [None] * len(uppers), [None] * len(uppers)
        for step in range(steps):
            rows = pl.ds(step * block, block)
            for k, s in enumerate(prefix_scores(v_ref, w_ref, rows, uppers)):
                logits = s * gains[k]
                peak = jnp.max(logits, axis=0, keepdims=True)
                mass = jnp.sum(jnp.exp2(logits - peak), axis=0, keepdims=True)
                if step:
                    top = jnp.maximum(peak, peaks[k])
                    mass = mass * jnp.exp2(peak - top) + masses[k] * jnp.exp2(peaks[k] - top)
                    peak = top
                peaks[k], masses[k] = peak, mass
        for k in range(len(uppers)):
            out_ref[k:k + 1, :] = peaks[k] + jnp.log(masses[k]) * LOG2E

    out_ref[len(uppers):len(uppers) + 1, :own] = partner_ref[...]


def document_ids(shape, axis, first, own_rows, masks, start=0):
    at = lax.broadcasted_iota(jnp.int32, shape, axis) + start
    shift = own_rows.bit_length() - 1
    piece = at >> shift
    device = first ^ (piece & 1)
    for s, mask in enumerate(masks):
        device = device ^ (((piece >> (1 + s)) & 1) * mask)
    return (device * own_rows + (at & (own_rows - 1))).astype(jnp.float32)


def grads_kernel(pieces, uppers, own_rows, masks, *refs):
    me_ref = refs[0]
    groups = pieces // 2
    stat_refs = refs[1:1 + groups]
    v_refs = refs[1 + groups:1 + groups + pieces]
    w_refs = refs[1 + groups + pieces:1 + groups + 2 * pieces]
    out_refs = refs[1 + groups + 2 * pieces:1 + 2 * groups + 2 * pieces]
    v_ref, w_ref, score_ref, col_ref = refs[1 + 2 * groups + 2 * pieces:]
    load_tile(v_refs, v_ref)
    load_tile(w_refs, w_ref)
    total = v_ref.shape[0]
    block = block_of(total)
    chip_rows = total // groups
    count = len(uppers)
    scales = [logit_gain * m ** -0.5 for m in uppers]
    me = me_ref[0]
    lead = leads(me)

    parts = []
    partners = []
    for j, ref in enumerate(stat_refs):
        parts.append(jnp.concatenate(
            [ref[:, (i ^ j) * chip_rows:((i ^ j) + 1) * chip_rows] for i in range(groups)], axis=1))
        partners.append(ref[count:count + 1, :chip_rows])
    peak = functools.reduce(jnp.maximum, parts)
    mass = functools.reduce(lambda a, b: a + b, [jnp.exp2(part - peak) for part in parts])
    totals = peak + jnp.log(mass) * LOG2E
    partner_row = jnp.concatenate(partners, axis=1)
    packed = jnp.concatenate(
        [totals[:count], partner_row, jnp.zeros((LANES - count - 1, total), jnp.float32)], axis=0)
    col_ref[...] = packed.T
    zero_or = lambda keep, x: jnp.where(keep, x, jnp.zeros_like(x))
    document_row = document_ids((1, total), 1, other_core(me), own_rows, masks)
    id_row = jnp.where(lead, document_row, partner_row)
    shifts = [math.log2(s) for s in scales]
    total_rows = [zero_or(jnp.logical_not(lead), totals[k:k + 1]) - shifts[k] for k in range(count)]

    narrow = [m for m in uppers if m <= LANES]
    for step in range(total // block):
        rows = pl.ds(step * block, block)
        document_col = document_ids((block, 1), 0, other_core(me), own_rows, masks, step * block)
        id_col = jnp.where(lead, col_ref[rows, count:count + 1], document_col)
        hit = id_col == id_row
        for k, s in enumerate(prefix_scores(v_ref, w_ref, rows, uppers)):
            score_ref[k] = s
        running = None
        stack = []
        for k in reversed(range(count)):
            gain = scales[k] * LOG2E
            total_col = zero_or(lead, col_ref[rows, k:k + 1])
            weight = jnp.exp2(score_ref[k] * gain - total_col - total_rows[k])
            weight = weight - jnp.where(hit, scales[k], 0.0)
            running = weight if running is None else running + weight
            band = running.astype(jnp.bfloat16)
            if k >= len(narrow):
                lower, upper = uppers[k - 1], uppers[k]
                product = jnp.dot(band, w_ref[:, lower:upper], preferred_element_type=jnp.float32)
                store(out_refs, product, step * block, lower, upper, chip_rows)
            else:
                stack.append(band)
        product = jnp.dot(
            jnp.concatenate(stack, axis=0), w_ref[:, :LANES], preferred_element_type=jnp.float32)
        lane = lax.broadcasted_iota(jnp.int32, (block, LANES), 1)
        chosen = product[:block]
        for at_stack in range(1, len(stack)):
            k = len(narrow) - 1 - at_stack
            chosen = jnp.where(
                lane < uppers[k], product[at_stack * block:(at_stack + 1) * block], chosen)
        store(out_refs, chosen, step * block, 0, LANES, chip_rows)


def rows_of(refs, lower, upper):
    return jnp.concatenate([ref[:, lower:upper] for ref in refs], axis=0)


def subtile_scores(v_refs, w_refs, uppers):
    narrow = [m for m in uppers if m <= LANES]
    left, right = rows_of(v_refs, 0, LANES), rows_of(w_refs, 0, LANES)
    slim = right.shape[0] < 2 * LANES
    head = right if slim else left
    count = head.shape[0]
    lane = lax.broadcasted_iota(jnp.int32, head.shape, 1)
    masked = jnp.concatenate(
        [jnp.where(lane < m, head, jnp.zeros_like(head)) for m in narrow], axis=0)
    if slim:
        stacked = transposed_dot(left, masked)
        parts = [stacked[:, k * count:(k + 1) * count] for k in range(len(narrow))]
    else:
        stacked = transposed_dot(masked, right)
        parts = [stacked[k * count:(k + 1) * count] for k in range(len(narrow))]
    yield from parts
    lower, running = narrow[-1], parts[-1]
    for upper in uppers[len(narrow):]:
        running = running + transposed_dot(
            rows_of(v_refs, lower, upper), rows_of(w_refs, lower, upper))
        yield running
        lower = upper


def subtile(lead, v_refs, w_refs, uppers, refs):
    power_ref, col_ref, line_ref = refs
    gains = [logit_gain * m ** -0.5 * LOG2E for m in uppers]
    count, across = power_ref.shape[1:]

    @pl.when(lead)
    def _():
        lane = lax.broadcasted_iota(jnp.int32, (count, LANES), 1)
        both = jnp.where(lane < STATS, 0.0, 1.0)
        for k, s in enumerate(subtile_scores(v_refs, w_refs, uppers)):
            logits = s * gains[k]
            peak = jnp.max(logits, axis=1, keepdims=True)
            power = jnp.exp2(logits - peak)
            power_ref[k] = power
            both = jnp.where(lane == k, peak, both)
            both = jnp.where(lane == STATS + k, jnp.sum(power, axis=1, keepdims=True), both)
        col_ref[...] = both
        line_ref[:, :count] = both.T[:2 * STATS]

    @pl.when(jnp.logical_not(lead))
    def _():
        line_ref[:STATS, :] = jnp.zeros((STATS, line_ref.shape[1]), jnp.float32)
        line_ref[STATS:, :] = jnp.ones((STATS, line_ref.shape[1]), jnp.float32)
        for k, s in enumerate(subtile_scores(v_refs, w_refs, uppers)):
            logits = s * gains[k]
            peak = jnp.max(logits, axis=0, keepdims=True)
            power = jnp.exp2(logits - peak)
            power_ref[k] = power
            line_ref[k:k + 1, :across] = peak
            line_ref[STATS + k:STATS + k + 1, :across] = jnp.sum(power, axis=0, keepdims=True)


def log_sum(pairs):
    top = functools.reduce(jnp.maximum, [peak for peak, _ in pairs])
    mass = functools.reduce(
        lambda a, b: a + b, [mass * jnp.exp2(peak - top) for peak, mass in pairs])
    return top + jnp.log(mass) * LOG2E


def tile_kernel(span, counts, uppers, own_rows, finish, *refs):
    groups = len(counts)
    shapes = subtiles(groups)
    tiles = [shapes[i] for i in span]
    r0, r1, c0, c1 = extent(tiles)
    me_ref, partner_ref = refs[:2]
    at = 2 + sum(counts[r0:r1])
    v_refs, w_refs = refs[2:at], refs[at:at + sum(counts[c0:c1])]
    at += sum(counts[c0:c1])
    earlier = refs[at:at + finish]
    outs = refs[at + finish:]
    lead = leads(me_ref[0])
    for i, (t0, t1, u0, u1) in enumerate(tiles):
        subtile(
            lead, v_refs[sum(counts[r0:t0]):sum(counts[r0:t1])],
            w_refs[sum(counts[c0:u0]):sum(counts[c0:u1])], uppers, outs[3 * i:3 * i + 3])
    if not finish:
        outs[-1][...] = partner_ref[...]
        return
    stats_ref = outs[-1]
    every = [*earlier, *outs[2:3 * len(tiles):3]]
    segments = segments_of(groups)
    chip_rows = 2 * own_rows

    def merge(axis):
        for s0, s1 in segments:
            pairs = []
            for shape, line in zip(shapes, every):
                low, high = shape[axis:axis + 2]
                if low <= s0 and s1 <= high:
                    at = slice((s0 - low) * chip_rows, (s1 - low) * chip_rows)
                    pairs.append((line[:STATS, at], line[STATS:, at]))
            stats_ref[:, s0 * chip_rows:s1 * chip_rows] = log_sum(pairs)

    pl.when(lead)(lambda: merge(0))
    pl.when(jnp.logical_not(lead))(lambda: merge(2))

    count = len(uppers)
    stats_ref[count:count + 1, :chip_rows] = partner_ref[...]


def segments_of(groups):
    low, middle = groups // 2, groups // 2 + groups // 4
    return [(0, low), (low, middle), (middle, groups)]


def subtiles(groups):
    (_, low), (_, middle), _ = segments_of(groups)
    return [(0, low, 0, low), (low, middle, 0, low), (0, middle, low, middle),
            (middle, groups, 0, middle), (0, groups, middle, groups)]


def extent(tiles):
    first, second, third, fourth = zip(*tiles)
    return min(first), max(second), min(third), max(fourth)


def band_setup(groups, uppers, own_rows, masks, me_ref, stat_refs):
    count = len(uppers)
    total = stat_refs[0].shape[1]
    chip_rows = total // groups
    me = me_ref[0]
    lead = leads(me)
    own, first, second, swapped = [ref[...] for ref in stat_refs]
    odd = (me & 1) == 1
    values = [own, jnp.where(odd, swapped, first), second, jnp.where(odd, first, swapped)]
    parts, partners = [], []
    for j, value in enumerate(values):
        parts.append(jnp.concatenate(
            [value[:, (i ^ j) * chip_rows:((i ^ j) + 1) * chip_rows] for i in range(groups)], axis=1))
        partners.append(value[count:count + 1, :chip_rows])
    peak = functools.reduce(jnp.maximum, parts)
    mass = functools.reduce(lambda a, b: a + b, [jnp.exp2(part - peak) for part in parts])
    partner_row = jnp.concatenate(partners, axis=1)
    sub = lax.broadcasted_iota(jnp.int32, (STATS, total), 0)
    totals = peak + jnp.log(mass) * LOG2E
    for k in range(count):
        totals = jnp.where(sub == k, totals - math.log2(logit_gain * uppers[k] ** -0.5), totals)
    packed = jnp.concatenate(
        [totals[:count], partner_row, jnp.zeros((LANES - count - 1, total), jnp.float32)], axis=0)
    cols = packed.T
    id_row = jnp.where(
        lead, document_ids((1, total), 1, other_core(me), own_rows, masks), partner_row)
    id_col = jnp.where(
        lead, cols[:, count:count + 1],
        document_ids((total, 1), 0, other_core(me), own_rows, masks))
    return lead, totals, cols, id_row, id_col


def weights_of(segment, groups, setup, power_refs, col_refs, row_refs):
    lead, totals, cols, _, _ = setup
    chip_rows = totals.shape[1] // groups
    s0, s1 = segment
    strip = []
    for (r0, r1, c0, c1), power, col_peak, line in zip(
            subtiles(groups), power_refs, col_refs, row_refs):
        if r0 <= s0 and s1 <= r1:
            inner = slice((s0 - r0) * chip_rows, (s1 - r0) * chip_rows)
            outer = slice(s0 * chip_rows, s1 * chip_rows)
            across = slice(c0 * chip_rows, c1 * chip_rows)
            strip.append((
                c0, power, inner,
                jnp.where(lead, jnp.exp2(col_peak[inner, :] - cols[outer]), 1.0),
                jnp.where(lead, 1.0, jnp.exp2(line[:STATS, :(c1 - c0) * chip_rows] - totals[:, across]))))
    strip.sort(key=lambda item: item[0])
    return lambda k: jnp.concatenate([
        power[k, inner] * col_gain[:, k:k + 1] * row_gain[k:k + 1, :]
        for _, power, inner, col_gain, row_gain in strip], axis=1)


def last_band_kernel(groups, uppers, own_rows, masks, *refs):
    tiles = len(subtiles(groups))
    setup = band_setup(groups, uppers, own_rows, masks, refs[0], refs[1:1 + groups])
    at = 1 + groups
    power_refs, col_refs, row_refs = [refs[at + i * tiles:at + (i + 1) * tiles] for i in range(3)]
    segment = segments_of(groups)[-1]
    farthest = segment[1] - segment[0]
    w_refs, out_refs, after_ref = refs[at + 3 * tiles:-farthest - 1], refs[-farthest - 1:-1], refs[-1]
    _, totals, _, id_row, id_col = setup
    chip_rows = totals.shape[1] // groups
    k = len(uppers) - 1
    rows = slice(segment[0] * chip_rows, segment[1] * chip_rows)
    weight = weights_of(segment, groups, setup, power_refs, col_refs, row_refs)(k)
    weight = weight - jnp.where(id_col[rows] == id_row, logit_gain * uppers[k] ** -0.5, 0.0)
    after_ref[...] = weight
    product = jnp.dot(
        weight.astype(jnp.bfloat16), rows_of(w_refs, uppers[k - 1], uppers[k]),
        preferred_element_type=jnp.float32)
    store(out_refs, product, 0, 0, uppers[k] - uppers[k - 1], chip_rows)


def bands_kernel(groups, uppers, own_rows, masks, *refs):
    tiles = len(subtiles(groups))
    setup = band_setup(groups, uppers, own_rows, masks, refs[0], refs[1:1 + groups])
    at = 1 + groups
    power_refs, col_refs, row_refs = [refs[at + i * tiles:at + (i + 1) * tiles] for i in range(3)]
    segments = segments_of(groups)
    outs = groups + segments[-1][0]
    before_ref = refs[-outs - 1]
    w_refs, others, widest = refs[at + 3 * tiles:-outs - 1], refs[-outs:-outs + groups], refs[-outs + groups:]
    _, totals, _, id_row, id_col = setup
    chip_rows = totals.shape[1] // groups
    scales = [logit_gain * m ** -0.5 for m in uppers]
    last = len(uppers) - 1
    narrow = [k for k in range(last, -1, -1) if uppers[k] <= LANES]
    for block in (segments[1:], segments[:1]):
        first = block[0][0] * chip_rows
        rows = slice(first, block[-1][1] * chip_rows)
        height = rows.stop - first
        hit = id_col[rows] == id_row
        weights = [
            weights_of(segment, groups, setup, power_refs, col_refs, row_refs) for segment in block]
        tall = (block[0][1] - block[0][0]) * chip_rows
        running = weights[0](last) - jnp.where(hit[:tall], scales[last], 0.0)
        lower, upper = uppers[last - 1], uppers[last]
        product = jnp.dot(
            running.astype(jnp.bfloat16), rows_of(w_refs, lower, upper),
            preferred_element_type=jnp.float32)
        store(widest, product, first, 0, upper - lower, chip_rows)
        if len(block) > 1:
            running = jnp.concatenate([running, before_ref[...]], axis=0)
        stack = []
        for k in range(last - 1, -1, -1):
            weight = jnp.concatenate([part(k) for part in weights], axis=0)
            running = running + (weight - jnp.where(hit, scales[k], 0.0))
            band = running.astype(jnp.bfloat16)
            if k in narrow:
                stack.append(band)
                continue
            lower, upper = uppers[k - 1], uppers[k]
            product = jnp.dot(
                band, rows_of(w_refs, lower, upper), preferred_element_type=jnp.float32)
            store(others, product, first, lower, upper, chip_rows)
        product = jnp.dot(
            jnp.concatenate(stack, axis=0), rows_of(w_refs, 0, LANES),
            preferred_element_type=jnp.float32)
        lane = lax.broadcasted_iota(jnp.int32, (height, LANES), 1)
        chosen = product[:height]
        for i in range(1, len(stack)):
            chosen = jnp.where(
                lane < uppers[narrow[i]], product[i * height:(i + 1) * height], chosen)
        store(others, chosen, first, 0, LANES, chip_rows)


def store(out_refs, value, first_row, lower, upper, chip_rows):
    for at in range(0, value.shape[0], chip_rows):
        ref = out_refs[(first_row + at) // chip_rows]
        ref[:, lower:upper] = value[at:at + chip_rows].astype(ref.dtype)


def put_kernel(columns, me_ref, *refs):
    kept_ref, near_ref, given_ref, far_ref = refs[:4]
    queries_ref, documents_ref, ours_ref, theirs_ref, sems = refs[-5:]
    ours_ref[...] = kept_ref[...] + near_ref[...].astype(jnp.float32)
    theirs_ref[...] = given_ref[...] + far_ref[...].astype(jnp.float32)

    def write(first, second):
        copies = [pltpu.make_async_copy(ours_ref, first.at[:, columns], sems.at[0]),
                  pltpu.make_async_copy(theirs_ref, second.at[:, columns], sems.at[1])]
        for copy in copies:
            copy.start()
        for copy in copies:
            copy.wait()

    lead = leads(me_ref[0])
    pl.when(lead)(lambda: write(queries_ref, documents_ref))
    pl.when(jnp.logical_not(lead))(lambda: write(documents_ref, queries_ref))


def on_device(queries, documents, partner):
    own_rows, feature_dim = queries.shape
    uppers = width_list(feature_dim)
    dp_size, rep_size = lax.axis_size("dp"), lax.axis_size("rep")
    devices = dp_size * rep_size
    bits = devices.bit_length() - 1
    assert rep_size == 2 and devices == 1 << bits and bits % 2 == 1
    stages = (bits - 1) // 2
    groups = 1 << stages
    pieces = 2 * groups
    query_masks = [1 << (2 * s + 1) for s in range(stages)]
    document_masks = [1 << (2 * s + 2) for s in range(stages)]
    total = pieces * own_rows
    chip_rows = 2 * own_rows

    role = lax.axis_index("rep")
    me = (lax.axis_index("dp") * rep_size + role).astype(jnp.int32).reshape(1)
    lead = leads(role)

    def exchange(x, masks_of):
        return lax.ppermute(x, AXES, [(i, i ^ masks_of(i)) for i in range(devices)])

    def swap(x):
        return exchange(x, lambda i: 1)

    def along(x, stage):
        return exchange(x, lambda i: query_masks[stage] if leads(i) else document_masks[stage])

    vmem = pl.BlockSpec(memory_space=pltpu.VMEM)
    smem = pl.BlockSpec(memory_space=pltpu.SMEM)
    hbm = pl.BlockSpec(memory_space=pltpu.HBM)
    mine = jnp.where(lead, queries, documents)
    other = jnp.where(lead, documents, queries)
    got = swap(other)
    small = groups == 4 and WIDTHS * total * total * 4 <= 16 << 20
    cut = own_rows // 2 if small and own_rows % 32 == 0 else own_rows
    v = {0: [mine, got]}
    w = {0: [swap(mine), other]}
    for stage in reversed(range(stages)):
        for j in sorted(v):
            parts = v[j]
            if cut < own_rows and j == 0 and stage:
                parts = [mine, got[:cut], got[cut:]]
            v[j | 1 << stage] = [
                along(part, stage) for part in parts]
    for j in range(1, groups):
        w[j] = [swap(part) for part in v[j]]
    counts = [len(v[j]) for j in range(groups)]
    v_list = [part for j in range(groups) for part in v[j]]
    w_list = [part for j in range(groups) for part in w[j]]

    own_partner = partner.astype(jnp.float32).reshape(1, own_rows)
    far_partner = swap(own_partner)
    chip_partner = jnp.where(
        lead,
        jnp.concatenate([own_partner, far_partner], axis=1),
        jnp.concatenate([far_partner, own_partner], axis=1))

    def query_mask(j):
        return sum(mask for s, mask in enumerate(query_masks) if j >> s & 1)

    def gathered(stats):
        return [stats] + [exchange(stats, lambda i: query_mask(j)) for j in range(1, groups)]

    shape = lambda *dims: jax.ShapeDtypeStruct(dims, jnp.float32)

    def gradient_shapes(columns):
        return [
            jax.ShapeDtypeStruct((chip_rows, columns), jnp.bfloat16 if j & 1 else jnp.float32)
            for j in range(groups)]

    if not small:
        limit = 60 << 20
        stats = pl.pallas_call(
            functools.partial(stats_kernel, pieces, uppers),
            out_shape=shape(STATS, total),
            in_specs=[smem] + [vmem] * (1 + 2 * pieces),
            out_specs=vmem,
            scratch_shapes=[
                pltpu.VMEM((total, feature_dim), jnp.bfloat16),
                pltpu.VMEM((total, feature_dim), jnp.bfloat16),
                pltpu.VMEM((total, LANES), jnp.float32),
            ],
            compiler_params=pltpu.CompilerParams(vmem_limit_bytes=limit),
            name="tile_stats",
        )(me, chip_partner, *v_list, *w_list)
        whole = pl.pallas_call(
            functools.partial(grads_kernel, pieces, uppers, own_rows, document_masks),
            out_shape=gradient_shapes(feature_dim),
            in_specs=[smem] + [vmem] * (groups + 2 * pieces),
            out_specs=[vmem] * groups,
            scratch_shapes=[
                pltpu.VMEM((total, feature_dim), jnp.bfloat16),
                pltpu.VMEM((total, feature_dim), jnp.bfloat16),
                pltpu.VMEM((WIDTHS, block_of(total), total), jnp.float32),
                pltpu.VMEM((total, LANES), jnp.float32),
            ],
            compiler_params=pltpu.CompilerParams(vmem_limit_bytes=limit),
            name="tile_grads",
        )(me, *gathered(stats), *v_list, *w_list)
        chunks = [whole]
    else:
        shapes = subtiles(groups)
        limit = 20 << 20
        params = pltpu.CompilerParams(vmem_limit_bytes=limit)

        def tile(span, partner_row, earlier=()):
            first, end, left, right = extent([shapes[i] for i in span])
            operands = v_list[sum(counts[:first]):sum(counts[:end])]
            operands += w_list[sum(counts[:left]):sum(counts[:right])]
            stat_shapes = [shape(STATS, total)] if earlier else [shape(1, chip_rows)]
            result, area = [], 0
            for i in span:
                r0, r1, c0, c1 = shapes[i]
                tall, wide = (r1 - r0) * chip_rows, (c1 - c0) * chip_rows
                area += tall * wide
                result += [shape(WIDTHS, tall, wide), shape(tall, LANES),
                           shape(2 * STATS, max(tall, wide))]
            *arrays, last_array = pl.pallas_call(
                functools.partial(
                    tile_kernel, span, counts, uppers, own_rows, len(earlier)),
                out_shape=result + stat_shapes,
                in_specs=[smem] + [vmem] * (1 + len(operands) + len(earlier)),
                out_specs=[vmem] * (len(result) + 1),
                compiler_params=params,
                cost_estimate=pl.CostEstimate(
                    flops=6 * area * feature_dim, transcendentals=0,
                    bytes_accessed=2 * total * feature_dim),
            )(me, partner_row, *operands, *[one[2] for one in earlier])
            return [arrays[3 * i:3 * i + 3] for i in range(len(span))], last_array

        done, chip_partner = tile([0], chip_partner)
        for at in (1, 2, 3):
            more, chip_partner = tile([at], chip_partner)
            done += more
        more, stats = tile([4], chip_partner, done)
        done += more
        first = exchange(
            stats, lambda i: query_mask(3) if i & 1 else query_mask(1))
        second = exchange(stats, lambda i: query_mask(2))
        swapped = swap(first)
        common = [me, stats, first, second, swapped, *[t[0] for t in done], *[t[1] for t in done],
                  *[t[2] for t in done], *w_list]
        near = segments_of(groups)[-1][0]
        widest = feature_dim - uppers[-2]

        def bands(kernel, more, outs):
            return pl.pallas_call(
                functools.partial(kernel, groups, uppers, own_rows, document_masks),
                out_shape=outs,
                in_specs=[smem] + [vmem] * (len(common) - 1 + len(more)),
                out_specs=[vmem] * len(outs),
                compiler_params=params,
                cost_estimate=pl.CostEstimate(
                    flops=2 * total * total * feature_dim, transcendentals=0,
                    bytes_accessed=4 * total * feature_dim),
            )(*common, *more)

        *far_ones, running = bands(
            last_band_kernel, [],
            gradient_shapes(widest)[near:] + [shape((groups - near) * chip_rows, total)])
        rest = bands(
            bands_kernel, [running], gradient_shapes(uppers[-2]) + gradient_shapes(widest)[:near])
        chunks = [[*rest[groups:], *far_ones], rest[:groups]]

    def put(columns, parts, before):
        return pl.pallas_call(
            functools.partial(put_kernel, columns),
            out_shape=[jax.ShapeDtypeStruct(queries.shape, jnp.float32)] * 2,
            in_specs=[smem] + [vmem] * 4 + [hbm] * len(before),
            out_specs=[hbm, hbm],
            scratch_shapes=[pltpu.VMEM(parts[0].shape, jnp.float32)] * 2
            + [pltpu.SemaphoreType.DMA((2,))],
            input_output_aliases={5 + i: i for i in range(len(before))},
            compiler_params=pltpu.CompilerParams(vmem_limit_bytes=8 << 20),
            cost_estimate=pl.CostEstimate(flops=1000, transcendentals=0, bytes_accessed=1000),
        )(me, *parts, *before)

    gradients, end = [], feature_dim
    for c, chunk in enumerate(chunks):
        partial = dict(enumerate(chunk))
        for stage in range(stages - 1):
            step = 1 << stage
            for j in sorted([j for j in partial if j & step], reverse=True):
                arrived = along(partial.pop(j).astype(jnp.bfloat16), stage)
                partial[j ^ step] = partial[j ^ step] + arrived.astype(jnp.float32)
                if stage == stages - 2 and j ^ step:
                    partial[j ^ step] = partial[j ^ step].astype(jnp.bfloat16)
        stage = stages - 1
        outgoing = partial[1 << stage]
        kept = partial[0]
        start = end - kept.shape[1]
        if c < len(chunks) - 1:
            arrived = along(outgoing, stage)
            near = arrived[:own_rows]
            theirs = kept[own_rows:] + arrived[own_rows:].astype(jnp.float32)
            parts = [kept[:own_rows], near, swap(theirs), jnp.zeros_like(near)]
        else:
            far = lambda i: 1 ^ (query_masks[stage] if leads(i) else document_masks[stage])
            near_arrived = along(outgoing[:own_rows], stage)
            far_arrived = exchange(outgoing[own_rows:], far)
            ours, theirs = lax.optimization_barrier((kept[:own_rows], kept[own_rows:]))
            parts = [ours, near_arrived, swap(theirs), far_arrived]
        gradients = put(slice(start, end), parts, gradients)
        end = start
    return tuple(gradients)


def solution(mesh):
    return jax.shard_map(
        on_device,
        mesh=mesh,
        in_specs=(P(AXES, None), P(AXES, None), P(AXES)),
        out_specs=(P(AXES, None), P(AXES, None)),
        check_vma=False,
    )
```

```python
import functools
import math

import jax
import jax.numpy as jnp
from jax import lax
from jax.experimental import pallas as pl
from jax.experimental.pallas import tpu as pltpu
from jax.sharding import PartitionSpec as P


WIDTHS = 9
AXES = ("dp", "rep")
LOG2E = 1.4426950408889634
STATS = 16
LANES = 128


logit_gain = 3.0


def width_list(feature_dim):
    return [feature_dim >> WIDTHS - 1 - nested for nested in range(WIDTHS)]


def transposed_dot(a, b):
    return lax.dot_general(a, b, (((1,), (1,)), ((), ())), preferred_element_type=jnp.float32)


def prefix_scores(v_ref, w_ref, rows, uppers):
    narrow = [m for m in uppers if m <= LANES]
    count = rows.size
    head = v_ref[rows, :LANES]
    lane = lax.broadcasted_iota(jnp.int32, head.shape, 1)
    masked = [jnp.where(lane < m, head, jnp.zeros_like(head)) for m in narrow]
    stacked = transposed_dot(jnp.concatenate(masked, axis=0), w_ref[:, :LANES])
    result = [stacked[k * count:(k + 1) * count] for k in range(len(narrow))]
    lower = narrow[-1]
    for upper in uppers[len(narrow):]:
        part = transposed_dot(v_ref[rows, lower:upper], w_ref[:, lower:upper])
        result.append(result[-1] + part)
        lower = upper
    return result


def block_of(total):
    return min(total, 256)


def load_tile(refs, scratch):
    at = 0
    for ref in refs:
        scratch[at:at + ref.shape[0], :] = ref[...]
        at += ref.shape[0]


def stats_kernel(pieces, uppers, *refs):
    role_ref, partner_ref = refs[:2]
    v_refs, w_refs = refs[2:2 + pieces], refs[2 + pieces:2 + 2 * pieces]
    out_ref, v_ref, w_ref, col_ref = refs[2 + 2 * pieces:]
    load_tile(v_refs, v_ref)
    load_tile(w_refs, w_ref)
    total = v_ref.shape[0]
    block = block_of(total)
    steps = total // block
    gains = [logit_gain * m ** -0.5 * LOG2E for m in uppers]
    own = partner_ref.shape[1]
    out_ref[...] = jnp.zeros_like(out_ref)

    @pl.when((role_ref[0] & 1) == 0)
    def _():
        for step in range(steps):
            rows = pl.ds(step * block, block)
            col_ref[rows, :] = jnp.zeros((block, LANES), jnp.float32)
            for k, s in enumerate(prefix_scores(v_ref, w_ref, rows, uppers)):
                logits = s * gains[k]
                peak = jnp.max(logits, axis=1, keepdims=True)
                mass = jnp.sum(jnp.exp2(logits - peak), axis=1, keepdims=True)
                col_ref[rows, k:k + 1] = peak + jnp.log(mass) * LOG2E
        out_ref[...] = col_ref[...].T[:STATS]

    @pl.when((role_ref[0] & 1) != 0)
    def _():
        peaks, masses = [None] * len(uppers), [None] * len(uppers)
        for step in range(steps):
            rows = pl.ds(step * block, block)
            for k, s in enumerate(prefix_scores(v_ref, w_ref, rows, uppers)):
                logits = s * gains[k]
                peak = jnp.max(logits, axis=0, keepdims=True)
                mass = jnp.sum(jnp.exp2(logits - peak), axis=0, keepdims=True)
                if step:
                    top = jnp.maximum(peak, peaks[k])
                    mass = mass * jnp.exp2(peak - top) + masses[k] * jnp.exp2(peaks[k] - top)
                    peak = top
                peaks[k], masses[k] = peak, mass
        for k in range(len(uppers)):
            out_ref[k:k + 1, :] = peaks[k] + jnp.log(masses[k]) * LOG2E

    out_ref[len(uppers):len(uppers) + 1, :own] = partner_ref[...]


def document_ids(shape, axis, first, own_rows, masks, start=0):
    at = lax.broadcasted_iota(jnp.int32, shape, axis) + start
    shift = own_rows.bit_length() - 1
    piece = at >> shift
    device = first ^ (piece & 1)
    for s, mask in enumerate(masks):
        device = device ^ (((piece >> (1 + s)) & 1) * mask)
    return (device * own_rows + (at & (own_rows - 1))).astype(jnp.float32)


def grads_kernel(pieces, uppers, own_rows, masks, *refs):
    me_ref = refs[0]
    groups = pieces // 2
    stat_refs = refs[1:1 + groups]
    v_refs = refs[1 + groups:1 + groups + pieces]
    w_refs = refs[1 + groups + pieces:1 + groups + 2 * pieces]
    out_refs = refs[1 + groups + 2 * pieces:1 + 2 * groups + 2 * pieces]
    v_ref, w_ref, score_ref, col_ref = refs[1 + 2 * groups + 2 * pieces:]
    load_tile(v_refs, v_ref)
    load_tile(w_refs, w_ref)
    total = v_ref.shape[0]
    block = block_of(total)
    chip_rows = total // groups
    count = len(uppers)
    scales = [logit_gain * m ** -0.5 for m in uppers]
    me = me_ref[0]
    lead = (me & 1) == 0

    parts = []
    partners = []
    for j, ref in enumerate(stat_refs):
        parts.append(jnp.concatenate(
            [ref[:, (i ^ j) * chip_rows:((i ^ j) + 1) * chip_rows] for i in range(groups)], axis=1))
        partners.append(ref[count:count + 1, :chip_rows])
    peak = functools.reduce(jnp.maximum, parts)
    mass = functools.reduce(lambda a, b: a + b, [jnp.exp2(part - peak) for part in parts])
    totals = peak + jnp.log(mass) * LOG2E
    partner_row = jnp.concatenate(partners, axis=1)
    packed = jnp.concatenate(
        [totals[:count], partner_row, jnp.zeros((LANES - count - 1, total), jnp.float32)], axis=0)
    col_ref[...] = packed.T
    zero_or = lambda keep, x: jnp.where(keep, x, jnp.zeros_like(x))
    document_row = document_ids((1, total), 1, me | 1, own_rows, masks)
    id_row = jnp.where(lead, document_row, partner_row)
    shifts = [math.log2(s) for s in scales]
    total_rows = [zero_or(jnp.logical_not(lead), totals[k:k + 1]) - shifts[k] for k in range(count)]

    narrow = [m for m in uppers if m <= LANES]
    for step in range(total // block):
        rows = pl.ds(step * block, block)
        document_col = document_ids((block, 1), 0, me | 1, own_rows, masks, step * block)
        id_col = jnp.where(lead, col_ref[rows, count:count + 1], document_col)
        hit = id_col == id_row
        for k, s in enumerate(prefix_scores(v_ref, w_ref, rows, uppers)):
            score_ref[k] = s
        running = None
        stack = []
        for k in reversed(range(count)):
            gain = scales[k] * LOG2E
            total_col = zero_or(lead, col_ref[rows, k:k + 1])
            weight = jnp.exp2(score_ref[k] * gain - total_col - total_rows[k])
            weight = weight - jnp.where(hit, scales[k], 0.0)
            running = weight if running is None else running + weight
            band = running.astype(jnp.bfloat16)
            if k >= len(narrow):
                lower, upper = uppers[k - 1], uppers[k]
                product = jnp.dot(band, w_ref[:, lower:upper], preferred_element_type=jnp.float32)
                store(out_refs, product, step * block, lower, upper, chip_rows)
            else:
                stack.append(band)
        product = jnp.dot(
            jnp.concatenate(stack, axis=0), w_ref[:, :LANES], preferred_element_type=jnp.float32)
        lane = lax.broadcasted_iota(jnp.int32, (block, LANES), 1)
        chosen = product[:block]
        for at_stack in range(1, len(stack)):
            k = len(narrow) - 1 - at_stack
            chosen = jnp.where(
                lane < uppers[k], product[at_stack * block:(at_stack + 1) * block], chosen)
        store(out_refs, chosen, step * block, 0, LANES, chip_rows)


def rows_of(refs, lower, upper):
    return jnp.concatenate([ref[:, lower:upper] for ref in refs], axis=0)


def subtile_scores(v_refs, w_refs, uppers):
    narrow = [m for m in uppers if m <= LANES]
    left, right = rows_of(v_refs, 0, LANES), rows_of(w_refs, 0, LANES)
    slim = right.shape[0] < 2 * LANES
    head = right if slim else left
    count = head.shape[0]
    lane = lax.broadcasted_iota(jnp.int32, head.shape, 1)
    masked = jnp.concatenate(
        [jnp.where(lane < m, head, jnp.zeros_like(head)) for m in narrow], axis=0)
    if slim:
        stacked = transposed_dot(left, masked)
        parts = [stacked[:, k * count:(k + 1) * count] for k in range(len(narrow))]
    else:
        stacked = transposed_dot(masked, right)
        parts = [stacked[k * count:(k + 1) * count] for k in range(len(narrow))]
    yield from parts
    lower, running = narrow[-1], parts[-1]
    for upper in uppers[len(narrow):]:
        running = running + transposed_dot(
            rows_of(v_refs, lower, upper), rows_of(w_refs, lower, upper))
        yield running
        lower = upper


def subtile(lead, v_refs, w_refs, uppers, refs):
    power_ref, col_ref, line_ref = refs
    gains = [logit_gain * m ** -0.5 * LOG2E for m in uppers]
    count, across = power_ref.shape[1:]

    @pl.when(lead)
    def _():
        lane = lax.broadcasted_iota(jnp.int32, (count, LANES), 1)
        both = jnp.where(lane < STATS, 0.0, 1.0)
        for k, s in enumerate(subtile_scores(v_refs, w_refs, uppers)):
            logits = s * gains[k]
            peak = jnp.max(logits, axis=1, keepdims=True)
            power = jnp.exp2(logits - peak)
            power_ref[k] = power
            both = jnp.where(lane == k, peak, both)
            both = jnp.where(lane == STATS + k, jnp.sum(power, axis=1, keepdims=True), both)
        col_ref[...] = both
        line_ref[:, :count] = both.T[:2 * STATS]

    @pl.when(jnp.logical_not(lead))
    def _():
        line_ref[:STATS, :] = jnp.zeros((STATS, line_ref.shape[1]), jnp.float32)
        line_ref[STATS:, :] = jnp.ones((STATS, line_ref.shape[1]), jnp.float32)
        for k, s in enumerate(subtile_scores(v_refs, w_refs, uppers)):
            logits = s * gains[k]
            peak = jnp.max(logits, axis=0, keepdims=True)
            power = jnp.exp2(logits - peak)
            power_ref[k] = power
            line_ref[k:k + 1, :across] = peak
            line_ref[STATS + k:STATS + k + 1, :across] = jnp.sum(power, axis=0, keepdims=True)


def log_sum(pairs):
    top = functools.reduce(jnp.maximum, [peak for peak, _ in pairs])
    mass = functools.reduce(
        lambda a, b: a + b, [mass * jnp.exp2(peak - top) for peak, mass in pairs])
    return top + jnp.log(mass) * LOG2E


def tile_kernel(span, counts, uppers, own_rows, finish, *refs):
    groups = len(counts)
    shapes = subtiles(groups)
    tiles = [shapes[i] for i in span]
    r0, r1, c0, c1 = extent(tiles)
    me_ref, partner_ref = refs[:2]
    at = 2 + sum(counts[r0:r1])
    v_refs, w_refs = refs[2:at], refs[at:at + sum(counts[c0:c1])]
    at += sum(counts[c0:c1])
    earlier = refs[at:at + finish]
    outs = refs[at + finish:]
    lead = (me_ref[0] & 1) == 0
    for i, (t0, t1, u0, u1) in enumerate(tiles):
        subtile(
            lead, v_refs[sum(counts[r0:t0]):sum(counts[r0:t1])],
            w_refs[sum(counts[c0:u0]):sum(counts[c0:u1])], uppers, outs[3 * i:3 * i + 3])
    if not finish:
        outs[-1][...] = partner_ref[...]
        return
    stats_ref = outs[-1]
    every = [*earlier, *outs[2:3 * len(tiles):3]]
    segments = segments_of(groups)
    chip_rows = 2 * own_rows

    def merge(axis):
        for s0, s1 in segments:
            pairs = []
            for shape, line in zip(shapes, every):
                low, high = shape[axis:axis + 2]
                if low <= s0 and s1 <= high:
                    at = slice((s0 - low) * chip_rows, (s1 - low) * chip_rows)
                    pairs.append((line[:STATS, at], line[STATS:, at]))
            stats_ref[:, s0 * chip_rows:s1 * chip_rows] = log_sum(pairs)

    pl.when(lead)(lambda: merge(0))
    pl.when(jnp.logical_not(lead))(lambda: merge(2))

    count = len(uppers)
    stats_ref[count:count + 1, :chip_rows] = partner_ref[...]


def segments_of(groups):
    low, middle = groups // 2, groups // 2 + groups // 4
    return [(0, low), (low, middle), (middle, groups)]


def subtiles(groups):
    (_, low), (_, middle), _ = segments_of(groups)
    return [(0, low, 0, low), (low, middle, 0, low), (0, middle, low, middle),
            (middle, groups, 0, middle), (0, groups, middle, groups)]


def extent(tiles):
    first, second, third, fourth = zip(*tiles)
    return min(first), max(second), min(third), max(fourth)


def band_setup(groups, uppers, own_rows, masks, me_ref, stat_refs):
    count = len(uppers)
    total = stat_refs[0].shape[1]
    chip_rows = total // groups
    me = me_ref[0]
    lead = (me & 1) == 0
    own, first, second, swapped = [ref[...] for ref in stat_refs]
    values = [own, jnp.where(lead, first, swapped), second, jnp.where(lead, swapped, first)]
    parts, partners = [], []
    for j, value in enumerate(values):
        parts.append(jnp.concatenate(
            [value[:, (i ^ j) * chip_rows:((i ^ j) + 1) * chip_rows] for i in range(groups)], axis=1))
        partners.append(value[count:count + 1, :chip_rows])
    peak = functools.reduce(jnp.maximum, parts)
    mass = functools.reduce(lambda a, b: a + b, [jnp.exp2(part - peak) for part in parts])
    partner_row = jnp.concatenate(partners, axis=1)
    sub = lax.broadcasted_iota(jnp.int32, (STATS, total), 0)
    totals = peak + jnp.log(mass) * LOG2E
    for k in range(count):
        totals = jnp.where(sub == k, totals - math.log2(logit_gain * uppers[k] ** -0.5), totals)
    packed = jnp.concatenate(
        [totals[:count], partner_row, jnp.zeros((LANES - count - 1, total), jnp.float32)], axis=0)
    cols = packed.T
    id_row = jnp.where(
        lead, document_ids((1, total), 1, me | 1, own_rows, masks), partner_row)
    id_col = jnp.where(
        lead, cols[:, count:count + 1],
        document_ids((total, 1), 0, me | 1, own_rows, masks))
    return lead, totals, cols, id_row, id_col


def weights_of(segment, groups, setup, power_refs, col_refs, row_refs):
    lead, totals, cols, _, _ = setup
    chip_rows = totals.shape[1] // groups
    s0, s1 = segment
    strip = []
    for (r0, r1, c0, c1), power, col_peak, line in zip(
            subtiles(groups), power_refs, col_refs, row_refs):
        if r0 <= s0 and s1 <= r1:
            inner = slice((s0 - r0) * chip_rows, (s1 - r0) * chip_rows)
            outer = slice(s0 * chip_rows, s1 * chip_rows)
            across = slice(c0 * chip_rows, c1 * chip_rows)
            strip.append((
                c0, power, inner,
                jnp.where(lead, jnp.exp2(col_peak[inner, :] - cols[outer]), 1.0),
                jnp.where(lead, 1.0, jnp.exp2(line[:STATS, :(c1 - c0) * chip_rows] - totals[:, across]))))
    strip.sort(key=lambda item: item[0])
    return lambda k: jnp.concatenate([
        power[k, inner] * col_gain[:, k:k + 1] * row_gain[k:k + 1, :]
        for _, power, inner, col_gain, row_gain in strip], axis=1)


def last_band_kernel(groups, uppers, own_rows, masks, *refs):
    tiles = len(subtiles(groups))
    setup = band_setup(groups, uppers, own_rows, masks, refs[0], refs[1:1 + groups])
    at = 1 + groups
    power_refs, col_refs, row_refs = [refs[at + i * tiles:at + (i + 1) * tiles] for i in range(3)]
    segment = segments_of(groups)[-1]
    farthest = segment[1] - segment[0]
    w_refs, out_refs, after_ref = refs[at + 3 * tiles:-farthest - 1], refs[-farthest - 1:-1], refs[-1]
    _, totals, _, id_row, id_col = setup
    chip_rows = totals.shape[1] // groups
    k = len(uppers) - 1
    rows = slice(segment[0] * chip_rows, segment[1] * chip_rows)
    weight = weights_of(segment, groups, setup, power_refs, col_refs, row_refs)(k)
    weight = weight - jnp.where(id_col[rows] == id_row, logit_gain * uppers[k] ** -0.5, 0.0)
    after_ref[...] = weight
    product = jnp.dot(
        weight.astype(jnp.bfloat16), rows_of(w_refs, uppers[k - 1], uppers[k]),
        preferred_element_type=jnp.float32)
    store(out_refs, product, 0, 0, uppers[k] - uppers[k - 1], chip_rows)


def bands_kernel(groups, uppers, own_rows, masks, *refs):
    tiles = len(subtiles(groups))
    setup = band_setup(groups, uppers, own_rows, masks, refs[0], refs[1:1 + groups])
    at = 1 + groups
    power_refs, col_refs, row_refs = [refs[at + i * tiles:at + (i + 1) * tiles] for i in range(3)]
    segments = segments_of(groups)
    outs = groups + segments[-1][0]
    before_ref = refs[-outs - 1]
    w_refs, others, widest = refs[at + 3 * tiles:-outs - 1], refs[-outs:-outs + groups], refs[-outs + groups:]
    _, totals, _, id_row, id_col = setup
    chip_rows = totals.shape[1] // groups
    scales = [logit_gain * m ** -0.5 for m in uppers]
    last = len(uppers) - 1
    narrow = [k for k in range(last, -1, -1) if uppers[k] <= LANES]
    for block in (segments[1:], segments[:1]):
        first = block[0][0] * chip_rows
        rows = slice(first, block[-1][1] * chip_rows)
        height = rows.stop - first
        hit = id_col[rows] == id_row
        weights = [
            weights_of(segment, groups, setup, power_refs, col_refs, row_refs) for segment in block]
        tall = (block[0][1] - block[0][0]) * chip_rows
        running = weights[0](last) - jnp.where(hit[:tall], scales[last], 0.0)
        lower, upper = uppers[last - 1], uppers[last]
        product = jnp.dot(
            running.astype(jnp.bfloat16), rows_of(w_refs, lower, upper),
            preferred_element_type=jnp.float32)
        store(widest, product, first, 0, upper - lower, chip_rows)
        if len(block) > 1:
            running = jnp.concatenate([running, before_ref[...]], axis=0)
        stack = []
        for k in range(last - 1, -1, -1):
            weight = jnp.concatenate([part(k) for part in weights], axis=0)
            running = running + (weight - jnp.where(hit, scales[k], 0.0))
            band = running.astype(jnp.bfloat16)
            if k in narrow:
                stack.append(band)
                continue
            lower, upper = uppers[k - 1], uppers[k]
            product = jnp.dot(
                band, rows_of(w_refs, lower, upper), preferred_element_type=jnp.float32)
            store(others, product, first, lower, upper, chip_rows)
        product = jnp.dot(
            jnp.concatenate(stack, axis=0), rows_of(w_refs, 0, LANES),
            preferred_element_type=jnp.float32)
        lane = lax.broadcasted_iota(jnp.int32, (height, LANES), 1)
        chosen = product[:height]
        for i in range(1, len(stack)):
            chosen = jnp.where(
                lane < uppers[narrow[i]], product[i * height:(i + 1) * height], chosen)
        store(others, chosen, first, 0, LANES, chip_rows)


def store(out_refs, value, first_row, lower, upper, chip_rows):
    for at in range(0, value.shape[0], chip_rows):
        ref = out_refs[(first_row + at) // chip_rows]
        ref[:, lower:upper] = value[at:at + chip_rows].astype(ref.dtype)


def put_kernel(columns, me_ref, *refs):
    kept_ref, near_ref, given_ref, far_ref = refs[:4]
    queries_ref, documents_ref, ours_ref, theirs_ref, sems = refs[-5:]
    ours_ref[...] = kept_ref[...] + near_ref[...].astype(jnp.float32)
    theirs_ref[...] = given_ref[...] + far_ref[...].astype(jnp.float32)

    def write(first, second):
        copies = [pltpu.make_async_copy(ours_ref, first.at[:, columns], sems.at[0]),
                  pltpu.make_async_copy(theirs_ref, second.at[:, columns], sems.at[1])]
        for copy in copies:
            copy.start()
        for copy in copies:
            copy.wait()

    lead = (me_ref[0] & 1) == 0
    pl.when(lead)(lambda: write(queries_ref, documents_ref))
    pl.when(jnp.logical_not(lead))(lambda: write(documents_ref, queries_ref))


def on_device(queries, documents, partner):
    own_rows, feature_dim = queries.shape
    uppers = width_list(feature_dim)
    dp_size, rep_size = lax.axis_size("dp"), lax.axis_size("rep")
    devices = dp_size * rep_size
    bits = devices.bit_length() - 1
    assert rep_size == 2 and devices == 1 << bits and bits % 2 == 1
    stages = (bits - 1) // 2
    groups = 1 << stages
    pieces = 2 * groups
    query_masks = [1 << (2 * s + 1) for s in range(stages)]
    document_masks = [1 << (2 * s + 2) for s in range(stages)]
    total = pieces * own_rows
    chip_rows = 2 * own_rows

    role = lax.axis_index("rep")
    me = (lax.axis_index("dp") * rep_size + role).astype(jnp.int32).reshape(1)
    lead = role == 0

    def exchange(x, masks_of):
        return lax.ppermute(x, AXES, [(i, i ^ masks_of(i)) for i in range(devices)])

    def swap(x):
        return exchange(x, lambda i: 1)

    def along(x, stage):
        return exchange(x, lambda i: document_masks[stage] if i & 1 else query_masks[stage])

    vmem = pl.BlockSpec(memory_space=pltpu.VMEM)
    smem = pl.BlockSpec(memory_space=pltpu.SMEM)
    hbm = pl.BlockSpec(memory_space=pltpu.HBM)
    mine = jnp.where(lead, queries, documents)
    other = jnp.where(lead, documents, queries)
    got = swap(other)
    small = groups == 4 and WIDTHS * total * total * 4 <= 16 << 20
    cut = own_rows // 2 if small and own_rows % 32 == 0 else own_rows
    v = {0: [mine, got]}
    w = {0: [swap(mine), other]}
    for stage in reversed(range(stages)):
        for j in sorted(v):
            parts = v[j]
            if cut < own_rows and j == 0 and stage:
                parts = [mine, got[:cut], got[cut:]]
            v[j | 1 << stage] = [
                along(part, stage) for part in parts]
    for j in range(1, groups):
        w[j] = [swap(part) for part in v[j]]
    counts = [len(v[j]) for j in range(groups)]
    v_list = [part for j in range(groups) for part in v[j]]
    w_list = [part for j in range(groups) for part in w[j]]

    own_partner = partner.astype(jnp.float32).reshape(1, own_rows)
    far_partner = swap(own_partner)
    chip_partner = jnp.where(
        lead,
        jnp.concatenate([own_partner, far_partner], axis=1),
        jnp.concatenate([far_partner, own_partner], axis=1))

    def query_mask(j):
        return sum(mask for s, mask in enumerate(query_masks) if j >> s & 1)

    def gathered(stats):
        return [stats] + [exchange(stats, lambda i: query_mask(j)) for j in range(1, groups)]

    shape = lambda *dims: jax.ShapeDtypeStruct(dims, jnp.float32)

    def gradient_shapes(columns):
        return [
            jax.ShapeDtypeStruct((chip_rows, columns), jnp.bfloat16 if j & 1 else jnp.float32)
            for j in range(groups)]

    if not small:
        limit = 60 << 20
        stats = pl.pallas_call(
            functools.partial(stats_kernel, pieces, uppers),
            out_shape=shape(STATS, total),
            in_specs=[smem] + [vmem] * (1 + 2 * pieces),
            out_specs=vmem,
            scratch_shapes=[
                pltpu.VMEM((total, feature_dim), jnp.bfloat16),
                pltpu.VMEM((total, feature_dim), jnp.bfloat16),
                pltpu.VMEM((total, LANES), jnp.float32),
            ],
            compiler_params=pltpu.CompilerParams(vmem_limit_bytes=limit),
            name="tile_stats",
        )(me, chip_partner, *v_list, *w_list)
        whole = pl.pallas_call(
            functools.partial(grads_kernel, pieces, uppers, own_rows, document_masks),
            out_shape=gradient_shapes(feature_dim),
            in_specs=[smem] + [vmem] * (groups + 2 * pieces),
            out_specs=[vmem] * groups,
            scratch_shapes=[
                pltpu.VMEM((total, feature_dim), jnp.bfloat16),
                pltpu.VMEM((total, feature_dim), jnp.bfloat16),
                pltpu.VMEM((WIDTHS, block_of(total), total), jnp.float32),
                pltpu.VMEM((total, LANES), jnp.float32),
            ],
            compiler_params=pltpu.CompilerParams(vmem_limit_bytes=limit),
            name="tile_grads",
        )(me, *gathered(stats), *v_list, *w_list)
        chunks = [whole]
    else:
        shapes = subtiles(groups)
        limit = 20 << 20
        params = pltpu.CompilerParams(vmem_limit_bytes=limit)

        def tile(span, partner_row, earlier=()):
            first, end, left, right = extent([shapes[i] for i in span])
            operands = v_list[sum(counts[:first]):sum(counts[:end])]
            operands += w_list[sum(counts[:left]):sum(counts[:right])]
            stat_shapes = [shape(STATS, total)] if earlier else [shape(1, chip_rows)]
            result, area = [], 0
            for i in span:
                r0, r1, c0, c1 = shapes[i]
                tall, wide = (r1 - r0) * chip_rows, (c1 - c0) * chip_rows
                area += tall * wide
                result += [shape(WIDTHS, tall, wide), shape(tall, LANES),
                           shape(2 * STATS, max(tall, wide))]
            *arrays, last_array = pl.pallas_call(
                functools.partial(
                    tile_kernel, span, counts, uppers, own_rows, len(earlier)),
                out_shape=result + stat_shapes,
                in_specs=[smem] + [vmem] * (1 + len(operands) + len(earlier)),
                out_specs=[vmem] * (len(result) + 1),
                compiler_params=params,
                cost_estimate=pl.CostEstimate(
                    flops=6 * area * feature_dim, transcendentals=0,
                    bytes_accessed=2 * total * feature_dim),
            )(me, partner_row, *operands, *[one[2] for one in earlier])
            return [arrays[3 * i:3 * i + 3] for i in range(len(span))], last_array

        done, chip_partner = tile([0], chip_partner)
        for at in (1, 2, 3):
            more, chip_partner = tile([at], chip_partner)
            done += more
        more, stats = tile([4], chip_partner, done)
        done += more
        first = exchange(
            stats, lambda i: query_mask(3) if i & 1 else query_mask(1))
        second = exchange(stats, lambda i: query_mask(2))
        swapped = swap(first)
        common = [me, stats, first, second, swapped, *[t[0] for t in done], *[t[1] for t in done],
                  *[t[2] for t in done], *w_list]
        near = segments_of(groups)[-1][0]
        widest = feature_dim - uppers[-2]

        def bands(kernel, more, outs):
            return pl.pallas_call(
                functools.partial(kernel, groups, uppers, own_rows, document_masks),
                out_shape=outs,
                in_specs=[smem] + [vmem] * (len(common) - 1 + len(more)),
                out_specs=[vmem] * len(outs),
                compiler_params=params,
                cost_estimate=pl.CostEstimate(
                    flops=2 * total * total * feature_dim, transcendentals=0,
                    bytes_accessed=4 * total * feature_dim),
            )(*common, *more)

        *far_ones, running = bands(
            last_band_kernel, [],
            gradient_shapes(widest)[near:] + [shape((groups - near) * chip_rows, total)])
        rest = bands(
            bands_kernel, [running], gradient_shapes(uppers[-2]) + gradient_shapes(widest)[:near])
        chunks = [[*rest[groups:], *far_ones], rest[:groups]]

    def put(columns, parts, before):
        return pl.pallas_call(
            functools.partial(put_kernel, columns),
            out_shape=[jax.ShapeDtypeStruct(queries.shape, jnp.float32)] * 2,
            in_specs=[smem] + [vmem] * 4 + [hbm] * len(before),
            out_specs=[hbm, hbm],
            scratch_shapes=[pltpu.VMEM(parts[0].shape, jnp.float32)] * 2
            + [pltpu.SemaphoreType.DMA((2,))],
            input_output_aliases={5 + i: i for i in range(len(before))},
            compiler_params=pltpu.CompilerParams(vmem_limit_bytes=8 << 20),
            cost_estimate=pl.CostEstimate(flops=1000, transcendentals=0, bytes_accessed=1000),
        )(me, *parts, *before)

    gradients, end = [], feature_dim
    for c, chunk in enumerate(chunks):
        partial = dict(enumerate(chunk))
        for stage in range(stages - 1):
            step = 1 << stage
            for j in sorted([j for j in partial if j & step], reverse=True):
                arrived = along(partial.pop(j).astype(jnp.bfloat16), stage)
                partial[j ^ step] = partial[j ^ step] + arrived.astype(jnp.float32)
                if stage == stages - 2 and j ^ step:
                    partial[j ^ step] = partial[j ^ step].astype(jnp.bfloat16)
        stage = stages - 1
        outgoing = partial[1 << stage]
        kept = partial[0]
        start = end - kept.shape[1]
        if c < len(chunks) - 1:
            arrived = along(outgoing, stage)
            near = arrived[:own_rows]
            theirs = kept[own_rows:] + arrived[own_rows:].astype(jnp.float32)
            parts = [kept[:own_rows], near, swap(theirs), jnp.zeros_like(near)]
        else:
            far = lambda i: document_masks[stage] ^ 1 if i & 1 else query_masks[stage] ^ 1
            near_arrived = along(outgoing[:own_rows], stage)
            far_arrived = exchange(outgoing[own_rows:], far)
            ours, theirs = lax.optimization_barrier((kept[:own_rows], kept[own_rows:]))
            parts = [ours, near_arrived, swap(theirs), far_arrived]
        gradients = put(slice(start, end), parts, gradients)
        end = start
    return tuple(gradients)


def solution(mesh):
    return jax.shard_map(
        on_device,
        mesh=mesh,
        in_specs=(P(AXES, None), P(AXES, None), P(AXES)),
        out_specs=(P(AXES, None), P(AXES, None)),
        check_vma=False,
    )
```
